16 devices in a mesh: tp: 4 (over z, y), dp: 4 (over x, core).
Axes of the slice: x: 2, y: 2, z: 2, core: 2. Of those that a mesh axis runs over, the one named last changes fastest.
Arguments:
- x_in: bfloat16 [2, 128, 4096], P(None, ('dp', 'tp'))
- w_gate: bfloat16 [4096, 14336], P('dp', 'tp')
- w_up: bfloat16 [4096, 14336], P('dp', 'tp')
- w_down: bfloat16 [14336, 4096], P('tp', 'dp')
- grad_y: bfloat16 [2, 128, 4096], P(None, ('dp', 'tp'))
Outputs:
- output 1: bfloat16 [2, 128, 4096], P(None, ('dp', 'tp'))
- output 2: bfloat16 [2, 128, 4096], P(None, ('dp', 'tp'))
- output 3: float32 [4096, 14336], P('dp', 'tp')
- output 4: float32 [4096, 14336], P('dp', 'tp')
- output 5: float32 [14336, 4096], P('tp', 'dp')
All inputs are finite; a program needn't handle non-finite values.
Results may differ from the reference program's by a relative error of at most 0.001.
Values are sent between devices in bfloat16 or wider.
A program may use at most 1 GiB of HBM per device.

```python
import jax
import jax.numpy as jnp
from jax import lax

D = 4096
FF = 14336
T_ROWS = 8
DATA_SIZE = 4
MODEL_SIZE = 4
MICRO_STEPS = 2
ALL_ROWS = DATA_SIZE * MODEL_SIZE * T_ROWS


def setup_inputs(seed: int = 0) -> dict:
    keys = jax.random.split(jax.random.key(seed), 5)
    x_in = jax.random.normal(keys[0], (MICRO_STEPS, ALL_ROWS, D), jnp.float32)
    w_gate = jax.random.normal(keys[1], (D, FF), jnp.float32) * D ** -0.5
    w_up = jax.random.normal(keys[2], (D, FF), jnp.float32) * D ** -0.5
    w_down = jax.random.normal(keys[3], (FF, D), jnp.float32) * FF ** -0.5
    grad_y = jax.random.normal(keys[4], (MICRO_STEPS, ALL_ROWS, D), jnp.float32)
    return {"x_in": x_in.astype(jnp.bfloat16), "w_gate": w_gate.astype(jnp.bfloat16), "w_up": w_up.astype(jnp.bfloat16), "w_down": w_down.astype(jnp.bfloat16), "grad_y": grad_y.astype(jnp.bfloat16)}


def mlp_rows(x_blk, dy_blk, w_gate, w_up, w_down):
    gate_pre = jnp.dot(x_blk, w_gate, preferred_element_type=jnp.float32)
    up_pre = jnp.dot(x_blk, w_up, preferred_element_type=jnp.float32)
    sig_gate = jax.nn.sigmoid(gate_pre)
    act_gate = gate_pre * sig_gate
    hidden = (act_gate * up_pre).astype(jnp.bfloat16)
    y_blk = (x_blk.astype(jnp.float32) + jnp.dot(hidden, w_down, preferred_element_type=jnp.float32)).astype(jnp.bfloat16)
    grad_h = jnp.dot(dy_blk, w_down.T, preferred_element_type=jnp.float32)
    grad_gate = (grad_h * up_pre * sig_gate * (1.0 + gate_pre * (1.0 - sig_gate))).astype(jnp.bfloat16)
    grad_up = (grad_h * act_gate).astype(jnp.bfloat16)
    dx_blk = (dy_blk.astype(jnp.float32) + jnp.dot(grad_gate, w_gate.T, preferred_element_type=jnp.float32) + jnp.dot(grad_up, w_up.T, preferred_element_type=jnp.float32)).astype(jnp.bfloat16)
    dw_gate = jnp.dot(x_blk.T, grad_gate, preferred_element_type=jnp.float32)
    dw_up = jnp.dot(x_blk.T, grad_up, preferred_element_type=jnp.float32)
    dw_down = jnp.dot(hidden.T, dy_blk, preferred_element_type=jnp.float32)
    return y_blk, dx_blk, dw_gate, dw_up, dw_down


def reference(x_in, w_gate, w_up, w_down, grad_y):
    blocks = MICRO_STEPS * DATA_SIZE * MODEL_SIZE
    x_blocks = x_in.reshape(blocks, T_ROWS, D)
    dy_blocks = grad_y.reshape(blocks, T_ROWS, D)

    def scan_step(acc_sums, row_pair):
        y_blk, dx_blk, dw_gate, dw_up, dw_down = mlp_rows(row_pair[0], row_pair[1], w_gate, w_up, w_down)
        new_sums = (acc_sums[0] + dw_gate, acc_sums[1] + dw_up, acc_sums[2] + dw_down)
        return new_sums, (y_blk, dx_blk)

    zero_sums = (jnp.zeros((D, FF), jnp.float32), jnp.zeros((D, FF), jnp.float32), jnp.zeros((FF, D), jnp.float32))
    (sum_gate, sum_up, sum_down), (y_blocks, dx_blocks) = lax.scan(scan_step, zero_sums, (x_blocks, dy_blocks))
    return (y_blocks.reshape(x_in.shape), dx_blocks.reshape(x_in.shape), sum_gate, sum_up, sum_down)
```

```python
import jax
import jax.numpy as jnp
from jax import lax
from jax.experimental import pallas as pl
from jax.experimental.pallas import tpu as pltpu
from jax.sharding import PartitionSpec as P

MESH = pl.DeviceIdType.MESH
F32 = jnp.float32
BF16 = jnp.bfloat16
GROUPS = 4
SLOTS = 4
FINAL_LAG = 4
FORWARD_LAG = 7
BACK_LAG = 8


def dot(lhs, rhs):
    return lax.dot_general(lhs, rhs, (((1,), (0,)), ((), ())), preferred_element_type=F32)


def dot_t(lhs, rhs):
    return lax.dot_general(lhs, rhs, (((1,), (1,)), ((), ())), preferred_element_type=F32)


def make_kernel(chunks, width):
    total = GROUPS * chunks
    rest = total - chunks

    def kernel(x_ref, dy_ref, wg_hbm, wu_hbm, wd_hbm,
               y_out, dx_out, h_out, da_out, db_out, xc_out, dyc_out,
               wg, wu, wd, cols, part, near, far, hid, acc, acc_in, tail, rows,
               w_sem, first_send, first_recv, spread_send, spread_recv,
               near_send, near_recv, far_send, far_recv,
               hc_send, hc_recv, hx_send, hx_recv, hf_send, hf_recv,
               acc_send, acc_recv, tail_send, tail_recv, out_sem, cols_sem, row_sem):
        tp = lax.axis_index("tp")
        dp = lax.axis_index("dp")
        z, y = tp // 2, tp % 2
        x, core = dp // 2, dp % 2
        ox, oc = 1 - x, 1 - core
        core_peer = {"tp": tp, "dp": x * 2 + oc}
        x_peer = {"tp": tp, "dp": ox * 2 + core}
        mine = core * 2 + x
        depth = cols.shape[-1]

        def tp_peer(group):
            return {"tp": ((z + group // 2) % 2) * 2 + (y + group % 2) % 2, "dp": dp}

        def dp_peer(k):
            px, pc = (x + k // 2) % 2, (core + k % 2) % 2
            return px * 2 + pc, pc * 2 + px

        def weight_copies(c):
            span = pl.ds(pl.multiple_of(c * width, width), width)
            return (pltpu.make_async_copy(wg_hbm.at[:, span], wg.at[c], w_sem.at[c, 0]),
                    pltpu.make_async_copy(wu_hbm.at[:, span], wu.at[c], w_sem.at[c, 1]),
                    pltpu.make_async_copy(wd_hbm.at[span], wd.at[c], w_sem.at[c, 2]))

        def remote(src, dst, send, recv, device):
            return pltpu.make_async_remote_copy(src_ref=src, dst_ref=dst, send_sem=send, recv_sem=recv,
                                                device_id=device, device_id_type=MESH)

        def first_copy(kind, k):
            peer, _ = dp_peer(k)
            src = (x_ref, dy_ref)[kind].at[:, pl.ds(pl.multiple_of(peer * depth, depth), depth)]
            return remote(src, cols.at[0, kind, mine], first_send.at[kind, k - 1], first_recv.at[kind, k - 1], {"tp": tp, "dp": peer})

        def spread_copy(group):
            return remote(cols.at[0], cols.at[group], spread_send.at[group - 1], spread_recv.at[group - 1], tp_peer(group))

        def near_copy(i):
            return remote(part.at[i, pl.ds(oc * 2, 2)], near.at[i], near_send.at[i], near_recv.at[i], core_peer)

        def far_copy(i):
            return remote(near.at[i, ox], far.at[i], far_send.at[i], far_recv.at[i], x_peer)

        def hc_copy(i):
            here = hid.at[i, :, mine]
            return remote(here, here, hc_send.at[i], hc_recv.at[i], core_peer)

        def hx_copy(i):
            here = hid.at[i, :, mine]
            return remote(here, here, hx_send.at[i], hx_recv.at[i], x_peer)

        def hf_copy(i):
            there = hid.at[i, :, core * 2 + ox]
            return remote(there, there, hf_send.at[i], hf_recv.at[i], core_peer)

        def acc_copy(group):
            return remote(acc.at[group], acc_in.at[group - 1], acc_send.at[group - 1], acc_recv.at[group - 1], tp_peer(group))

        def out_copies(i):
            group, c = i // chunks, i % chunks
            span = pl.ds(pl.multiple_of(c * width, width), width)
            return [pltpu.make_async_copy(hid.at[i, k], ref.at[group, :, :, span], out_sem.at[i, k])
                    for k, ref in enumerate((h_out, da_out, db_out))]

        def cols_copies(group):
            return [pltpu.make_async_copy(cols.at[group, k], ref.at[group], cols_sem.at[group, k])
                    for k, ref in enumerate((xc_out, dyc_out))]

        def tail_copy(kind, k):
            peer, slot = dp_peer(k)
            dst = rows.at[kind, :, pl.ds(pl.multiple_of(dp * depth, depth), depth)]
            return remote(tail.at[kind, slot], dst, tail_send.at[kind, k - 1], tail_recv.at[kind, k - 1], {"tp": tp, "dp": peer})

        for c in range(chunks):
            for copy in weight_copies(c):
                copy.start()

        barrier = pltpu.get_barrier_semaphore()
        for k in range(1, 4):
            pl.semaphore_signal(barrier, inc=1, device_id={"tp": tp, "dp": dp_peer(k)[0]}, device_id_type=MESH)
            pl.semaphore_signal(barrier, inc=1, device_id=tp_peer(k), device_id_type=MESH)
        pl.semaphore_wait(barrier, 6)

        for k in (2, 3, 1):
            for kind in range(2):
                first_copy(kind, k).start()
        own = pl.ds(pl.multiple_of(dp * depth, depth), depth)
        cols[0, 0, mine] = x_ref[:, own]
        cols[0, 1, mine] = dy_ref[:, own]
        acc[...] = jnp.zeros_like(acc)
        for k in (1, 2, 3):
            for kind in range(2):
                first_copy(kind, k).wait_recv()
        for group in (1, 2, 3):
            spread_copy(group).start()

        def products(i):
            group, c = i // chunks, i % chunks

            @pl.when(group == 0)
            def _():
                for copy in weight_copies(c):
                    copy.wait()

            @pl.when(jnp.logical_and(group > 0, c == 0))
            def _():
                spread_copy(group).wait_recv()

            x_rows = cols[group, 0].reshape(SLOTS * 16, depth)
            dy_rows = cols[group, 1].reshape(SLOTS * 16, depth)
            for k, value in enumerate((dot(x_rows, wg[c]), dot(x_rows, wu[c]), dot_t(dy_rows, wd[c]))):
                for slot in range(SLOTS):
                    part[i, slot, k] = value[slot * 16:(slot + 1) * 16]
            near_copy(i).start()

        def half_sum(i):
            near_copy(i).wait_recv()
            near[i, ox] = near[i, ox] + part[i, core * 2 + ox]
            far_copy(i).start()

        def activations(i):
            far_copy(i).wait_recv()
            gate = part[i, mine, 0] + near[i, x, 0] + far[i, 0]
            up = part[i, mine, 1] + near[i, x, 1] + far[i, 1]
            grad = part[i, mine, 2] + near[i, x, 2] + far[i, 2]
            sig = jax.nn.sigmoid(gate)
            act = gate * sig
            hid[i, 0, mine] = (act * up).astype(BF16)
            hid[i, 1, mine] = (grad * up * sig * (1.0 + gate * (1.0 - sig))).astype(BF16)
            hid[i, 2, mine] = (grad * act).astype(BF16)
            hc_copy(i).start()

        def back(i):
            group, c = i // chunks, i % chunks
            hc_copy(i).wait_recv()
            hf_copy(i).wait_recv()
            for copy in out_copies(i):
                copy.start()
            h_rows = hid[i, 0].reshape(SLOTS * 16, width)
            da_rows = hid[i, 1].reshape(SLOTS * 16, width)
            db_rows = hid[i, 2].reshape(SLOTS * 16, width)
            acc[group, 0] += dot(h_rows, wd[c]).reshape(SLOTS, 16, depth)
            acc[group, 1] += (dot_t(da_rows, wg[c]) + dot_t(db_rows, wu[c])).reshape(SLOTS, 16, depth)

            @pl.when(jnp.logical_and(group > 0, c == chunks - 1))
            def _():
                acc_copy(group).start()

        def step(s, carry):
            @pl.when(s < total)
            def _():
                products(s)

            @pl.when(jnp.logical_and(s >= 1, s < total + 1))
            def _():
                half_sum(s - 1)

            @pl.when(jnp.logical_and(s >= FINAL_LAG, s < total + FINAL_LAG))
            def _():
                activations(s - FINAL_LAG)

            @pl.when(jnp.logical_and(s >= chunks + FINAL_LAG, s < total + FINAL_LAG))
            def _():
                hx_copy(s - FINAL_LAG).start()

            @pl.when(jnp.logical_and(s >= total, s < total + chunks))
            def _():
                hx_copy(s - total).start()

            @pl.when(jnp.logical_and(s >= chunks + FORWARD_LAG, s < chunks + FORWARD_LAG + total))
            def _():
                i = (s - FORWARD_LAG) % total
                hx_copy(i).wait_recv()
                hf_copy(i).start()

            @pl.when(s >= chunks + BACK_LAG)
            def _():
                back((s - BACK_LAG) % total)

            return carry

        lax.fori_loop(0, total + chunks + BACK_LAG, step, 0)

        for group in range(GROUPS):
            for copy in cols_copies(group):
                copy.start()
        for group in (1, 2, 3):
            acc_copy(group).wait_recv()
        for kind in range(2):
            value = acc[0, kind] + acc_in[0, kind] + acc_in[1, kind] + acc_in[2, kind]
            tail[kind] = (cols[0, kind].astype(F32) + value).astype(BF16)
        for k in (2, 3, 1):
            for kind in range(2):
                tail_copy(kind, k).start()
        for kind in range(2):
            rows[kind, :, own] = tail[kind, mine]
        for k in (1, 2, 3):
            for kind in range(2):
                tail_copy(kind, k).wait_recv()
        row_copies = [pltpu.make_async_copy(rows.at[k], ref, row_sem.at[k]) for k, ref in enumerate((y_out, dx_out))]
        for copy in row_copies:
            copy.start()

        for k in (1, 2, 3):
            for kind in range(2):
                first_copy(kind, k).wait_send()
                tail_copy(kind, k).wait_send()
            spread_copy(k).wait_send()
            acc_copy(k).wait_send()

        def drain(i, carry):
            near_copy(i).wait_send()
            far_copy(i).wait_send()
            hc_copy(i).wait_send()
            hx_copy(i).wait_send()
            hf_copy(i).wait_send()
            for copy in out_copies(i):
                copy.wait()
            return carry

        lax.fori_loop(0, total, drain, 0)
        for group in range(GROUPS):
            for copy in cols_copies(group):
                copy.wait()
        for copy in row_copies:
            copy.wait()

    return kernel, total


def solution(mesh):
    row_spec = P(None, ("dp", "tp"), None)
    in_specs = (row_spec, P("dp", "tp"), P("dp", "tp"), P("tp", "dp"), row_spec)
    out_specs = (row_spec, row_spec, P("dp", "tp"), P("dp", "tp"), P("tp", "dp"))

    def local_step(x_loc, w_gate_loc, w_up_loc, w_down_loc, dy_loc):
        depth, hidden = w_gate_loc.shape
        micro, local_rows, model = x_loc.shape
        width = 512
        chunks = hidden // width
        kernel, total = make_kernel(chunks, width)
        dma = pltpu.SemaphoreType.DMA
        any_space = pl.BlockSpec(memory_space=pl.ANY)
        vmem = pl.BlockSpec(memory_space=pltpu.VMEM)
        hid_shape = jax.ShapeDtypeStruct((GROUPS, SLOTS, 16, hidden), BF16)
        col_shape = jax.ShapeDtypeStruct((GROUPS, SLOTS, 16, depth), BF16)
        row_shape = jax.ShapeDtypeStruct((16, model), BF16)
        outs = pl.pallas_call(
            kernel,
            out_shape=[row_shape, row_shape, hid_shape, hid_shape, hid_shape, col_shape, col_shape],
            in_specs=[vmem, vmem, any_space, any_space, any_space],
            out_specs=[any_space] * 7,
            scratch_shapes=[
                pltpu.VMEM((chunks, depth, width), BF16),
                pltpu.VMEM((chunks, depth, width), BF16),
                pltpu.VMEM((chunks, width, depth), BF16),
                pltpu.VMEM((GROUPS, 2, SLOTS, 16, depth), BF16),
                pltpu.VMEM((total, SLOTS, 3, 16, width), F32),
                pltpu.VMEM((total, 2, 3, 16, width), F32),
                pltpu.VMEM((total, 3, 16, width), F32),
                pltpu.VMEM((total, 3, SLOTS, 16, width), BF16),
                pltpu.VMEM((GROUPS, 2, SLOTS, 16, depth), F32),
                pltpu.VMEM((GROUPS - 1, 2, SLOTS, 16, depth), F32),
                pltpu.VMEM((2, SLOTS, 16, depth), BF16),
                pltpu.VMEM((2, 16, model), BF16),
                dma((chunks, 3)),
                dma((2, 3)), dma((2, 3)),
                dma((3,)), dma((3,)),
                dma((total,)), dma((total,)),
                dma((total,)), dma((total,)),
                dma((total,)), dma((total,)),
                dma((total,)), dma((total,)),
                dma((total,)), dma((total,)),
                dma((3,)), dma((3,)),
                dma((2, 3)), dma((2, 3)),
                dma((total, 3)), dma((GROUPS, 2)), dma((2,)),
            ],
            compiler_params=pltpu.CompilerParams(collective_id=0, has_side_effects=True, vmem_limit_bytes=67043328),
        )(x_loc.reshape(micro * local_rows, model), dy_loc.reshape(micro * local_rows, model), w_gate_loc, w_up_loc, w_down_loc)
        y_rows, dx_rows, h_all, da_all, db_all, x_cols, dy_cols = outs
        flat = lambda value: value.reshape(-1, value.shape[-1])
        over_rows = (((0,), (0,)), ((), ()))
        dw_gate = lax.dot_general(flat(x_cols), flat(da_all), over_rows, preferred_element_type=F32)
        dw_up = lax.dot_general(flat(x_cols), flat(db_all), over_rows, preferred_element_type=F32)
        dw_down = lax.dot_general(flat(h_all), flat(dy_cols), over_rows, preferred_element_type=F32)
        return y_rows.reshape(x_loc.shape), dx_rows.reshape(x_loc.shape), dw_gate, dw_up, dw_down

    return jax.shard_map(local_step, mesh=mesh, in_specs=in_specs, out_specs=out_specs, check_vma=False)
```

```python
import jax
import jax.numpy as jnp
from jax import lax
from jax.experimental import pallas as pl
from jax.experimental.pallas import tpu as pltpu
from jax.sharding import PartitionSpec as P

MESH = pl.DeviceIdType.MESH
F32 = jnp.float32
BF16 = jnp.bfloat16
GROUPS = 4
SLOTS = 4
FINAL_LAG = 4
FORWARD_LAG = 12
BACK_LAG = 13
EARLY = 4


def dot(lhs, rhs):
    return lax.dot_general(lhs, rhs, (((1,), (0,)), ((), ())), preferred_element_type=F32)


def dot_t(lhs, rhs):
    return lax.dot_general(lhs, rhs, (((1,), (1,)), ((), ())), preferred_element_type=F32)


def make_kernel(chunks, width):
    total = GROUPS * chunks

    def kernel(x_hbm, dy_hbm, wg_hbm, wu_hbm, wd_hbm,
               y_out, dx_out, h_out, da_out, db_out, xc_out, dyc_out,
               wg, wu, wd, x_ref, dy_ref, cols, part, near, far, hid, acc, acc_in, tail, rows,
               w_sem, first_send, first_recv, spread_send, spread_recv,
               near_send, near_recv, far_send, far_recv,
               hc_send, hc_recv, hx_send, hx_recv, hf_send, hf_recv,
               acc_send, acc_recv, tail_send, tail_recv, out_sem, cols_sem, row_sem, in_sem):
        tp = lax.axis_index("tp")
        dp = lax.axis_index("dp")
        z, y = tp // 2, tp % 2
        x, core = dp // 2, dp % 2
        ox, oc = 1 - x, 1 - core
        core_peer = {"tp": tp, "dp": x * 2 + oc}
        x_peer = {"tp": tp, "dp": ox * 2 + core}
        mine = core * 2 + x
        depth = cols.shape[-1]

        def tp_peer(group):
            return {"tp": ((z + group % 2) % 2) * 2 + (y + ((group + 1) // 2) % 2) % 2, "dp": dp}

        def chunk_at(s):
            return jnp.where(s < EARLY, s, jnp.where(s < total - chunks + EARLY, s + chunks - EARLY, s + chunks - total))

        def dp_peer(k):
            px, pc = (x + k // 2) % 2, (core + k % 2) % 2
            return px * 2 + pc, pc * 2 + px

        def weight_copies(c):
            span = pl.ds(pl.multiple_of(c * width, width), width)
            return (pltpu.make_async_copy(wg_hbm.at[:, span], wg.at[c], w_sem.at[c, 0]),
                    pltpu.make_async_copy(wu_hbm.at[:, span], wu.at[c], w_sem.at[c, 1]),
                    pltpu.make_async_copy(wd_hbm.at[span], wd.at[c], w_sem.at[c, 2]))

        def remote(src, dst, send, recv, device):
            return pltpu.make_async_remote_copy(src_ref=src, dst_ref=dst, send_sem=send, recv_sem=recv,
                                                device_id=device, device_id_type=MESH)

        def first_copy(kind, k):
            peer, _ = dp_peer(k)
            src = (x_ref, dy_ref)[kind].at[:, pl.ds(pl.multiple_of(peer * depth, depth), depth)]
            return remote(src, cols.at[0, kind, mine], first_send.at[kind, k - 1], first_recv.at[kind, k - 1], {"tp": tp, "dp": peer})

        def spread_copy(group):
            return remote(cols.at[0], cols.at[group], spread_send.at[group - 1], spread_recv.at[group - 1], tp_peer(group))

        def near_copy(i):
            return remote(part.at[i, pl.ds(oc * 2, 2)], near.at[i], near_send.at[i], near_recv.at[i], core_peer)

        def far_copy(i):
            return remote(near.at[i, ox], far.at[i], far_send.at[i], far_recv.at[i], x_peer)

        def hc_copy(i):
            here = hid.at[i, :, mine]
            return remote(here, here, hc_send.at[i], hc_recv.at[i], core_peer)

        def hx_copy(i):
            here = hid.at[i, :, mine]
            return remote(here, here, hx_send.at[i], hx_recv.at[i], x_peer)

        def hf_copy(i):
            there = hid.at[i, :, core * 2 + ox]
            return remote(there, there, hf_send.at[i], hf_recv.at[i], core_peer)

        def acc_copy(group):
            return remote(acc.at[group], acc_in.at[group - 1], acc_send.at[group - 1], acc_recv.at[group - 1], tp_peer(group))

        def out_copies(i):
            group, c = i // chunks, i % chunks
            span = pl.ds(pl.multiple_of(c * width, width), width)
            return [pltpu.make_async_copy(hid.at[i, k], ref.at[group, :, :, span], out_sem.at[i, k])
                    for k, ref in enumerate((h_out, da_out, db_out))]

        def cols_copies(group):
            return [pltpu.make_async_copy(cols.at[group, k], ref.at[group], cols_sem.at[group, k])
                    for k, ref in enumerate((xc_out, dyc_out))]

        def tail_copy(kind, k):
            peer, slot = dp_peer(k)
            dst = rows.at[kind, :, pl.ds(pl.multiple_of(dp * depth, depth), depth)]
            return remote(tail.at[kind, slot], dst, tail_send.at[kind, k - 1], tail_recv.at[kind, k - 1], {"tp": tp, "dp": peer})

        row_loads = [pltpu.make_async_copy(src, dst, in_sem.at[k]) for k, (src, dst) in enumerate(((x_hbm, x_ref), (dy_hbm, dy_ref)))]
        for copy in row_loads:
            copy.start()
        for c in range(chunks):
            for copy in weight_copies(c):
                copy.start()

        barrier = pltpu.get_barrier_semaphore()
        for k in range(1, 4):
            pl.semaphore_signal(barrier, inc=1, device_id={"tp": tp, "dp": dp_peer(k)[0]}, device_id_type=MESH)
            pl.semaphore_signal(barrier, inc=1, device_id=tp_peer(k), device_id_type=MESH)
        for copy in row_loads:
            copy.wait()
        pl.semaphore_wait(barrier, 6)

        for k in (2, 3, 1):
            for kind in range(2):
                first_copy(kind, k).start()
        own = pl.ds(pl.multiple_of(dp * depth, depth), depth)
        cols[0, 0, mine] = x_ref[:, own]
        cols[0, 1, mine] = dy_ref[:, own]
        acc[...] = jnp.zeros_like(acc)
        for k in (1, 2, 3):
            for kind in range(2):
                first_copy(kind, k).wait_recv()
        for group in (1, 2, 3):
            spread_copy(group).start()

        def products(i):
            group, c = i // chunks, i % chunks

            @pl.when(group == jnp.where(c < EARLY, 0, 1))
            def _():
                for copy in weight_copies(c):
                    copy.wait()

            @pl.when(jnp.logical_and(group > 0, c == 0))
            def _():
                spread_copy(group).wait_recv()

            x_rows = cols[group, 0].reshape(SLOTS * 16, depth)
            dy_rows = cols[group, 1].reshape(SLOTS * 16, depth)
            for k, value in enumerate((dot(x_rows, wg[c]), dot(x_rows, wu[c]), dot_t(dy_rows, wd[c]))):
                for slot in range(SLOTS):
                    part[i, slot, k] = value[slot * 16:(slot + 1) * 16]
            near_copy(i).start()

        def half_sum(i):
            near_copy(i).wait_recv()
            near[i, ox] = near[i, ox] + part[i, core * 2 + ox]
            far_copy(i).start()

        def activations(i):
            far_copy(i).wait_recv()
            gate = part[i, mine, 0] + near[i, x, 0] + far[i, 0]
            up = part[i, mine, 1] + near[i, x, 1] + far[i, 1]
            grad = part[i, mine, 2] + near[i, x, 2] + far[i, 2]
            sig = jax.nn.sigmoid(gate)
            act = gate * sig
            hid[i, 0, mine] = (act * up).astype(BF16)
            hid[i, 1, mine] = (grad * up * sig * (1.0 + gate * (1.0 - sig))).astype(BF16)
            hid[i, 2, mine] = (grad * act).astype(BF16)
            hc_copy(i).start()

        def back(i):
            group, c = i // chunks, i % chunks
            hc_copy(i).wait_recv()
            hf_copy(i).wait_recv()
            for copy in out_copies(i):
                copy.start()
            h_rows = hid[i, 0].reshape(SLOTS * 16, width)
            da_rows = hid[i, 1].reshape(SLOTS * 16, width)
            db_rows = hid[i, 2].reshape(SLOTS * 16, width)
            acc[group, 0] += dot(h_rows, wd[c]).reshape(SLOTS, 16, depth)
            acc[group, 1] += (dot_t(da_rows, wg[c]) + dot_t(db_rows, wu[c])).reshape(SLOTS, 16, depth)

            @pl.when(jnp.logical_and(group > 0, c == chunks - 1))
            def _():
                acc_copy(group).start()

        def step(s, carry):
            @pl.when(s < total)
            def _():
                products(chunk_at(s))

            @pl.when(jnp.logical_and(s >= 1, s < total + 1))
            def _():
                half_sum(chunk_at(s - 1))

            @pl.when(jnp.logical_and(s >= FINAL_LAG, s < total + FINAL_LAG))
            def _():
                activations(chunk_at(s - FINAL_LAG))

            @pl.when(jnp.logical_and(s >= EARLY + FINAL_LAG, s < total - chunks + EARLY + FINAL_LAG))
            def _():
                hx_copy(s - FINAL_LAG + chunks - EARLY).start()

            @pl.when(jnp.logical_and(s >= total, s < total + chunks))
            def _():
                hx_copy(s - total).start()

            @pl.when(jnp.logical_and(s >= FORWARD_LAG, s < FORWARD_LAG + total))
            def _():
                i = (s - FORWARD_LAG + chunks) % total
                hx_copy(i).wait_recv()
                hf_copy(i).start()

            @pl.when(s >= BACK_LAG)
            def _():
                back((s - BACK_LAG + chunks) % total)

            return carry

        lax.fori_loop(0, total + BACK_LAG, step, 0)

        for group in range(GROUPS):
            for copy in cols_copies(group):
                copy.start()
        for group in (1, 2, 3):
            acc_copy(group).wait_recv()
        for kind in range(2):
            value = acc[0, kind] + acc_in[0, kind] + acc_in[1, kind] + acc_in[2, kind]
            tail[kind] = (cols[0, kind].astype(F32) + value).astype(BF16)
        for k in (2, 3, 1):
            for kind in range(2):
                tail_copy(kind, k).start()
        for kind in range(2):
            rows[kind, :, own] = tail[kind, mine]
        for k in (1, 2, 3):
            for kind in range(2):
                tail_copy(kind, k).wait_recv()
        row_copies = [pltpu.make_async_copy(rows.at[k], ref, row_sem.at[k]) for k, ref in enumerate((y_out, dx_out))]
        for copy in row_copies:
            copy.start()

        for k in (1, 2, 3):
            for kind in range(2):
                first_copy(kind, k).wait_send()
                tail_copy(kind, k).wait_send()
            spread_copy(k).wait_send()
            acc_copy(k).wait_send()

        def drain(i, carry):
            near_copy(i).wait_send()
            far_copy(i).wait_send()
            hc_copy(i).wait_send()
            hx_copy(i).wait_send()
            hf_copy(i).wait_send()
            for copy in out_copies(i):
                copy.wait()
            return carry

        lax.fori_loop(0, total, drain, 0)
        for group in range(GROUPS):
            for copy in cols_copies(group):
                copy.wait()
        for copy in row_copies:
            copy.wait()

    return kernel, total


def weight_grads(h, da, db, x_cols, dy_cols, width):
    count, hidden = h.shape
    depth = x_cols.shape[1]
    chunks = hidden // width
    ring = 4

    def kernel(h_hbm, da_hbm, db_hbm, x_hbm, dy_hbm, dg_hbm, du_hbm, dd_hbm,
               h_in, da_in, db_in, x_in, dy_in, x_t, g_tile, u_tile, d_tile, in_sem, row_sem, out_sem):
        def span(c):
            return pl.ds(pl.multiple_of(c * width, width), width)

        def loads(c):
            return [pltpu.make_async_copy(src.at[:, span(c)], dst.at[c], in_sem.at[k, c])
                    for k, (src, dst) in enumerate(((da_hbm, da_in), (db_hbm, db_in), (h_hbm, h_in)))]

        def stores(c):
            slot = c % ring
            return (pltpu.make_async_copy(g_tile.at[slot], dg_hbm.at[:, span(c)], out_sem.at[0, slot]),
                    pltpu.make_async_copy(u_tile.at[slot], du_hbm.at[:, span(c)], out_sem.at[1, slot]),
                    pltpu.make_async_copy(d_tile.at[slot], dd_hbm.at[span(c)], out_sem.at[2, slot]))

        rows = [pltpu.make_async_copy(src, dst, row_sem.at[k]) for k, (src, dst) in enumerate(((x_hbm, x_in), (dy_hbm, dy_in)))]
        rows[0].start()
        for c in range(chunks):
            for copy in loads(c):
                copy.start()
            if c == 0:
                rows[1].start()
        rows[0].wait()
        x_t[...] = x_in[...].T
        rows[1].wait()

        def step(c, carry):
            slot = c % ring
            for k, value in enumerate(loads(c)):
                value.wait()
            old, new = stores(c - ring), stores(c)
            for k in range(3):
                @pl.when(c >= ring)
                def _(k=k):
                    old[k].wait()
                if k == 0:
                    g_tile[slot] = dot(x_t[...], da_in[c])
                elif k == 1:
                    u_tile[slot] = dot(x_t[...], db_in[c])
                else:
                    d_tile[slot] = dot(h_in[c].T, dy_in[...])
                new[k].start()
            return carry

        lax.fori_loop(0, chunks, step, 0)
        for c in range(chunks - ring, chunks):
            for copy in stores(c):
                copy.wait()

    dma = pltpu.SemaphoreType.DMA
    any_space = pl.BlockSpec(memory_space=pl.ANY)
    return pl.pallas_call(
        kernel,
        out_shape=[jax.ShapeDtypeStruct((depth, hidden), F32), jax.ShapeDtypeStruct((depth, hidden), F32), jax.ShapeDtypeStruct((hidden, depth), F32)],
        in_specs=[any_space] * 5,
        out_specs=[any_space] * 3,
        scratch_shapes=[
            pltpu.VMEM((chunks, count, width), BF16),
            pltpu.VMEM((chunks, count, width), BF16),
            pltpu.VMEM((chunks, count, width), BF16),
            pltpu.VMEM((count, depth), BF16),
            pltpu.VMEM((count, depth), BF16),
            pltpu.VMEM((depth, count), BF16),
            pltpu.VMEM((ring, depth, width), F32),
            pltpu.VMEM((ring, depth, width), F32),
            pltpu.VMEM((ring, width, depth), F32),
            dma((3, chunks)), dma((2,)), dma((3, ring)),
        ],
        compiler_params=pltpu.CompilerParams(vmem_limit_bytes=67043328),
        cost_estimate=pl.CostEstimate(flops=6 * count * depth * hidden, bytes_accessed=12 * depth * hidden, transcendentals=0),
    )(h, da, db, x_cols, dy_cols)


def solution(mesh):
    row_spec = P(None, ("dp", "tp"), None)
    in_specs = (row_spec, P("dp", "tp"), P("dp", "tp"), P("tp", "dp"), row_spec)
    out_specs = (row_spec, row_spec, P("dp", "tp"), P("dp", "tp"), P("tp", "dp"))

    def local_step(x_loc, w_gate_loc, w_up_loc, w_down_loc, dy_loc):
        depth, hidden = w_gate_loc.shape
        micro, local_rows, model = x_loc.shape
        width = 512
        chunks = hidden // width
        kernel, total = make_kernel(chunks, width)
        dma = pltpu.SemaphoreType.DMA
        any_space = pl.BlockSpec(memory_space=pl.ANY)
        hid_shape = jax.ShapeDtypeStruct((GROUPS, SLOTS, 16, hidden), BF16)
        col_shape = jax.ShapeDtypeStruct((GROUPS, SLOTS, 16, depth), BF16)
        row_shape = jax.ShapeDtypeStruct((16, model), BF16)
        outs = pl.pallas_call(
            kernel,
            out_shape=[row_shape, row_shape, hid_shape, hid_shape, hid_shape, col_shape, col_shape],
            in_specs=[any_space] * 5,
            out_specs=[any_space] * 7,
            scratch_shapes=[
                pltpu.VMEM((chunks, depth, width), BF16),
                pltpu.VMEM((chunks, depth, width), BF16),
                pltpu.VMEM((chunks, width, depth), BF16),
                pltpu.VMEM((16, model), BF16),
                pltpu.VMEM((16, model), BF16),
                pltpu.VMEM((GROUPS, 2, SLOTS, 16, depth), BF16),
                pltpu.VMEM((total, SLOTS, 3, 16, width), F32),
                pltpu.VMEM((total, 2, 3, 16, width), F32),
                pltpu.VMEM((total, 3, 16, width), F32),
                pltpu.VMEM((total, 3, SLOTS, 16, width), BF16),
                pltpu.VMEM((GROUPS, 2, SLOTS, 16, depth), F32),
                pltpu.VMEM((GROUPS - 1, 2, SLOTS, 16, depth), F32),
                pltpu.VMEM((2, SLOTS, 16, depth), BF16),
                pltpu.VMEM((2, 16, model), BF16),
                dma((chunks, 3)),
                dma((2, 3)), dma((2, 3)),
                dma((3,)), dma((3,)),
                dma((total,)), dma((total,)),
                dma((total,)), dma((total,)),
                dma((total,)), dma((total,)),
                dma((total,)), dma((total,)),
                dma((total,)), dma((total,)),
                dma((3,)), dma((3,)),
                dma((2, 3)), dma((2, 3)),
                dma((total, 3)), dma((GROUPS, 2)), dma((2,)), dma((2,)),
            ],
            compiler_params=pltpu.CompilerParams(collective_id=0, has_side_effects=True, vmem_limit_bytes=67043328),
        )(x_loc.reshape(micro * local_rows, model), dy_loc.reshape(micro * local_rows, model), w_gate_loc, w_up_loc, w_down_loc)
        y_rows, dx_rows, h_all, da_all, db_all, x_cols, dy_cols = outs
        flat = lambda value: value.reshape(-1, value.shape[-1])
        dw_gate, dw_up, dw_down = weight_grads(flat(h_all), flat(da_all), flat(db_all), flat(x_cols), flat(dy_cols), width)
        return y_rows.reshape(x_loc.shape), dx_rows.reshape(x_loc.shape), dw_gate, dw_up, dw_down

    return jax.shard_map(local_step, mesh=mesh, in_specs=in_specs, out_specs=out_specs, check_vma=False)
```

```python
import jax
import jax.numpy as jnp
from jax import lax
from jax.experimental import pallas as pl
from jax.experimental.pallas import tpu as pltpu
from jax.sharding import PartitionSpec as P

MESH = pl.DeviceIdType.MESH
F32 = jnp.float32
BF16 = jnp.bfloat16
GROUPS = 4
SLOTS = 4
FINAL_LAG = 4
FORWARD_LAG = 12
BACK_LAG = 13
EARLY = 4


def dot(lhs, rhs):
    return lax.dot_general(lhs, rhs, (((1,), (0,)), ((), ())), preferred_element_type=F32)


def dot_t(lhs, rhs):
    return lax.dot_general(lhs, rhs, (((1,), (1,)), ((), ())), preferred_element_type=F32)


def make_kernel(chunks, width):
    total = GROUPS * chunks

    def kernel(x_hbm, dy_hbm, wg_hbm, wu_hbm, wd_hbm,
               rows, hid, cols, x_turned,
               wg, wu, wd, x_ref, dy_ref, part, near, far, acc, acc_in, tail,
               w_sem, first_send, first_recv, spread_send, spread_recv,
               near_send, near_recv, far_send, far_recv,
               hc_send, hc_recv, hx_send, hx_recv, hf_send, hf_recv,
               acc_send, acc_recv, tail_send, tail_recv, in_sem):
        tp = lax.axis_index("tp")
        dp = lax.axis_index("dp")
        z, y = tp // 2, tp % 2
        x, core = dp // 2, dp % 2
        ox, oc = 1 - x, 1 - core
        core_peer = {"tp": tp, "dp": x * 2 + oc}
        x_peer = {"tp": tp, "dp": ox * 2 + core}
        mine = core * 2 + x
        depth = cols.shape[-1]

        def tp_peer(group):
            return {"tp": ((z + group // 2) % 2) * 2 + (y + group % 2) % 2, "dp": dp}

        def chunk_at(s):
            return jnp.where(s < EARLY, s, jnp.where(s < total - chunks + EARLY, s + chunks - EARLY, s + chunks - total))

        def dp_peer(k):
            px, pc = (x + k // 2) % 2, (core + k % 2) % 2
            return px * 2 + pc, pc * 2 + px

        def weight_copies(c):
            span = pl.ds(pl.multiple_of(c * width, width), width)
            return (pltpu.make_async_copy(wg_hbm.at[:, span], wg.at[c], w_sem.at[c, 0]),
                    pltpu.make_async_copy(wu_hbm.at[:, span], wu.at[c], w_sem.at[c, 1]),
                    pltpu.make_async_copy(wd_hbm.at[span], wd.at[c], w_sem.at[c, 2]))

        def remote(src, dst, send, recv, device):
            return pltpu.make_async_remote_copy(src_ref=src, dst_ref=dst, send_sem=send, recv_sem=recv,
                                                device_id=device, device_id_type=MESH)

        def first_copy(kind, k):
            peer, _ = dp_peer(k)
            src = (x_ref, dy_ref)[kind].at[:, pl.ds(pl.multiple_of(peer * depth, depth), depth)]
            return remote(src, cols.at[0, kind, mine], first_send.at[kind, k - 1], first_recv.at[kind, k - 1], {"tp": tp, "dp": peer})

        def spread_copy(group):
            return remote(cols.at[0], cols.at[group], spread_send.at[group - 1], spread_recv.at[group - 1], tp_peer(group))

        def near_copy(i):
            return remote(part.at[i, pl.ds(oc * 2, 2)], near.at[i], near_send.at[i], near_recv.at[i], core_peer)

        def far_copy(i):
            return remote(near.at[i, ox], far.at[i], far_send.at[i], far_recv.at[i], x_peer)

        def hc_copy(i):
            here = hid.at[i, :, mine]
            return remote(here, here, hc_send.at[i], hc_recv.at[i], core_peer)

        def hx_copy(i):
            here = hid.at[i, :, mine]
            return remote(here, here, hx_send.at[i], hx_recv.at[i], x_peer)

        def hf_copy(i):
            there = hid.at[i, :, core * 2 + ox]
            return remote(there, there, hf_send.at[i], hf_recv.at[i], core_peer)

        def acc_copy(group):
            return remote(acc.at[group], acc_in.at[group - 1], acc_send.at[group - 1], acc_recv.at[group - 1], tp_peer(group))

        def tail_copy(kind, k):
            peer, slot = dp_peer(k)
            dst = rows.at[kind, :, pl.ds(pl.multiple_of(dp * depth, depth), depth)]
            return remote(tail.at[kind, slot], dst, tail_send.at[kind, k - 1], tail_recv.at[kind, k - 1], {"tp": tp, "dp": peer})

        row_loads = [pltpu.make_async_copy(src, dst, in_sem.at[k]) for k, (src, dst) in enumerate(((x_hbm, x_ref), (dy_hbm, dy_ref)))]
        for copy in row_loads:
            copy.start()
        for c in range(chunks):
            for copy in weight_copies(c):
                copy.start()

        barrier = pltpu.get_barrier_semaphore()
        for k in range(1, 4):
            pl.semaphore_signal(barrier, inc=1, device_id={"tp": tp, "dp": dp_peer(k)[0]}, device_id_type=MESH)
            pl.semaphore_signal(barrier, inc=1, device_id=tp_peer(k), device_id_type=MESH)
        for copy in row_loads:
            copy.wait()
        pl.semaphore_wait(barrier, 6)

        for k in (2, 3, 1):
            for kind in range(2):
                first_copy(kind, k).start()
        own = pl.ds(pl.multiple_of(dp * depth, depth), depth)
        cols[0, 0, mine] = x_ref[:, own]
        cols[0, 1, mine] = dy_ref[:, own]
        acc[...] = jnp.zeros_like(acc)
        for k in (1, 2, 3):
            for kind in range(2):
                first_copy(kind, k).wait_recv()
        for group in (1, 2, 3):
            spread_copy(group).start()

        def products(i):
            group, c = i // chunks, i % chunks

            @pl.when(group == jnp.where(c < EARLY, 0, 1))
            def _():
                for copy in weight_copies(c):
                    copy.wait()

            @pl.when(jnp.logical_and(group > 0, c == 0))
            def _():
                spread_copy(group).wait_recv()

            x_rows = cols[group, 0].reshape(SLOTS * 16, depth)
            dy_rows = cols[group, 1].reshape(SLOTS * 16, depth)
            for k, value in enumerate((dot(x_rows, wg[c]), dot(x_rows, wu[c]), dot_t(dy_rows, wd[c]))):
                for slot in range(SLOTS):
                    part[i, slot, k] = value[slot * 16:(slot + 1) * 16]
            near_copy(i).start()

        def half_sum(i):
            near_copy(i).wait_recv()
            near[i, ox] = near[i, ox] + part[i, core * 2 + ox]
            far_copy(i).start()

        def activations(i):
            far_copy(i).wait_recv()
            gate = part[i, mine, 0] + near[i, x, 0] + far[i, 0]
            up = part[i, mine, 1] + near[i, x, 1] + far[i, 1]
            grad = part[i, mine, 2] + near[i, x, 2] + far[i, 2]
            sig = jax.nn.sigmoid(gate)
            act = gate * sig
            hid[i, 0, mine] = (act * up).astype(BF16)
            hid[i, 1, mine] = (grad * up * sig * (1.0 + gate * (1.0 - sig))).astype(BF16)
            hid[i, 2, mine] = (grad * act).astype(BF16)
            hc_copy(i).start()

        def back(i):
            group, c = i // chunks, i % chunks
            hc_copy(i).wait_recv()
            hf_copy(i).wait_recv()
            h_rows = hid[i, 0].reshape(SLOTS * 16, width)
            da_rows = hid[i, 1].reshape(SLOTS * 16, width)
            db_rows = hid[i, 2].reshape(SLOTS * 16, width)
            acc[group, 0] += dot(h_rows, wd[c]).reshape(SLOTS, 16, depth)
            acc[group, 1] += (dot_t(da_rows, wg[c]) + dot_t(db_rows, wu[c])).reshape(SLOTS, 16, depth)

            @pl.when(jnp.logical_and(group > 0, c == chunks - 1))
            def _():
                acc_copy(group).start()

        def step(s, carry):
            @pl.when(s < total)
            def _():
                products(chunk_at(s))

            @pl.when(jnp.logical_and(s >= 1, s < total + 1))
            def _():
                half_sum(chunk_at(s - 1))

            @pl.when(jnp.logical_and(s >= FINAL_LAG, s < total + FINAL_LAG))
            def _():
                activations(chunk_at(s - FINAL_LAG))

            @pl.when(jnp.logical_and(s >= EARLY + FINAL_LAG, s < total - chunks + EARLY + FINAL_LAG))
            def _():
                hx_copy(s - FINAL_LAG + chunks - EARLY).start()

            @pl.when(jnp.logical_and(s >= total, s < total + chunks))
            def _():
                hx_copy(s - total).start()

            @pl.when(jnp.logical_and(s >= FORWARD_LAG, s < FORWARD_LAG + total))
            def _():
                i = (s - FORWARD_LAG + chunks) % total
                hx_copy(i).wait_recv()
                hf_copy(i).start()

            @pl.when(s == total + FINAL_LAG)
            def _():
                x_turned[...] = cols[:, 0].reshape(GROUPS * SLOTS * 16, depth).T

            @pl.when(s >= BACK_LAG)
            def _():
                back((s - BACK_LAG + chunks) % total)

            return carry

        lax.fori_loop(0, total + BACK_LAG, step, 0)

        for group in (1, 2, 3):
            acc_copy(group).wait_recv()
        for kind in range(2):
            value = acc[0, kind] + acc_in[0, kind] + acc_in[1, kind] + acc_in[2, kind]
            tail[kind] = (cols[0, kind].astype(F32) + value).astype(BF16)
        for k in (2, 3, 1):
            for kind in range(2):
                tail_copy(kind, k).start()
        for kind in range(2):
            rows[kind, :, own] = tail[kind, mine]
        for k in (1, 2, 3):
            for kind in range(2):
                tail_copy(kind, k).wait_recv()
        for k in (1, 2, 3):
            for kind in range(2):
                first_copy(kind, k).wait_send()
                tail_copy(kind, k).wait_send()
            spread_copy(k).wait_send()
            acc_copy(k).wait_send()

        def drain(i, carry):
            near_copy(i).wait_send()
            far_copy(i).wait_send()
            hc_copy(i).wait_send()
            hx_copy(i).wait_send()
            hf_copy(i).wait_send()
            return carry

        lax.fori_loop(0, total, drain, 0)

    return kernel, total


def finish(rows, hid, cols, x_turned):
    _, local_rows, model = rows.shape
    total, _, _, _, width = hid.shape
    depth, count = x_turned.shape
    chunks = total // GROUPS
    hidden = chunks * width
    ring = 4

    def kernel(rows_ref, hid_ref, cols_ref, x_ref, y_hbm, dx_hbm, dg_hbm, du_hbm, dd_hbm, g_tile, u_tile, d_tile, row_sem, out_sem):
        row_copies = [pltpu.make_async_copy(rows_ref.at[k], dst, row_sem.at[k]) for k, dst in enumerate((y_hbm, dx_hbm))]

        def all_rows(c, k):
            return jnp.concatenate([hid_ref[group * chunks + c, k].reshape(SLOTS * 16, width) for group in range(GROUPS)])

        def stores(c):
            slot = c % ring
            span = pl.ds(pl.multiple_of(c * width, width), width)
            return (pltpu.make_async_copy(g_tile.at[slot], dg_hbm.at[:, span], out_sem.at[0, slot]),
                    pltpu.make_async_copy(u_tile.at[slot], du_hbm.at[:, span], out_sem.at[1, slot]),
                    pltpu.make_async_copy(d_tile.at[slot], dd_hbm.at[span], out_sem.at[2, slot]))

        def step(c, carry):
            slot = c % ring
            old, new = stores(c - ring), stores(c)
            for k in range(3):
                @pl.when(c >= ring)
                def _(k=k):
                    old[k].wait()
                if k == 0:
                    g_tile[slot] = dot(x_ref[...], all_rows(c, 1))
                elif k == 1:
                    u_tile[slot] = dot(x_ref[...], all_rows(c, 2))
                else:
                    d_tile[slot] = dot(all_rows(c, 0).T, cols_ref[:, 1].reshape(count, depth))
                new[k].start()
            return carry

        lax.fori_loop(0, chunks, step, 0)
        for copy in row_copies:
            copy.start()
        for c in range(chunks - ring, chunks):
            for copy in stores(c):
                copy.wait()
        for copy in row_copies:
            copy.wait()

    dma = pltpu.SemaphoreType.DMA
    any_space = pl.BlockSpec(memory_space=pl.ANY)
    vmem = pl.BlockSpec(memory_space=pltpu.VMEM)
    row_shape = jax.ShapeDtypeStruct((local_rows, model), BF16)
    held = [pltpu.with_memory_space_constraint(value, pltpu.VMEM) for value in (rows, hid, cols, x_turned)]
    return pl.pallas_call(
        kernel,
        out_shape=[row_shape, row_shape, jax.ShapeDtypeStruct((depth, hidden), F32), jax.ShapeDtypeStruct((depth, hidden), F32), jax.ShapeDtypeStruct((hidden, depth), F32)],
        in_specs=[vmem] * 4,
        out_specs=[any_space] * 5,
        scratch_shapes=[
            pltpu.VMEM((ring, depth, width), F32),
            pltpu.VMEM((ring, depth, width), F32),
            pltpu.VMEM((ring, width, depth), F32),
            dma((2,)), dma((3, ring)),
        ],
        compiler_params=pltpu.CompilerParams(vmem_limit_bytes=40 * 2**20),
        cost_estimate=pl.CostEstimate(flops=6 * count * depth * hidden, bytes_accessed=12 * depth * hidden, transcendentals=0),
    )(*held)


def solution(mesh):
    row_spec = P(None, ("dp", "tp"), None)
    in_specs = (row_spec, P("dp", "tp"), P("dp", "tp"), P("tp", "dp"), row_spec)
    out_specs = (row_spec, row_spec, P("dp", "tp"), P("dp", "tp"), P("tp", "dp"))

    def local_step(x_loc, w_gate_loc, w_up_loc, w_down_loc, dy_loc):
        depth, hidden = w_gate_loc.shape
        micro, local_rows, model = x_loc.shape
        width = 512
        chunks = hidden // width
        kernel, total = make_kernel(chunks, width)
        dma = pltpu.SemaphoreType.DMA
        any_space = pl.BlockSpec(memory_space=pl.ANY)
        vmem = pl.BlockSpec(memory_space=pltpu.VMEM)
        outs = pl.pallas_call(
            kernel,
            out_shape=[
                pltpu.VMEM((2, micro * local_rows, model), BF16),
                pltpu.VMEM((total, 3, SLOTS, 16, width), BF16),
                pltpu.VMEM((GROUPS, 2, SLOTS, 16, depth), BF16),
                pltpu.VMEM((depth, GROUPS * SLOTS * 16), BF16),
            ],
            in_specs=[any_space] * 5,
            out_specs=[vmem] * 4,
            scratch_shapes=[
                pltpu.VMEM((chunks, depth, width), BF16),
                pltpu.VMEM((chunks, depth, width), BF16),
                pltpu.VMEM((chunks, width, depth), BF16),
                pltpu.VMEM((16, model), BF16),
                pltpu.VMEM((16, model), BF16),
                pltpu.VMEM((total, SLOTS, 3, 16, width), F32),
                pltpu.VMEM((total, 2, 3, 16, width), F32),
                pltpu.VMEM((total, 3, 16, width), F32),
                pltpu.VMEM((GROUPS, 2, SLOTS, 16, depth), F32),
                pltpu.VMEM((GROUPS - 1, 2, SLOTS, 16, depth), F32),
                pltpu.VMEM((2, SLOTS, 16, depth), BF16),
                dma((chunks, 3)),
                dma((2, 3)), dma((2, 3)),
                dma((3,)), dma((3,)),
                dma((total,)), dma((total,)),
                dma((total,)), dma((total,)),
                dma((total,)), dma((total,)),
                dma((total,)), dma((total,)),
                dma((total,)), dma((total,)),
                dma((3,)), dma((3,)),
                dma((2, 3)), dma((2, 3)),
                dma((2,)),
            ],
            compiler_params=pltpu.CompilerParams(collective_id=0, has_side_effects=True, vmem_limit_bytes=53 * 2**20),
        )(x_loc.reshape(micro * local_rows, model), dy_loc.reshape(micro * local_rows, model), w_gate_loc, w_up_loc, w_down_loc)
        y_rows, dx_rows, dw_gate, dw_up, dw_down = finish(*outs)
        return y_rows.reshape(x_loc.shape), dx_rows.reshape(x_loc.shape), dw_gate, dw_up, dw_down

    return jax.shard_map(local_step, mesh=mesh, in_specs=in_specs, out_specs=out_specs, check_vma=False)
```

```python
import jax
import jax.numpy as jnp
from jax import lax
from jax.experimental import pallas as pl
from jax.experimental.pallas import tpu as pltpu
from jax.sharding import PartitionSpec as P

MESH = pl.DeviceIdType.MESH
F32 = jnp.float32
BF16 = jnp.bfloat16
GROUPS = 4
SLOTS = 4
FINAL_LAG = 3
FORWARD_LAG = 9
BACK_LAG = 10
EARLY = 4


def dot(lhs, rhs):
    return lax.dot_general(lhs, rhs, (((1,), (0,)), ((), ())), preferred_element_type=F32)


def dot_t(lhs, rhs):
    return lax.dot_general(lhs, rhs, (((1,), (1,)), ((), ())), preferred_element_type=F32)


def make_kernel(chunks, width):
    total = GROUPS * chunks

    def kernel(x_hbm, dy_hbm, wg_hbm, wu_hbm, wd_hbm,
               rows, hid, cols, x_turned,
               wg, wu, wd, x_ref, dy_ref, part, near, far, acc, acc_in, tail,
               w_sem, first_send, first_recv, spread_send, spread_recv,
               near_send, near_recv, far_send, far_recv,
               hc_send, hc_recv, hx_send, hx_recv, hf_send, hf_recv,
               acc_send, acc_recv, tail_send, tail_recv, in_sem, open_send, open_recv):
        tp = lax.axis_index("tp")
        dp = lax.axis_index("dp")
        z, y = tp // 2, tp % 2
        x, core = dp // 2, dp % 2
        ox, oc = 1 - x, 1 - core
        core_peer = {"tp": tp, "dp": x * 2 + oc}
        x_peer = {"tp": tp, "dp": ox * 2 + core}
        mine = core * 2 + x
        depth = cols.shape[-1]

        def tp_peer(group):
            return {"tp": ((z + group // 2) % 2) * 2 + (y + group % 2) % 2, "dp": dp}

        def chunk_at(s):
            return jnp.where(s < EARLY, s, jnp.where(s < total - chunks + EARLY, s + chunks - EARLY, s + chunks - total))

        def dp_peer(k):
            px, pc = (x + k // 2) % 2, (core + k % 2) % 2
            return px * 2 + pc, pc * 2 + px

        def weight_copies(c):
            span = pl.ds(pl.multiple_of(c * width, width), width)
            return (pltpu.make_async_copy(wg_hbm.at[:, span], wg.at[c], w_sem.at[c, 0]),
                    pltpu.make_async_copy(wu_hbm.at[:, span], wu.at[c], w_sem.at[c, 1]),
                    pltpu.make_async_copy(wd_hbm.at[span], wd.at[c], w_sem.at[c, 2]))

        def remote(src, dst, send, recv, device):
            return pltpu.make_async_remote_copy(src_ref=src, dst_ref=dst, send_sem=send, recv_sem=recv,
                                                device_id=device, device_id_type=MESH)

        def first_copy(kind, k):
            peer, _ = dp_peer(k)
            src = (x_ref, dy_ref)[kind].at[:, pl.ds(pl.multiple_of(peer * depth, depth), depth)]
            return remote(src, cols.at[0, kind, mine], first_send.at[kind, k - 1], first_recv.at[kind, k - 1], {"tp": tp, "dp": peer})

        def spread_copy(group):
            return remote(cols.at[0], cols.at[group], spread_send.at[group - 1], spread_recv.at[group - 1], tp_peer(group))

        def near_copy(i):
            return remote(part.at[i, pl.ds(oc * 2, 2)], near.at[i], near_send.at[i], near_recv.at[i], core_peer)

        def open_copy(k):
            kinds = pl.ds(2 * k, 2 - k)
            return remote(part.at[0, pl.ds(oc * 2, 2), kinds], near.at[0, :, kinds], open_send.at[k], open_recv.at[k], core_peer)

        def open_far_copy(k):
            kinds = pl.ds(2 * k, 2 - k)
            return remote(near.at[0, ox, kinds], far.at[0, kinds], far_send.at[0], far_recv.at[0], x_peer)

        def far_copy(i):
            return remote(near.at[i, ox], far.at[i], far_send.at[i], far_recv.at[i], x_peer)

        def hc_copy(i):
            here = hid.at[i, :, mine]
            return remote(here, here, hc_send.at[i], hc_recv.at[i], core_peer)

        def hx_copy(i):
            here = hid.at[i, :, mine]
            return remote(here, here, hx_send.at[i], hx_recv.at[i], x_peer)

        def hf_copy(i):
            there = hid.at[i, :, core * 2 + ox]
            return remote(there, there, hf_send.at[i], hf_recv.at[i], core_peer)

        def acc_copy(group):
            return remote(acc.at[group], acc_in.at[group - 1], acc_send.at[group - 1], acc_recv.at[group - 1], tp_peer(group))

        def tail_copy(kind, k):
            peer, slot = dp_peer(k)
            dst = rows.at[kind, :, pl.ds(pl.multiple_of(dp * depth, depth), depth)]
            return remote(tail.at[kind, slot], dst, tail_send.at[kind, k - 1], tail_recv.at[kind, k - 1], {"tp": tp, "dp": peer})

        row_loads = [pltpu.make_async_copy(src, dst, in_sem.at[k]) for k, (src, dst) in enumerate(((x_hbm, x_ref), (dy_hbm, dy_ref)))]
        for copy in row_loads:
            copy.start()
        for c in range(chunks):
            for copy in weight_copies(c):
                copy.start()

        barrier = pltpu.get_barrier_semaphore()
        for k in range(1, 4):
            pl.semaphore_signal(barrier, inc=1, device_id={"tp": tp, "dp": dp_peer(k)[0]}, device_id_type=MESH)
            pl.semaphore_signal(barrier, inc=1, device_id=tp_peer(k), device_id_type=MESH)
        for copy in row_loads:
            copy.wait()
        pl.semaphore_wait(barrier, 6)

        for kind in range(2):
            for k in (2, 3, 1):
                first_copy(kind, k).start()
        own = pl.ds(pl.multiple_of(dp * depth, depth), depth)
        cols[0, 0, mine] = x_ref[:, own]
        cols[0, 1, mine] = dy_ref[:, own]
        acc[...] = jnp.zeros_like(acc)
        for copy in weight_copies(0):
            copy.wait()
        for kind in range(2):
            for k in (1, 2, 3):
                first_copy(kind, k).wait_recv()
            rows_in = cols[0, kind].reshape(SLOTS * 16, depth)
            for k in ((0, 1), (2,))[kind]:
                value = dot_t(rows_in, wd[0]) if kind else dot(rows_in, (wg, wu)[k][0])
                for slot in range(SLOTS):
                    part[0, slot, k] = value[slot * 16:(slot + 1) * 16]
            open_copy(kind).start()
        spread_copy(1).start()
        for k in range(2):
            open_copy(k).wait_recv()
            kinds = pl.ds(2 * k, 2 - k)
            near[0, ox, kinds] = near[0, ox, kinds] + part[0, core * 2 + ox, kinds]
            open_far_copy(k).start()

        def products(i):
            group, c = i // chunks, i % chunks

            @pl.when(jnp.logical_and(i > 0, group == jnp.where(c < EARLY, 0, 1)))
            def _():
                for copy in weight_copies(c):
                    copy.wait()

            @pl.when(jnp.logical_and(group > 0, c == 0))
            def _():
                spread_copy(group).wait_recv()

            x_rows = cols[group, 0].reshape(SLOTS * 16, depth)
            dy_rows = cols[group, 1].reshape(SLOTS * 16, depth)
            for k, value in enumerate((dot(x_rows, wg[c]), dot(x_rows, wu[c]), dot_t(dy_rows, wd[c]))):
                for slot in range(SLOTS):
                    part[i, slot, k] = value[slot * 16:(slot + 1) * 16]
            near_copy(i).start()

        def half_sum(i):
            near_copy(i).wait_recv()
            near[i, ox] = near[i, ox] + part[i, core * 2 + ox]
            far_copy(i).start()

        def activations(i):
            far_copy(i).wait_recv()
            gate = part[i, mine, 0] + near[i, x, 0] + far[i, 0]
            up = part[i, mine, 1] + near[i, x, 1] + far[i, 1]
            grad = part[i, mine, 2] + near[i, x, 2] + far[i, 2]
            sig = jax.nn.sigmoid(gate)
            act = gate * sig
            hid[i, 0, mine] = (act * up).astype(BF16)
            hid[i, 1, mine] = (grad * up * sig * (1.0 + gate * (1.0 - sig))).astype(BF16)
            hid[i, 2, mine] = (grad * act).astype(BF16)
            hc_copy(i).start()

        def back(i):
            group, c = i // chunks, i % chunks
            hc_copy(i).wait_recv()
            hf_copy(i).wait_recv()
            h_rows = hid[i, 0].reshape(SLOTS * 16, width)
            da_rows = hid[i, 1].reshape(SLOTS * 16, width)
            db_rows = hid[i, 2].reshape(SLOTS * 16, width)
            acc[group, 0] += dot(h_rows, wd[c]).reshape(SLOTS, 16, depth)
            acc[group, 1] += (dot_t(da_rows, wg[c]) + dot_t(db_rows, wu[c])).reshape(SLOTS, 16, depth)

            @pl.when(jnp.logical_and(group > 0, c == chunks - 1))
            def _():
                acc_copy(group).start()

        def step(s, carry):
            @pl.when(s == EARLY)
            def _():
                half_sum(EARLY - 1)

            @pl.when(s < total)
            def _():
                products(chunk_at(s))

            @pl.when(s == EARLY)
            def _():
                spread_copy(2).start()

            @pl.when(s == EARLY + 3)
            def _():
                spread_copy(3).start()

            @pl.when(jnp.logical_and(jnp.logical_and(s >= 2, s < total + 1), s != EARLY))
            def _():
                half_sum(chunk_at(s - 1))

            @pl.when(jnp.logical_and(s >= FINAL_LAG, s < total + FINAL_LAG))
            def _():
                activations(chunk_at(s - FINAL_LAG))

            @pl.when(jnp.logical_and(s >= EARLY + FINAL_LAG, s < total - chunks + EARLY + FINAL_LAG))
            def _():
                hx_copy(s - FINAL_LAG + chunks - EARLY).start()

            @pl.when(jnp.logical_and(s >= total, s < total + chunks))
            def _():
                hx_copy(s - total).start()

            @pl.when(jnp.logical_and(s >= FORWARD_LAG, s < FORWARD_LAG + total))
            def _():
                i = (s - FORWARD_LAG + chunks) % total
                hx_copy(i).wait_recv()
                hf_copy(i).start()

            @pl.when(s == total + FINAL_LAG)
            def _():
                x_turned[...] = cols[:, 0].reshape(GROUPS * SLOTS * 16, depth).T

            @pl.when(s >= BACK_LAG)
            def _():
                back((s - BACK_LAG + chunks) % total)

            return carry

        lax.fori_loop(1, total + BACK_LAG, step, 0)

        for group in (1, 2, 3):
            acc_copy(group).wait_recv()
        for kind in range(2):
            value = acc[0, kind] + acc_in[0, kind] + acc_in[1, kind] + acc_in[2, kind]
            tail[kind] = (cols[0, kind].astype(F32) + value).astype(BF16)
        for k in (2, 3, 1):
            for kind in range(2):
                tail_copy(kind, k).start()
        for kind in range(2):
            rows[kind, :, own] = tail[kind, mine]
        for k in (1, 2, 3):
            for kind in range(2):
                tail_copy(kind, k).wait_recv()
        for k in (1, 2, 3):
            for kind in range(2):
                first_copy(kind, k).wait_send()
                tail_copy(kind, k).wait_send()
            spread_copy(k).wait_send()
            acc_copy(k).wait_send()

        for k in range(2):
            open_copy(k).wait_send()

        def drain(i, carry):
            @pl.when(i > 0)
            def _():
                near_copy(i).wait_send()

            far_copy(i).wait_send()
            hc_copy(i).wait_send()
            hx_copy(i).wait_send()
            hf_copy(i).wait_send()
            return carry

        lax.fori_loop(0, total, drain, 0)

    return kernel, total


def finish(rows, hid, cols, x_turned):
    _, local_rows, model = rows.shape
    total, _, _, _, width = hid.shape
    depth, count = x_turned.shape
    chunks = total // GROUPS
    hidden = chunks * width
    ring = 4

    def kernel(rows_ref, hid_ref, cols_ref, x_ref, y_hbm, dx_hbm, dg_hbm, du_hbm, dd_hbm, g_tile, u_tile, d_tile, row_sem, out_sem):
        row_copies = [pltpu.make_async_copy(rows_ref.at[k], dst, row_sem.at[k]) for k, dst in enumerate((y_hbm, dx_hbm))]

        def all_rows(c, k):
            return jnp.concatenate([hid_ref[group * chunks + c, k].reshape(SLOTS * 16, width) for group in range(GROUPS)])

        def stores(c):
            slot = c % ring
            span = pl.ds(pl.multiple_of(c * width, width), width)
            return (pltpu.make_async_copy(g_tile.at[slot], dg_hbm.at[:, span], out_sem.at[0, slot]),
                    pltpu.make_async_copy(u_tile.at[slot], du_hbm.at[:, span], out_sem.at[1, slot]),
                    pltpu.make_async_copy(d_tile.at[slot], dd_hbm.at[span], out_sem.at[2, slot]))

        def step(c, carry):
            slot = c % ring
            old, new = stores(c - ring), stores(c)
            for k in range(3):
                @pl.when(c >= ring)
                def _(k=k):
                    old[k].wait()
                if k == 0:
                    g_tile[slot] = dot(x_ref[...], all_rows(c, 1))
                elif k == 1:
                    u_tile[slot] = dot(x_ref[...], all_rows(c, 2))
                else:
                    d_tile[slot] = dot(all_rows(c, 0).T, cols_ref[:, 1].reshape(count, depth))
                new[k].start()
            return carry

        lax.fori_loop(0, chunks, step, 0)
        for copy in row_copies:
            copy.start()
        for c in range(chunks - ring, chunks):
            for copy in stores(c):
                copy.wait()
        for copy in row_copies:
            copy.wait()

    dma = pltpu.SemaphoreType.DMA
    any_space = pl.BlockSpec(memory_space=pl.ANY)
    vmem = pl.BlockSpec(memory_space=pltpu.VMEM)
    row_shape = jax.ShapeDtypeStruct((local_rows, model), BF16)
    held = [pltpu.with_memory_space_constraint(value, pltpu.VMEM) for value in (rows, hid, cols, x_turned)]
    return pl.pallas_call(
        kernel,
        out_shape=[row_shape, row_shape, jax.ShapeDtypeStruct((depth, hidden), F32), jax.ShapeDtypeStruct((depth, hidden), F32), jax.ShapeDtypeStruct((hidden, depth), F32)],
        in_specs=[vmem] * 4,
        out_specs=[any_space] * 5,
        scratch_shapes=[
            pltpu.VMEM((ring, depth, width), F32),
            pltpu.VMEM((ring, depth, width), F32),
            pltpu.VMEM((ring, width, depth), F32),
            dma((2,)), dma((3, ring)),
        ],
        compiler_params=pltpu.CompilerParams(vmem_limit_bytes=40 * 2**20),
        cost_estimate=pl.CostEstimate(flops=6 * count * depth * hidden, bytes_accessed=12 * depth * hidden, transcendentals=0),
    )(*held)


def solution(mesh):
    row_spec = P(None, ("dp", "tp"), None)
    in_specs = (row_spec, P("dp", "tp"), P("dp", "tp"), P("tp", "dp"), row_spec)
    out_specs = (row_spec, row_spec, P("dp", "tp"), P("dp", "tp"), P("tp", "dp"))

    def local_step(x_loc, w_gate_loc, w_up_loc, w_down_loc, dy_loc):
        depth, hidden = w_gate_loc.shape
        micro, local_rows, model = x_loc.shape
        width = 512
        chunks = hidden // width
        kernel, total = make_kernel(chunks, width)
        dma = pltpu.SemaphoreType.DMA
        any_space = pl.BlockSpec(memory_space=pl.ANY)
        vmem = pl.BlockSpec(memory_space=pltpu.VMEM)
        outs = pl.pallas_call(
            kernel,
            out_shape=[
                pltpu.VMEM((2, micro * local_rows, model), BF16),
                pltpu.VMEM((total, 3, SLOTS, 16, width), BF16),
                pltpu.VMEM((GROUPS, 2, SLOTS, 16, depth), BF16),
                pltpu.VMEM((depth, GROUPS * SLOTS * 16), BF16),
            ],
            in_specs=[any_space] * 5,
            out_specs=[vmem] * 4,
            scratch_shapes=[
                pltpu.VMEM((chunks, depth, width), BF16),
                pltpu.VMEM((chunks, depth, width), BF16),
                pltpu.VMEM((chunks, width, depth), BF16),
                pltpu.VMEM((16, model), BF16),
                pltpu.VMEM((16, model), BF16),
                pltpu.VMEM((total, SLOTS, 3, 16, width), F32),
                pltpu.VMEM((total, 2, 3, 16, width), F32),
                pltpu.VMEM((total, 3, 16, width), F32),
                pltpu.VMEM((GROUPS, 2, SLOTS, 16, depth), F32),
                pltpu.VMEM((GROUPS - 1, 2, SLOTS, 16, depth), F32),
                pltpu.VMEM((2, SLOTS, 16, depth), BF16),
                dma((chunks, 3)),
                dma((2, 3)), dma((2, 3)),
                dma((3,)), dma((3,)),
                dma((total,)), dma((total,)),
                dma((total,)), dma((total,)),
                dma((total,)), dma((total,)),
                dma((total,)), dma((total,)),
                dma((total,)), dma((total,)),
                dma((3,)), dma((3,)),
                dma((2, 3)), dma((2, 3)),
                dma((2,)), dma((2,)), dma((2,)),
            ],
            compiler_params=pltpu.CompilerParams(collective_id=0, has_side_effects=True, vmem_limit_bytes=53 * 2**20),
        )(x_loc.reshape(micro * local_rows, model), dy_loc.reshape(micro * local_rows, model), w_gate_loc, w_up_loc, w_down_loc)
        y_rows, dx_rows, dw_gate, dw_up, dw_down = finish(*outs)
        return y_rows.reshape(x_loc.shape), dx_rows.reshape(x_loc.shape), dw_gate, dw_up, dw_down

    return jax.shard_map(local_step, mesh=mesh, in_specs=in_specs, out_specs=out_specs, check_vma=False)
```

```python
import jax
import jax.numpy as jnp
from jax import lax
from jax.experimental import pallas as pl
from jax.experimental.pallas import tpu as pltpu
from jax.sharding import PartitionSpec as P

MESH = pl.DeviceIdType.MESH
F32 = jnp.float32
BF16 = jnp.bfloat16
GROUPS = 4
SLOTS = 4
FINAL_LAG = 4
FORWARD_LAG = 10
BACK_LAG = 11
EARLY = 3


def dot(lhs, rhs):
    return lax.dot_general(lhs, rhs, (((1,), (0,)), ((), ())), preferred_element_type=F32)


def dot_t(lhs, rhs):
    return lax.dot_general(lhs, rhs, (((1,), (1,)), ((), ())), preferred_element_type=F32)


def make_kernel(chunks, width):
    total = GROUPS * chunks

    def kernel(x_hbm, dy_hbm, wg_hbm, wu_hbm, wd_hbm,
               rows, hid, cols, x_turned,
               wg, wu, wd, x_ref, dy_ref, part, near, far, acc, acc_in, tail,
               w_sem, first_send, first_recv, spread_send, spread_recv,
               near_send, near_recv, far_send, far_recv,
               hc_send, hc_recv, hx_send, hx_recv, hf_send, hf_recv,
               acc_send, acc_recv, tail_send, tail_recv, in_sem, open_send, open_recv):
        tp = lax.axis_index("tp")
        dp = lax.axis_index("dp")
        z, y = tp // 2, tp % 2
        x, core = dp // 2, dp % 2
        ox, oc = 1 - x, 1 - core
        core_peer = {"tp": tp, "dp": x * 2 + oc}
        x_peer = {"tp": tp, "dp": ox * 2 + core}
        mine = core * 2 + x
        depth = cols.shape[-1]

        tp_peers = [{"tp": pz * 2 + py, "dp": dp} for pz, py in ((z, 1 - y), (1 - z, y), (1 - z, 1 - y))]
        rows_of = (pl.ds(0, 8), pl.ds(8, 8))

        def chunk_at(s):
            return jnp.where(s < EARLY, s, jnp.where(s < total - chunks + EARLY, s + chunks - EARLY, s + chunks - total))

        def dp_peer(k):
            px, pc = (x + k // 2) % 2, (core + k % 2) % 2
            return px * 2 + pc, pc * 2 + px

        def weight_copies(c):
            span = pl.ds(pl.multiple_of(c * width, width), width)
            return (pltpu.make_async_copy(wg_hbm.at[:, span], wg.at[c], w_sem.at[c, 0]),
                    pltpu.make_async_copy(wu_hbm.at[:, span], wu.at[c], w_sem.at[c, 1]),
                    pltpu.make_async_copy(wd_hbm.at[span], wd.at[c], w_sem.at[c, 2]))

        def remote(src, dst, send, recv, device):
            return pltpu.make_async_remote_copy(src_ref=src, dst_ref=dst, send_sem=send, recv_sem=recv,
                                                device_id=device, device_id_type=MESH)

        def first_copy(kind, k):
            peer, _ = dp_peer(k)
            src = (x_ref, dy_ref)[kind].at[:, pl.ds(pl.multiple_of(peer * depth, depth), depth)]
            return remote(src, cols.at[0, kind, mine], first_send.at[kind, k - 1], first_recv.at[kind, k - 1], {"tp": tp, "dp": peer})

        def spread_copies(group, kind):
            if group == 2:
                return [remote(cols.at[0, kind], cols.at[2, kind], spread_send.at[1, kind, 0], spread_recv.at[1, kind, 0], tp_peers[2])]
            return [remote(cols.at[0, kind, :, rows_of[group // 2]], cols.at[group, kind, :, rows_of[way]],
                           spread_send.at[group - 1, kind, way], spread_recv.at[group - 1, kind, way], tp_peers[way]) for way in range(2)]

        def near_copy(i):
            return remote(part.at[i, pl.ds(oc * 2, 2)], near.at[i], near_send.at[i], near_recv.at[i], core_peer)

        def open_copy(k):
            kinds = pl.ds(2 * k, 2 - k)
            return remote(part.at[0, pl.ds(oc * 2, 2), kinds], near.at[0, :, kinds], open_send.at[k], open_recv.at[k], core_peer)

        def open_far_copy(k):
            kinds = pl.ds(2 * k, 2 - k)
            return remote(near.at[0, ox, kinds], far.at[0, kinds], far_send.at[0], far_recv.at[0], x_peer)

        def far_copy(i):
            return remote(near.at[i, ox], far.at[i], far_send.at[i], far_recv.at[i], x_peer)

        def hc_copy(i):
            here = hid.at[i, :, mine]
            return remote(here, here, hc_send.at[i], hc_recv.at[i], core_peer)

        def hx_copy(i):
            here = hid.at[i, :, mine]
            return remote(here, here, hx_send.at[i], hx_recv.at[i], x_peer)

        def hf_copy(i):
            there = hid.at[i, :, core * 2 + ox]
            return remote(there, there, hf_send.at[i], hf_recv.at[i], core_peer)

        def acc_copies(group):
            if group == 2:
                return [remote(acc.at[2], acc_in.at[2], acc_send.at[1, 0], acc_recv.at[1, 0], tp_peers[2])]
            return [remote(acc.at[group, :, :, rows_of[way]], acc_in.at[way, :, :, rows_of[group // 2]],
                           acc_send.at[group - 1, way], acc_recv.at[group - 1, way], tp_peers[way]) for way in range(2)]

        def tail_copy(kind, k):
            peer, slot = dp_peer(k)
            dst = rows.at[kind, :, pl.ds(pl.multiple_of(dp * depth, depth), depth)]
            return remote(tail.at[kind, slot], dst, tail_send.at[kind, k - 1], tail_recv.at[kind, k - 1], {"tp": tp, "dp": peer})

        row_loads = [pltpu.make_async_copy(src, dst, in_sem.at[k]) for k, (src, dst) in enumerate(((x_hbm, x_ref), (dy_hbm, dy_ref)))]
        for copy in row_loads:
            copy.start()
        for c in range(chunks):
            for copy in weight_copies(c):
                copy.start()

        barrier = pltpu.get_barrier_semaphore()
        for k in range(1, 4):
            pl.semaphore_signal(barrier, inc=1, device_id={"tp": tp, "dp": dp_peer(k)[0]}, device_id_type=MESH)
            pl.semaphore_signal(barrier, inc=1, device_id=tp_peers[k - 1], device_id_type=MESH)
        for copy in row_loads:
            copy.wait()
        pl.semaphore_wait(barrier, 6)

        for kind in range(2):
            for k in (2, 3, 1):
                first_copy(kind, k).start()
        own = pl.ds(pl.multiple_of(dp * depth, depth), depth)
        cols[0, 0, mine] = x_ref[:, own]
        cols[0, 1, mine] = dy_ref[:, own]
        acc[...] = jnp.zeros_like(acc)
        for copy in weight_copies(0):
            copy.wait()
        for kind in range(2):
            for k in (1, 2, 3):
                first_copy(kind, k).wait_recv()
            for copy in spread_copies(1, kind):
                copy.start()
            rows_in = cols[0, kind].reshape(SLOTS * 16, depth)
            for k in ((0, 1), (2,))[kind]:
                value = dot_t(rows_in, wd[0]) if kind else dot(rows_in, (wg, wu)[k][0])
                for slot in range(SLOTS):
                    part[0, slot, k] = value[slot * 16:(slot + 1) * 16]
            open_copy(kind).start()
        for k in range(2):
            open_copy(k).wait_recv()
            kinds = pl.ds(2 * k, 2 - k)
            near[0, ox, kinds] = near[0, ox, kinds] + part[0, core * 2 + ox, kinds]
            open_far_copy(k).start()

        def products(i):
            group, c = i // chunks, i % chunks

            @pl.when(jnp.logical_and(i > 0, group == jnp.where(c < EARLY, 0, 1)))
            def _():
                for copy in weight_copies(c):
                    copy.wait()

            for other in (1, 2, 3):
                @pl.when(i == other * chunks)
                def _(other=other):
                    for kind in range(2):
                        for copy in spread_copies(other, kind):
                            copy.wait_recv()

            x_rows = cols[group, 0].reshape(SLOTS * 16, depth)
            dy_rows = cols[group, 1].reshape(SLOTS * 16, depth)
            for k, value in enumerate((dot(x_rows, wg[c]), dot(x_rows, wu[c]), dot_t(dy_rows, wd[c]))):
                for slot in range(SLOTS):
                    part[i, slot, k] = value[slot * 16:(slot + 1) * 16]
            near_copy(i).start()

        def half_sum(i):
            near_copy(i).wait_recv()
            near[i, ox] = near[i, ox] + part[i, core * 2 + ox]
            far_copy(i).start()

        def activations(i):
            far_copy(i).wait_recv()
            gate = part[i, mine, 0] + near[i, x, 0] + far[i, 0]
            up = part[i, mine, 1] + near[i, x, 1] + far[i, 1]
            grad = part[i, mine, 2] + near[i, x, 2] + far[i, 2]
            sig = jax.nn.sigmoid(gate)
            act = gate * sig
            hid[i, 0, mine] = (act * up).astype(BF16)
            hid[i, 1, mine] = (grad * up * sig * (1.0 + gate * (1.0 - sig))).astype(BF16)
            hid[i, 2, mine] = (grad * act).astype(BF16)
            hc_copy(i).start()

        def back(i):
            group, c = i // chunks, i % chunks
            hc_copy(i).wait_recv()
            hf_copy(i).wait_recv()
            h_rows = hid[i, 0].reshape(SLOTS * 16, width)
            da_rows = hid[i, 1].reshape(SLOTS * 16, width)
            db_rows = hid[i, 2].reshape(SLOTS * 16, width)
            acc[group, 0] += dot(h_rows, wd[c]).reshape(SLOTS, 16, depth)
            acc[group, 1] += (dot_t(da_rows, wg[c]) + dot_t(db_rows, wu[c])).reshape(SLOTS, 16, depth)

            for other in (1, 2, 3):
                @pl.when(i == other * chunks + chunks - 1)
                def _(other=other):
                    for copy in acc_copies(other):
                        copy.start()

        def step(s, carry):
            @pl.when(s == EARLY)
            def _():
                half_sum(EARLY - 1)

            @pl.when(s < total)
            def _():
                products(chunk_at(s))

            for other in (2, 3):
                @pl.when(s == EARLY + 3 * (other - 2))
                def _(other=other):
                    for kind in range(2):
                        for copy in spread_copies(other, kind):
                            copy.start()

            @pl.when(jnp.logical_and(jnp.logical_and(s >= 2, s < total + 1), s != EARLY))
            def _():
                half_sum(chunk_at(s - 1))

            @pl.when(jnp.logical_and(s >= FINAL_LAG, s < total + FINAL_LAG))
            def _():
                activations(chunk_at(s - FINAL_LAG))

            @pl.when(jnp.logical_and(s >= EARLY + FINAL_LAG, s < total - chunks + EARLY + FINAL_LAG))
            def _():
                hx_copy(s - FINAL_LAG + chunks - EARLY).start()

            @pl.when(s == total)
            def _():
                for c in range(EARLY):
                    hx_copy(c).start()

            @pl.when(jnp.logical_and(s >= total - chunks + EARLY + FINAL_LAG, s < total + FINAL_LAG))
            def _():
                hx_copy(s - FINAL_LAG + chunks - total).start()

            @pl.when(jnp.logical_and(s >= FORWARD_LAG, s < FORWARD_LAG + total))
            def _():
                i = (s - FORWARD_LAG + chunks) % total
                hx_copy(i).wait_recv()
                hf_copy(i).start()

            @pl.when(s == total + FINAL_LAG)
            def _():
                x_turned[...] = cols[:, 0].reshape(GROUPS * SLOTS * 16, depth).T

            @pl.when(s >= BACK_LAG)
            def _():
                back((s - BACK_LAG + chunks) % total)

            return carry

        lax.fori_loop(1, total + BACK_LAG, step, 0)

        for group in (1, 2, 3):
            for copy in acc_copies(group):
                copy.wait_recv()
        for kind in range(2):
            value = acc[0, kind] + acc_in[0, kind] + acc_in[1, kind] + acc_in[2, kind]
            tail[kind] = (cols[0, kind].astype(F32) + value).astype(BF16)
            for k in (2, 3, 1):
                tail_copy(kind, k).start()
        for kind in range(2):
            rows[kind, :, own] = tail[kind, mine]
        for k in (1, 2, 3):
            for kind in range(2):
                tail_copy(kind, k).wait_recv()
        for k in (1, 2, 3):
            for kind in range(2):
                first_copy(kind, k).wait_send()
                tail_copy(kind, k).wait_send()
            for copy in spread_copies(k, 0) + spread_copies(k, 1) + acc_copies(k):
                copy.wait_send()

        for k in range(2):
            open_copy(k).wait_send()

        def drain(i, carry):
            @pl.when(i > 0)
            def _():
                near_copy(i).wait_send()

            far_copy(i).wait_send()
            hc_copy(i).wait_send()
            hx_copy(i).wait_send()
            hf_copy(i).wait_send()
            return carry

        lax.fori_loop(0, total, drain, 0)

    return kernel, total


def finish(rows, hid, cols, x_turned):
    _, local_rows, model = rows.shape
    total, _, _, _, width = hid.shape
    depth, count = x_turned.shape
    chunks = total // GROUPS
    hidden = chunks * width
    ring = 4

    def kernel(rows_ref, hid_ref, cols_ref, x_ref, y_hbm, dx_hbm, dg_hbm, du_hbm, dd_hbm, g_tile, u_tile, d_tile, row_sem, out_sem):
        row_copies = [pltpu.make_async_copy(rows_ref.at[k], dst, row_sem.at[k]) for k, dst in enumerate((y_hbm, dx_hbm))]

        def all_rows(c, k):
            return jnp.concatenate([hid_ref[group * chunks + c, k].reshape(SLOTS * 16, width) for group in range(GROUPS)])

        def stores(c):
            slot = c % ring
            span = pl.ds(pl.multiple_of(c * width, width), width)
            return (pltpu.make_async_copy(g_tile.at[slot], dg_hbm.at[:, span], out_sem.at[0, slot]),
                    pltpu.make_async_copy(u_tile.at[slot], du_hbm.at[:, span], out_sem.at[1, slot]),
                    pltpu.make_async_copy(d_tile.at[slot], dd_hbm.at[span], out_sem.at[2, slot]))

        def step(c, carry):
            slot = c % ring
            old, new = stores(c - ring), stores(c)
            for k in range(3):
                @pl.when(c >= ring)
                def _(k=k):
                    old[k].wait()
                if k == 0:
                    g_tile[slot] = dot(x_ref[...], all_rows(c, 1))
                elif k == 1:
                    u_tile[slot] = dot(x_ref[...], all_rows(c, 2))
                else:
                    d_tile[slot] = dot(all_rows(c, 0).T, cols_ref[:, 1].reshape(count, depth))
                new[k].start()
            return carry

        lax.fori_loop(0, chunks, step, 0)
        for copy in row_copies:
            copy.start()
        for c in range(chunks - ring, chunks):
            for copy in stores(c):
                copy.wait()
        for copy in row_copies:
            copy.wait()

    dma = pltpu.SemaphoreType.DMA
    any_space = pl.BlockSpec(memory_space=pl.ANY)
    vmem = pl.BlockSpec(memory_space=pltpu.VMEM)
    row_shape = jax.ShapeDtypeStruct((local_rows, model), BF16)
    held = [pltpu.with_memory_space_constraint(value, pltpu.VMEM) for value in (rows, hid, cols, x_turned)]
    return pl.pallas_call(
        kernel,
        out_shape=[row_shape, row_shape, jax.ShapeDtypeStruct((depth, hidden), F32), jax.ShapeDtypeStruct((depth, hidden), F32), jax.ShapeDtypeStruct((hidden, depth), F32)],
        in_specs=[vmem] * 4,
        out_specs=[any_space] * 5,
        scratch_shapes=[
            pltpu.VMEM((ring, depth, width), F32),
            pltpu.VMEM((ring, depth, width), F32),
            pltpu.VMEM((ring, width, depth), F32),
            dma((2,)), dma((3, ring)),
        ],
        compiler_params=pltpu.CompilerParams(vmem_limit_bytes=40 * 2**20),
        cost_estimate=pl.CostEstimate(flops=6 * count * depth * hidden, bytes_accessed=12 * depth * hidden, transcendentals=0),
    )(*held)


def solution(mesh):
    row_spec = P(None, ("dp", "tp"), None)
    in_specs = (row_spec, P("dp", "tp"), P("dp", "tp"), P("tp", "dp"), row_spec)
    out_specs = (row_spec, row_spec, P("dp", "tp"), P("dp", "tp"), P("tp", "dp"))

    def local_step(x_loc, w_gate_loc, w_up_loc, w_down_loc, dy_loc):
        depth, hidden = w_gate_loc.shape
        micro, local_rows, model = x_loc.shape
        width = 512
        chunks = hidden // width
        kernel, total = make_kernel(chunks, width)
        dma = pltpu.SemaphoreType.DMA
        any_space = pl.BlockSpec(memory_space=pl.ANY)
        vmem = pl.BlockSpec(memory_space=pltpu.VMEM)
        outs = pl.pallas_call(
            kernel,
            out_shape=[
                pltpu.VMEM((2, micro * local_rows, model), BF16),
                pltpu.VMEM((total, 3, SLOTS, 16, width), BF16),
                pltpu.VMEM((GROUPS, 2, SLOTS, 16, depth), BF16),
                pltpu.VMEM((depth, GROUPS * SLOTS * 16), BF16),
            ],
            in_specs=[any_space] * 5,
            out_specs=[vmem] * 4,
            scratch_shapes=[
                pltpu.VMEM((chunks, depth, width), BF16),
                pltpu.VMEM((chunks, depth, width), BF16),
                pltpu.VMEM((chunks, width, depth), BF16),
                pltpu.VMEM((16, model), BF16),
                pltpu.VMEM((16, model), BF16),
                pltpu.VMEM((total, SLOTS, 3, 16, width), F32),
                pltpu.VMEM((total, 2, 3, 16, width), F32),
                pltpu.VMEM((total, 3, 16, width), F32),
                pltpu.VMEM((GROUPS, 2, SLOTS, 16, depth), F32),
                pltpu.VMEM((GROUPS - 1, 2, SLOTS, 16, depth), F32),
                pltpu.VMEM((2, SLOTS, 16, depth), BF16),
                dma((chunks, 3)),
                dma((2, 3)), dma((2, 3)),
                dma((3, 2, 2)), dma((3, 2, 2)),
                dma((total,)), dma((total,)),
                dma((total,)), dma((total,)),
                dma((total,)), dma((total,)),
                dma((total,)), dma((total,)),
                dma((total,)), dma((total,)),
                dma((3, 2)), dma((3, 2)),
                dma((2, 3)), dma((2, 3)),
                dma((2,)), dma((2,)), dma((2,)),
            ],
            compiler_params=pltpu.CompilerParams(collective_id=0, has_side_effects=True, vmem_limit_bytes=53 * 2**20),
        )(x_loc.reshape(micro * local_rows, model), dy_loc.reshape(micro * local_rows, model), w_gate_loc, w_up_loc, w_down_loc)
        y_rows, dx_rows, dw_gate, dw_up, dw_down = finish(*outs)
        return y_rows.reshape(x_loc.shape), dx_rows.reshape(x_loc.shape), dw_gate, dw_up, dw_down

    return jax.shard_map(local_step, mesh=mesh, in_specs=in_specs, out_specs=out_specs, check_vma=False)
```

```python
import jax
import jax.numpy as jnp
from jax import lax
from jax.experimental import pallas as pl
from jax.experimental.pallas import tpu as pltpu
from jax.sharding import PartitionSpec as P

MESH = pl.DeviceIdType.MESH
F32 = jnp.float32
BF16 = jnp.bfloat16
GROUPS = 4
SLOTS = 4
FINAL_LAG = 4
FORWARD_LAG = 11
BACK_LAG = 12
EARLY = 4


def dot(lhs, rhs):
    return lax.dot_general(lhs, rhs, (((1,), (0,)), ((), ())), preferred_element_type=F32)


def dot_t(lhs, rhs):
    return lax.dot_general(lhs, rhs, (((1,), (1,)), ((), ())), preferred_element_type=F32)


def make_kernel(chunks, width):
    total = GROUPS * chunks

    def kernel(x_hbm, dy_hbm, wg_hbm, wu_hbm, wd_hbm,
               rows, hid, cols, x_turned,
               wg, wu, wd, x_ref, dy_ref, part, near, far, acc, acc_in, tail,
               w_sem, first_send, first_recv, spread_send, spread_recv,
               near_send, near_recv, far_send, far_recv,
               hc_send, hc_recv, hx_send, hx_recv, hf_send, hf_recv,
               acc_send, acc_recv, tail_send, tail_recv, in_sem, open_send, open_recv):
        tp = lax.axis_index("tp")
        dp = lax.axis_index("dp")
        z, y = tp // 2, tp % 2
        x, core = dp // 2, dp % 2
        ox, oc = 1 - x, 1 - core
        core_peer = {"tp": tp, "dp": x * 2 + oc}
        x_peer = {"tp": tp, "dp": ox * 2 + core}
        home = core * 2 + x
        owned = core * 2 + ox
        depth = cols.shape[-1]

        tp_peers = [{"tp": pz * 2 + py, "dp": dp} for pz, py in ((z, 1 - y), (1 - z, y), (1 - z, 1 - y))]
        rows_of = (pl.ds(0, 8), pl.ds(8, 8))

        def chunk_at(s):
            return jnp.where(s < EARLY, s, jnp.where(s < total - chunks + EARLY, s + chunks - EARLY, s + chunks - total))

        def dp_peer(k):
            px, pc = (x + k // 2) % 2, (core + k % 2) % 2
            return px * 2 + pc, pc * 2 + px

        def weight_copies(c):
            span = pl.ds(pl.multiple_of(c * width, width), width)
            return (pltpu.make_async_copy(wg_hbm.at[:, span], wg.at[c], w_sem.at[c, 0]),
                    pltpu.make_async_copy(wu_hbm.at[:, span], wu.at[c], w_sem.at[c, 1]),
                    pltpu.make_async_copy(wd_hbm.at[span], wd.at[c], w_sem.at[c, 2]))

        def remote(src, dst, send, recv, device):
            return pltpu.make_async_remote_copy(src_ref=src, dst_ref=dst, send_sem=send, recv_sem=recv,
                                                device_id=device, device_id_type=MESH)

        def first_copy(kind, k):
            peer, _ = dp_peer(k)
            src = (x_ref, dy_ref)[kind].at[:, pl.ds(pl.multiple_of(peer * depth, depth), depth)]
            return remote(src, cols.at[0, kind, home], first_send.at[kind, k - 1], first_recv.at[kind, k - 1], {"tp": tp, "dp": peer})

        def spread_copies(group, kind):
            if group == 2:
                return [remote(cols.at[0, kind], cols.at[2, kind], spread_send.at[1, kind, 0], spread_recv.at[1, kind, 0], tp_peers[2])]
            return [remote(cols.at[0, kind, :, rows_of[group // 2]], cols.at[group, kind, :, rows_of[way]],
                           spread_send.at[group - 1, kind, way], spread_recv.at[group - 1, kind, way], tp_peers[way]) for way in range(2)]

        def near_copy(i):
            return remote(part.at[i, pl.ds(oc * 2, 2)], near.at[i], near_send.at[i], near_recv.at[i], core_peer)

        def open_copy(i, side, send, recv):
            return remote(part.at[i, oc * 2 + side], near.at[i, side], send.at[i], recv.at[i], core_peer)

        def here_copy(i):
            return open_copy(i, x, open_send, open_recv)

        def there_copy(i):
            return open_copy(i, ox, near_send, near_recv)

        def far_copy(i):
            return remote(near.at[i, x], far.at[i], far_send.at[i], far_recv.at[i], x_peer)

        def hc_copy(i):
            here = hid.at[i, :, owned]
            return remote(here, here, hc_send.at[i], hc_recv.at[i], core_peer)

        def hx_copy(i):
            here = hid.at[i, :, owned]
            return remote(here, here, hx_send.at[i], hx_recv.at[i], x_peer)

        def hf_copy(i):
            there = hid.at[i, :, home]
            return remote(there, there, hf_send.at[i], hf_recv.at[i], core_peer)

        def acc_copies(group):
            if group == 2:
                return [remote(acc.at[2], acc_in.at[2], acc_send.at[1, 0], acc_recv.at[1, 0], tp_peers[2])]
            return [remote(acc.at[group, :, :, rows_of[way]], acc_in.at[way, :, :, rows_of[group // 2]],
                           acc_send.at[group - 1, way], acc_recv.at[group - 1, way], tp_peers[way]) for way in range(2)]

        def tail_copy(kind, k):
            peer, slot = dp_peer(k)
            dst = rows.at[kind, :, pl.ds(pl.multiple_of(dp * depth, depth), depth)]
            return remote(tail.at[kind, slot], dst, tail_send.at[kind, k - 1], tail_recv.at[kind, k - 1], {"tp": tp, "dp": peer})

        barrier = pltpu.get_barrier_semaphore()
        for k in range(1, 4):
            pl.semaphore_signal(barrier, inc=1, device_id=tp_peers[k - 1], device_id_type=MESH)
            pl.semaphore_signal(barrier, inc=1, device_id={"tp": tp, "dp": dp_peer(k)[0]}, device_id_type=MESH)
        row_loads = [pltpu.make_async_copy(src, dst, in_sem.at[k]) for k, (src, dst) in enumerate(((x_hbm, x_ref), (dy_hbm, dy_ref)))]
        for copy in row_loads:
            copy.start()
        for c in range(chunks):
            for copy in weight_copies(c):
                copy.start()

        for copy in row_loads:
            copy.wait()
        pl.semaphore_wait(barrier, 6)

        for kind in range(2):
            for k in (1, 2, 3):
                first_copy(kind, k).start()
        own = pl.ds(pl.multiple_of(dp * depth, depth), depth)
        cols[0, 0, home] = x_ref[:, own]
        cols[0, 1, home] = dy_ref[:, own]
        acc[...] = jnp.zeros_like(acc)

        def half_products(i, side):
            rows_in = [jnp.concatenate([cols[0, kind, side], cols[0, kind, 2 + side]]) for kind in range(2)]
            for k, value in enumerate((dot(rows_in[0], wg[i]), dot(rows_in[0], wu[i]), dot_t(rows_in[1], wd[i]))):
                part[i, side, k] = value[:16]
                part[i, 2 + side, k] = value[16:]

        def half_sum(i, copy):
            copy.wait_recv()
            near[i, x] = near[i, x] + part[i, home]
            far_copy(i).start()

        for kind in range(2):
            first_copy(kind, 1).wait_recv()

        def open_here(i, carry):
            for copy in weight_copies(i):
                copy.wait()
            half_products(i, x)
            here_copy(i).start()

            @pl.when(i > 0)
            def _():
                half_sum(i - 1, here_copy(i - 1))

            return carry

        lax.fori_loop(0, EARLY, open_here, 0)
        for kind in range(2):
            for k in (2, 3):
                first_copy(kind, k).wait_recv()
            for copy in spread_copies(1, kind):
                copy.start()
        half_sum(EARLY - 1, here_copy(EARLY - 1))

        def open_there(i, carry):
            half_products(i, ox)
            there_copy(i).start()
            return carry

        lax.fori_loop(0, EARLY, open_there, 0)

        def products(i):
            group, c = i // chunks, i % chunks

            @pl.when(jnp.logical_and(group == 1, c >= EARLY))
            def _():
                for copy in weight_copies(c):
                    copy.wait()

            for other in (1, 2, 3):
                @pl.when(i == other * chunks)
                def _(other=other):
                    for kind in range(2):
                        for copy in spread_copies(other, kind):
                            copy.wait_recv()

            x_rows = cols[group, 0].reshape(SLOTS * 16, depth)
            dy_rows = cols[group, 1].reshape(SLOTS * 16, depth)
            for k, value in enumerate((dot(x_rows, wg[c]), dot(x_rows, wu[c]), dot_t(dy_rows, wd[c]))):
                for slot in range(SLOTS):
                    part[i, slot, k] = value[slot * 16:(slot + 1) * 16]
            near_copy(i).start()

        def activations(i):
            @pl.when(i < EARLY)
            def _():
                there_copy(i).wait_recv()

            far_copy(i).wait_recv()
            gate = part[i, owned, 0] + near[i, ox, 0] + far[i, 0]
            up = part[i, owned, 1] + near[i, ox, 1] + far[i, 1]
            grad = part[i, owned, 2] + near[i, ox, 2] + far[i, 2]
            sig = jax.nn.sigmoid(gate)
            act = gate * sig
            hid[i, 0, owned] = (act * up).astype(BF16)
            hid[i, 1, owned] = (grad * up * sig * (1.0 + gate * (1.0 - sig))).astype(BF16)
            hid[i, 2, owned] = (grad * act).astype(BF16)
            hc_copy(i).start()

        def back_rows(i, k):
            return hid[i, k].reshape(SLOTS * 16, width)

        def add_y(group, i, c):
            acc[group, 0] += dot(back_rows(i, 0), wd[c]).reshape(SLOTS, 16, depth)

        def add_dx(group, i, c):
            acc[group, 1] += (dot_t(back_rows(i, 1), wg[c]) + dot_t(back_rows(i, 2), wu[c])).reshape(SLOTS, 16, depth)

        def back(i):
            group, c = i // chunks, i % chunks
            hc_copy(i).wait_recv()
            hf_copy(i).wait_recv()
            add_y(group, i, c)
            add_dx(group, i, c)
            for other in (1, 2, 3):
                @pl.when(i == other * chunks + chunks - 1)
                def _(other=other):
                    for copy in acc_copies(other):
                        copy.start()

        def step(s, carry):
            @pl.when(s < total)
            def _():
                products(chunk_at(s))

            for other in (2, 3):
                @pl.when(s == EARLY + 3 * (other - 2))
                def _(other=other):
                    for kind in range(2):
                        for copy in spread_copies(other, kind):
                            copy.start()

            @pl.when(jnp.logical_and(s > EARLY, s < total + 1))
            def _():
                i = chunk_at(s - 1)
                half_sum(i, near_copy(i))

            @pl.when(jnp.logical_and(s >= FINAL_LAG, s < total + FINAL_LAG))
            def _():
                activations(chunk_at(s - FINAL_LAG))

            @pl.when(jnp.logical_and(s >= EARLY + FINAL_LAG, s < total - chunks + EARLY + FINAL_LAG))
            def _():
                hx_copy(s - FINAL_LAG + chunks - EARLY).start()

            @pl.when(s == total)
            def _():
                for c in range(EARLY):
                    hx_copy(c).start()

            @pl.when(jnp.logical_and(s >= total - chunks + EARLY + FINAL_LAG, s < total + FINAL_LAG))
            def _():
                hx_copy(s - FINAL_LAG + chunks - total).start()

            @pl.when(jnp.logical_and(s >= FORWARD_LAG, s < FORWARD_LAG + total))
            def _():
                i = (s - FORWARD_LAG + chunks) % total
                hx_copy(i).wait_recv()
                hf_copy(i).start()

            @pl.when(s == total + FINAL_LAG)
            def _():
                x_turned[...] = cols[:, 0].reshape(GROUPS * SLOTS * 16, depth).T

            @pl.when(s >= BACK_LAG)
            def _():
                back((s - BACK_LAG + chunks) % total)

            return carry

        lax.fori_loop(EARLY, total + BACK_LAG - 1, step, 0)

        last = chunks - 1
        hc_copy(last).wait_recv()
        hf_copy(last).wait_recv()
        for kind in range(2):
            (add_y, add_dx)[kind](0, last, last)
            if kind == 0:
                for group in (1, 2, 3):
                    for copy in acc_copies(group):
                        copy.wait_recv()
            value = acc[0, kind] + acc_in[0, kind] + acc_in[1, kind] + acc_in[2, kind]
            tail[kind] = (cols[0, kind].astype(F32) + value).astype(BF16)
            for k in (2, 3, 1):
                tail_copy(kind, k).start()
        for kind in range(2):
            rows[kind, :, own] = tail[kind, home]

        for k in (1, 2, 3):
            for copy in [first_copy(0, k), first_copy(1, k)] + spread_copies(k, 0) + spread_copies(k, 1) + acc_copies(k):
                copy.wait_send()

        def drain(i, carry):
            @pl.when(i < EARLY)
            def _():
                here_copy(i).wait_send()
                there_copy(i).wait_send()

            @pl.when(i >= EARLY)
            def _():
                near_copy(i).wait_send()

            far_copy(i).wait_send()
            hc_copy(i).wait_send()
            hx_copy(i).wait_send()
            hf_copy(i).wait_send()
            return carry

        lax.fori_loop(0, total, drain, 0)
        for kind in range(2):
            for k in (1, 2, 3):
                tail_copy(kind, k).wait()

    return kernel, total


def finish(rows, hid, cols, x_turned):
    _, local_rows, model = rows.shape
    total, _, _, _, width = hid.shape
    depth, count = x_turned.shape
    chunks = total // GROUPS
    hidden = chunks * width
    ring = 4

    def kernel(rows_ref, hid_ref, cols_ref, x_ref, y_hbm, dx_hbm, dg_hbm, du_hbm, dd_hbm, g_tile, u_tile, d_tile, row_sem, out_sem):
        row_copies = [pltpu.make_async_copy(rows_ref.at[k], dst, row_sem.at[k]) for k, dst in enumerate((y_hbm, dx_hbm))]

        def all_rows(c, k):
            return jnp.concatenate([hid_ref[group * chunks + c, k].reshape(SLOTS * 16, width) for group in range(GROUPS)])

        def stores(c):
            slot = c % ring
            span = pl.ds(pl.multiple_of(c * width, width), width)
            return (pltpu.make_async_copy(g_tile.at[slot], dg_hbm.at[:, span], out_sem.at[0, slot]),
                    pltpu.make_async_copy(u_tile.at[slot], du_hbm.at[:, span], out_sem.at[1, slot]),
                    pltpu.make_async_copy(d_tile.at[slot], dd_hbm.at[span], out_sem.at[2, slot]))

        def step(c, carry):
            slot = c % ring
            old, new = stores(c - ring), stores(c)
            for k in range(3):
                @pl.when(c >= ring)
                def _(k=k):
                    old[k].wait()
                if k == 0:
                    g_tile[slot] = dot(x_ref[...], all_rows(c, 1))
                elif k == 1:
                    u_tile[slot] = dot(x_ref[...], all_rows(c, 2))
                else:
                    d_tile[slot] = dot(all_rows(c, 0).T, cols_ref[:, 1].reshape(count, depth))
                new[k].start()
            return carry

        lax.fori_loop(0, chunks, step, 0)
        for copy in row_copies:
            copy.start()
        for c in range(chunks - ring, chunks):
            for copy in stores(c):
                copy.wait()
        for copy in row_copies:
            copy.wait()

    dma = pltpu.SemaphoreType.DMA
    any_space = pl.BlockSpec(memory_space=pl.ANY)
    vmem = pl.BlockSpec(memory_space=pltpu.VMEM)
    row_shape = jax.ShapeDtypeStruct((local_rows, model), BF16)
    held = [pltpu.with_memory_space_constraint(value, pltpu.VMEM) for value in (rows, hid, cols, x_turned)]
    return pl.pallas_call(
        kernel,
        out_shape=[row_shape, row_shape, jax.ShapeDtypeStruct((depth, hidden), F32), jax.ShapeDtypeStruct((depth, hidden), F32), jax.ShapeDtypeStruct((hidden, depth), F32)],
        in_specs=[vmem] * 4,
        out_specs=[any_space] * 5,
        scratch_shapes=[
            pltpu.VMEM((ring, depth, width), F32),
            pltpu.VMEM((ring, depth, width), F32),
            pltpu.VMEM((ring, width, depth), F32),
            dma((2,)), dma((3, ring)),
        ],
        compiler_params=pltpu.CompilerParams(vmem_limit_bytes=40 * 2**20),
        cost_estimate=pl.CostEstimate(flops=6 * count * depth * hidden, bytes_accessed=12 * depth * hidden, transcendentals=0),
    )(*held)


def solution(mesh):
    row_spec = P(None, ("dp", "tp"), None)
    in_specs = (row_spec, P("dp", "tp"), P("dp", "tp"), P("tp", "dp"), row_spec)
    out_specs = (row_spec, row_spec, P("dp", "tp"), P("dp", "tp"), P("tp", "dp"))

    def local_step(x_loc, w_gate_loc, w_up_loc, w_down_loc, dy_loc):
        depth, hidden = w_gate_loc.shape
        micro, local_rows, model = x_loc.shape
        width = 512
        chunks = hidden // width
        kernel, total = make_kernel(chunks, width)
        dma = pltpu.SemaphoreType.DMA
        any_space = pl.BlockSpec(memory_space=pl.ANY)
        vmem = pl.BlockSpec(memory_space=pltpu.VMEM)
        outs = pl.pallas_call(
            kernel,
            out_shape=[
                pltpu.VMEM((2, micro * local_rows, model), BF16),
                pltpu.VMEM((total, 3, SLOTS, 16, width), BF16),
                pltpu.VMEM((GROUPS, 2, SLOTS, 16, depth), BF16),
                pltpu.VMEM((depth, GROUPS * SLOTS * 16), BF16),
            ],
            in_specs=[any_space] * 5,
            out_specs=[vmem] * 4,
            scratch_shapes=[
                pltpu.VMEM((chunks, depth, width), BF16),
                pltpu.VMEM((chunks, depth, width), BF16),
                pltpu.VMEM((chunks, width, depth), BF16),
                pltpu.VMEM((16, model), BF16),
                pltpu.VMEM((16, model), BF16),
                pltpu.VMEM((total, SLOTS, 3, 16, width), F32),
                pltpu.VMEM((total, 2, 3, 16, width), F32),
                pltpu.VMEM((total, 3, 16, width), F32),
                pltpu.VMEM((GROUPS, 2, SLOTS, 16, depth), F32),
                pltpu.VMEM((GROUPS - 1, 2, SLOTS, 16, depth), F32),
                pltpu.VMEM((2, SLOTS, 16, depth), BF16),
                dma((chunks, 3)),
                dma((2, 3)), dma((2, 3)),
                dma((3, 2, 2)), dma((3, 2, 2)),
                dma((total,)), dma((total,)),
                dma((total,)), dma((total,)),
                dma((total,)), dma((total,)),
                dma((total,)), dma((total,)),
                dma((total,)), dma((total,)),
                dma((3, 2)), dma((3, 2)),
                dma((2, 3)), dma((2, 3)),
                dma((2,)), dma((EARLY,)), dma((EARLY,)),
            ],
            compiler_params=pltpu.CompilerParams(collective_id=0, has_side_effects=True, vmem_limit_bytes=53 * 2**20),
        )(x_loc.reshape(micro * local_rows, model), dy_loc.reshape(micro * local_rows, model), w_gate_loc, w_up_loc, w_down_loc)
        y_rows, dx_rows, dw_gate, dw_up, dw_down = finish(*outs)
        return y_rows.reshape(x_loc.shape), dx_rows.reshape(x_loc.shape), dw_gate, dw_up, dw_down

    return jax.shard_map(local_step, mesh=mesh, in_specs=in_specs, out_specs=out_specs, check_vma=False)
```

```python
import jax
import jax.numpy as jnp
from jax import lax
from jax.experimental import pallas as pl
from jax.experimental.pallas import tpu as pltpu
from jax.sharding import PartitionSpec as P

MESH = pl.DeviceIdType.MESH
F32 = jnp.float32
BF16 = jnp.bfloat16
GROUPS = 4
SLOTS = 4
FINAL_LAG = 4
FORWARD_LAG = 11
BACK_LAG = 12
EARLY = 4


def dot(lhs, rhs):
    return lax.dot_general(lhs, rhs, (((1,), (0,)), ((), ())), preferred_element_type=F32)


def dot_t(lhs, rhs):
    return lax.dot_general(lhs, rhs, (((1,), (1,)), ((), ())), preferred_element_type=F32)


def make_kernel(chunks, width):
    total = GROUPS * chunks

    def kernel(x_hbm, dy_hbm, wg_hbm, wu_hbm, wd_hbm,
               rows, hid, cols, x_turned,
               wg, wu, wd, x_ref, dy_ref, part, near, far, acc, acc_in, tail,
               w_sem, first_send, first_recv, spread_send, spread_recv,
               near_send, near_recv, far_send, far_recv,
               hc_send, hc_recv, hx_send, hx_recv, hf_send, hf_recv,
               acc_send, acc_recv, tail_send, tail_recv, in_sem, open_send, open_recv):
        tp = lax.axis_index("tp")
        dp = lax.axis_index("dp")
        z, y = tp // 2, tp % 2
        x, core = dp // 2, dp % 2
        ox, oc = 1 - x, 1 - core
        core_peer = {"tp": tp, "dp": x * 2 + oc}
        x_peer = {"tp": tp, "dp": ox * 2 + core}
        home = core * 2 + x
        owned = core * 2 + ox
        depth = cols.shape[-1]

        tp_peers = [{"tp": pz * 2 + py, "dp": dp} for pz, py in ((z, 1 - y), (1 - z, y), (1 - z, 1 - y))]
        rows_of = (pl.ds(0, 8), pl.ds(8, 8))

        def chunk_at(s):
            return jnp.where(s < EARLY, s, jnp.where(s < total - chunks + EARLY, s + chunks - EARLY, s + chunks - total))

        def dp_peer(k):
            px, pc = (x + k // 2) % 2, (core + k % 2) % 2
            return px * 2 + pc, pc * 2 + px

        def weight_copies(c):
            span = pl.ds(pl.multiple_of(c * width, width), width)
            return (pltpu.make_async_copy(wg_hbm.at[:, span], wg.at[c], w_sem.at[c, 0]),
                    pltpu.make_async_copy(wu_hbm.at[:, span], wu.at[c], w_sem.at[c, 1]),
                    pltpu.make_async_copy(wd_hbm.at[span], wd.at[c], w_sem.at[c, 2]))

        def remote(src, dst, send, recv, device):
            return pltpu.make_async_remote_copy(src_ref=src, dst_ref=dst, send_sem=send, recv_sem=recv,
                                                device_id=device, device_id_type=MESH)

        def first_copy(kind, k):
            peer, _ = dp_peer(k)
            src = (x_ref, dy_ref)[kind].at[:, pl.ds(pl.multiple_of(peer * depth, depth), depth)]
            return remote(src, cols.at[0, kind, home], first_send.at[kind, k - 1], first_recv.at[kind, k - 1], {"tp": tp, "dp": peer})

        def spread_copies(group, kind):
            if group == 2:
                return [remote(cols.at[0, kind], cols.at[2, kind], spread_send.at[1, kind, 0], spread_recv.at[1, kind, 0], tp_peers[2])]
            return [remote(cols.at[0, kind, :, rows_of[group // 2]], cols.at[group, kind, :, rows_of[way]],
                           spread_send.at[group - 1, kind, way], spread_recv.at[group - 1, kind, way], tp_peers[way]) for way in range(2)]

        def near_copy(i):
            return remote(part.at[i, pl.ds(oc * 2, 2)], near.at[i], near_send.at[i], near_recv.at[i], core_peer)

        def open_copy(i, side, send, recv):
            return remote(part.at[i, oc * 2 + side], near.at[i, side], send.at[i], recv.at[i], core_peer)

        def here_copy(i):
            return open_copy(i, x, open_send, open_recv)

        def there_copy(i):
            return open_copy(i, ox, near_send, near_recv)

        def far_copy(i):
            return remote(near.at[i, x], far.at[i], far_send.at[i], far_recv.at[i], x_peer)

        def hc_copy(i):
            here = hid.at[i, :, owned]
            return remote(here, here, hc_send.at[i], hc_recv.at[i], core_peer)

        def hx_copy(i):
            here = hid.at[i, :, owned]
            return remote(here, here, hx_send.at[i], hx_recv.at[i], x_peer)

        def hf_copy(i):
            there = hid.at[i, :, home]
            return remote(there, there, hf_send.at[i], hf_recv.at[i], core_peer)

        def acc_copies(group, kind):
            if group == 2:
                return [remote(acc.at[2, kind], acc_in.at[2, kind], acc_send.at[1, kind, 0], acc_recv.at[1, kind, 0], tp_peers[2])]
            return [remote(acc.at[group, kind, :, rows_of[way]], acc_in.at[way, kind, :, rows_of[group // 2]],
                           acc_send.at[group - 1, kind, way], acc_recv.at[group - 1, kind, way], tp_peers[way]) for way in range(2)]

        def tail_copy(micro, kind, k):
            peer, slot = dp_peer(k)
            dst = rows.at[kind, rows_of[micro], pl.ds(pl.multiple_of(dp * depth, depth), depth)]
            return remote(tail.at[kind, slot, rows_of[micro]], dst, tail_send.at[micro, kind, k - 1], tail_recv.at[micro, kind, k - 1],
                          {"tp": tp, "dp": peer})

        barrier = pltpu.get_barrier_semaphore()
        for k in range(1, 4):
            pl.semaphore_signal(barrier, inc=1, device_id=tp_peers[k - 1], device_id_type=MESH)
            pl.semaphore_signal(barrier, inc=1, device_id={"tp": tp, "dp": dp_peer(k)[0]}, device_id_type=MESH)
        row_loads = [pltpu.make_async_copy(src, dst, in_sem.at[k]) for k, (src, dst) in enumerate(((x_hbm, x_ref), (dy_hbm, dy_ref)))]
        for copy in row_loads:
            copy.start()
        for c in range(chunks):
            for copy in weight_copies(c):
                copy.start()

        for copy in row_loads:
            copy.wait()
        pl.semaphore_wait(barrier, 6)

        for kind in range(2):
            for k in (1, 2, 3):
                first_copy(kind, k).start()
        own = pl.ds(pl.multiple_of(dp * depth, depth), depth)
        cols[0, 0, home] = x_ref[:, own]
        cols[0, 1, home] = dy_ref[:, own]
        acc[...] = jnp.zeros_like(acc)

        def half_products(i, side):
            rows_in = [jnp.concatenate([cols[0, kind, side], cols[0, kind, 2 + side]]) for kind in range(2)]
            for k, value in enumerate((dot(rows_in[0], wg[i]), dot(rows_in[0], wu[i]), dot_t(rows_in[1], wd[i]))):
                part[i, side, k] = value[:16]
                part[i, 2 + side, k] = value[16:]

        def half_sum(i, copy):
            copy.wait_recv()
            near[i, x] = near[i, x] + part[i, home]
            far_copy(i).start()

        for kind in range(2):
            first_copy(kind, 1).wait_recv()

        def open_here(i, carry):
            for copy in weight_copies(i):
                copy.wait()
            half_products(i, x)
            here_copy(i).start()

            @pl.when(i > 0)
            def _():
                half_sum(i - 1, here_copy(i - 1))

            return carry

        lax.fori_loop(0, EARLY, open_here, 0)
        for kind in range(2):
            for k in (2, 3):
                first_copy(kind, k).wait_recv()
            for copy in spread_copies(1, kind):
                copy.start()
        half_sum(EARLY - 1, here_copy(EARLY - 1))

        def open_there(i, carry):
            half_products(i, ox)
            there_copy(i).start()
            return carry

        lax.fori_loop(0, EARLY, open_there, 0)

        def products(i):
            group, c = i // chunks, i % chunks

            @pl.when(jnp.logical_and(group == 1, c >= EARLY))
            def _():
                for copy in weight_copies(c):
                    copy.wait()

            for other in (1, 2, 3):
                @pl.when(i == other * chunks)
                def _(other=other):
                    for kind in range(2):
                        for copy in spread_copies(other, kind):
                            copy.wait_recv()

            x_rows = cols[group, 0].reshape(SLOTS * 16, depth)
            dy_rows = cols[group, 1].reshape(SLOTS * 16, depth)
            for k, value in enumerate((dot(x_rows, wg[c]), dot(x_rows, wu[c]), dot_t(dy_rows, wd[c]))):
                for slot in range(SLOTS):
                    part[i, slot, k] = value[slot * 16:(slot + 1) * 16]
            near_copy(i).start()

        def activations(i):
            @pl.when(i < EARLY)
            def _():
                there_copy(i).wait_recv()

            far_copy(i).wait_recv()
            gate = part[i, owned, 0] + near[i, ox, 0] + far[i, 0]
            up = part[i, owned, 1] + near[i, ox, 1] + far[i, 1]
            grad = part[i, owned, 2] + near[i, ox, 2] + far[i, 2]
            sig = jax.nn.sigmoid(gate)
            act = gate * sig
            hid[i, 0, owned] = (act * up).astype(BF16)
            hid[i, 1, owned] = (grad * up * sig * (1.0 + gate * (1.0 - sig))).astype(BF16)
            hid[i, 2, owned] = (grad * act).astype(BF16)
            hc_copy(i).start()

        def back_rows(i, k):
            return hid[i, k].reshape(SLOTS * 16, width)

        def add_y(group, i, c):
            acc[group, 0] += dot(back_rows(i, 0), wd[c]).reshape(SLOTS, 16, depth)

        def add_dx(group, i, c):
            acc[group, 1] += (dot_t(back_rows(i, 1), wg[c]) + dot_t(back_rows(i, 2), wu[c])).reshape(SLOTS, 16, depth)

        def back(i):
            group, c = i // chunks, i % chunks
            hc_copy(i).wait_recv()
            hf_copy(i).wait_recv()
            for kind in range(2):
                (add_y, add_dx)[kind](group, i, c)
                for other in (1, 2, 3):
                    @pl.when(i == other * chunks + chunks - 1)
                    def _(kind=kind, other=other):
                        for copy in acc_copies(other, kind):
                            copy.start()

        def step(s, carry):
            @pl.when(s < total)
            def _():
                products(chunk_at(s))

            for other in (2, 3):
                @pl.when(s == EARLY + 3 * (other - 2))
                def _(other=other):
                    for kind in range(2):
                        for copy in spread_copies(other, kind):
                            copy.start()

            @pl.when(jnp.logical_and(s > EARLY, s < total + 1))
            def _():
                i = chunk_at(s - 1)
                half_sum(i, near_copy(i))

            @pl.when(jnp.logical_and(s >= FINAL_LAG, s < total + FINAL_LAG))
            def _():
                activations(chunk_at(s - FINAL_LAG))

            @pl.when(jnp.logical_and(s >= EARLY + FINAL_LAG, s < total - chunks + EARLY + FINAL_LAG))
            def _():
                hx_copy(s - FINAL_LAG + chunks - EARLY).start()

            @pl.when(s == total)
            def _():
                for c in range(EARLY):
                    hx_copy(c).start()

            @pl.when(jnp.logical_and(s >= total - chunks + EARLY + FINAL_LAG, s < total + FINAL_LAG))
            def _():
                hx_copy(s - FINAL_LAG + chunks - total).start()

            @pl.when(jnp.logical_and(s >= FORWARD_LAG, s < FORWARD_LAG + total))
            def _():
                i = (s - FORWARD_LAG + chunks) % total
                hx_copy(i).wait_recv()
                hf_copy(i).start()

            @pl.when(s == total + FINAL_LAG)
            def _():
                x_turned[...] = cols[:, 0].reshape(GROUPS * SLOTS * 16, depth).T

            @pl.when(s >= BACK_LAG)
            def _():
                back((s - BACK_LAG + chunks) % total)

            return carry

        lax.fori_loop(EARLY, total + BACK_LAG - 1, step, 0)

        last = chunks - 1
        hc_copy(last).wait_recv()
        hf_copy(last).wait_recv()
        for kind in range(2):
            (add_y, add_dx)[kind](0, last, last)
        for kind in range(2):
            for copy in acc_copies(1, kind) + acc_copies(2, kind):
                copy.wait_recv()
        for micro in range(2):
            half = slice(8 * micro, 8 * micro + 8)
            for kind in range(2):
                if micro == 1:
                    for copy in acc_copies(3, kind):
                        copy.wait_recv()
                value = acc[0, kind, :, half] + acc_in[0, kind, :, half] + acc_in[1, kind, :, half] + acc_in[2, kind, :, half]
                tail[kind, :, half] = (cols[0, kind, :, half].astype(F32) + value).astype(BF16)
                for k in (2, 3, 1):
                    tail_copy(micro, kind, k).start()
        for kind in range(2):
            rows[kind, :, own] = tail[kind, home]

        for k in (1, 2, 3):
            for copy in [first_copy(0, k), first_copy(1, k)] + spread_copies(k, 0) + spread_copies(k, 1) + acc_copies(k, 0) + acc_copies(k, 1):
                copy.wait_send()

        def drain(i, carry):
            @pl.when(i < EARLY)
            def _():
                here_copy(i).wait_send()
                there_copy(i).wait_send()

            @pl.when(i >= EARLY)
            def _():
                near_copy(i).wait_send()

            far_copy(i).wait_send()
            hc_copy(i).wait_send()
            hx_copy(i).wait_send()
            hf_copy(i).wait_send()
            return carry

        lax.fori_loop(0, total, drain, 0)
        for micro in range(2):
            for kind in range(2):
                for k in (1, 2, 3):
                    tail_copy(micro, kind, k).wait()

    return kernel, total


def finish(rows, hid, cols, x_turned):
    _, local_rows, model = rows.shape
    total, _, _, _, width = hid.shape
    depth, count = x_turned.shape
    chunks = total // GROUPS
    hidden = chunks * width
    ring = 4

    def kernel(rows_ref, hid_ref, cols_ref, x_ref, y_hbm, dx_hbm, dg_hbm, du_hbm, dd_hbm, g_tile, u_tile, d_tile, row_sem, out_sem):
        row_copies = [pltpu.make_async_copy(rows_ref.at[k], dst, row_sem.at[k]) for k, dst in enumerate((y_hbm, dx_hbm))]

        def all_rows(c, k):
            return jnp.concatenate([hid_ref[group * chunks + c, k].reshape(SLOTS * 16, width) for group in range(GROUPS)])

        def stores(c, part):
            slot = c % ring
            span = pl.ds(pl.multiple_of(c * width, width), width)
            deep = pl.ds(part * (depth // 2), depth // 2)
            wide = pl.ds(part * (width // 2), width // 2)
            down = pl.ds(pl.multiple_of(c * width + part * (width // 2), width // 2), width // 2)
            return (pltpu.make_async_copy(g_tile.at[slot, deep], dg_hbm.at[deep, span], out_sem.at[0, slot, part]),
                    pltpu.make_async_copy(u_tile.at[slot, deep], du_hbm.at[deep, span], out_sem.at[1, slot, part]),
                    pltpu.make_async_copy(d_tile.at[slot, wide], dd_hbm.at[down], out_sem.at[2, slot, part]))

        def step(c, carry):
            slot = c % ring
            for k in range(3):
                value = all_rows(c, (1, 2, 0)[k])
                for part in range(2):
                    old, new = stores(c - ring, part)[k], stores(c, part)[k]

                    @pl.when(c >= ring)
                    def _(old=old):
                        old.wait()

                    deep = slice(part * (depth // 2), (part + 1) * (depth // 2))
                    wide = slice(part * (width // 2), (part + 1) * (width // 2))
                    if k == 0:
                        g_tile[slot, deep] = dot(x_ref[deep], value)
                    elif k == 1:
                        u_tile[slot, deep] = dot(x_ref[deep], value)
                    else:
                        d_tile[slot, wide] = dot(value[:, wide].T, cols_ref[:, 1].reshape(count, depth))
                    new.start()
            return carry

        lax.fori_loop(0, chunks, step, 0)
        for copy in row_copies:
            copy.start()
        for c in range(chunks - ring, chunks):
            for part in range(2):
                for copy in stores(c, part):
                    copy.wait()
        for copy in row_copies:
            copy.wait()

    dma = pltpu.SemaphoreType.DMA
    any_space = pl.BlockSpec(memory_space=pl.ANY)
    vmem = pl.BlockSpec(memory_space=pltpu.VMEM)
    row_shape = jax.ShapeDtypeStruct((local_rows, model), BF16)
    held = [pltpu.with_memory_space_constraint(value, pltpu.VMEM) for value in (rows, hid, cols, x_turned)]
    return pl.pallas_call(
        kernel,
        out_shape=[row_shape, row_shape, jax.ShapeDtypeStruct((depth, hidden), F32), jax.ShapeDtypeStruct((depth, hidden), F32), jax.ShapeDtypeStruct((hidden, depth), F32)],
        in_specs=[vmem] * 4,
        out_specs=[any_space] * 5,
        scratch_shapes=[
            pltpu.VMEM((ring, depth, width), F32),
            pltpu.VMEM((ring, depth, width), F32),
            pltpu.VMEM((ring, width, depth), F32),
            dma((2,)), dma((3, ring, 2)),
        ],
        compiler_params=pltpu.CompilerParams(vmem_limit_bytes=40 * 2**20),
        cost_estimate=pl.CostEstimate(flops=6 * count * depth * hidden, bytes_accessed=12 * depth * hidden, transcendentals=0),
    )(*held)


def solution(mesh):
    row_spec = P(None, ("dp", "tp"), None)
    in_specs = (row_spec, P("dp", "tp"), P("dp", "tp"), P("tp", "dp"), row_spec)
    out_specs = (row_spec, row_spec, P("dp", "tp"), P("dp", "tp"), P("tp", "dp"))

    def local_step(x_loc, w_gate_loc, w_up_loc, w_down_loc, dy_loc):
        depth, hidden = w_gate_loc.shape
        micro, local_rows, model = x_loc.shape
        width = 512
        chunks = hidden // width
        kernel, total = make_kernel(chunks, width)
        dma = pltpu.SemaphoreType.DMA
        any_space = pl.BlockSpec(memory_space=pl.ANY)
        vmem = pl.BlockSpec(memory_space=pltpu.VMEM)
        outs = pl.pallas_call(
            kernel,
            out_shape=[
                pltpu.VMEM((2, micro * local_rows, model), BF16),
                pltpu.VMEM((total, 3, SLOTS, 16, width), BF16),
                pltpu.VMEM((GROUPS, 2, SLOTS, 16, depth), BF16),
                pltpu.VMEM((depth, GROUPS * SLOTS * 16), BF16),
            ],
            in_specs=[any_space] * 5,
            out_specs=[vmem] * 4,
            scratch_shapes=[
                pltpu.VMEM((chunks, depth, width), BF16),
                pltpu.VMEM((chunks, depth, width), BF16),
                pltpu.VMEM((chunks, width, depth), BF16),
                pltpu.VMEM((16, model), BF16),
                pltpu.VMEM((16, model), BF16),
                pltpu.VMEM((total, SLOTS, 3, 16, width), F32),
                pltpu.VMEM((total, 2, 3, 16, width), F32),
                pltpu.VMEM((total, 3, 16, width), F32),
                pltpu.VMEM((GROUPS, 2, SLOTS, 16, depth), F32),
                pltpu.VMEM((GROUPS - 1, 2, SLOTS, 16, depth), F32),
                pltpu.VMEM((2, SLOTS, 16, depth), BF16),
                dma((chunks, 3)),
                dma((2, 3)), dma((2, 3)),
                dma((3, 2, 2)), dma((3, 2, 2)),
                dma((total,)), dma((total,)),
                dma((total,)), dma((total,)),
                dma((total,)), dma((total,)),
                dma((total,)), dma((total,)),
                dma((total,)), dma((total,)),
                dma((3, 2, 2)), dma((3, 2, 2)),
                dma((2, 2, 3)), dma((2, 2, 3)),
                dma((2,)), dma((EARLY,)), dma((EARLY,)),
            ],
            compiler_params=pltpu.CompilerParams(collective_id=0, has_side_effects=True, vmem_limit_bytes=53 * 2**20),
        )(x_loc.reshape(micro * local_rows, model), dy_loc.reshape(micro * local_rows, model), w_gate_loc, w_up_loc, w_down_loc)
        y_rows, dx_rows, dw_gate, dw_up, dw_down = finish(*outs)
        return y_rows.reshape(x_loc.shape), dx_rows.reshape(x_loc.shape), dw_gate, dw_up, dw_down

    return jax.shard_map(local_step, mesh=mesh, in_specs=in_specs, out_specs=out_specs, check_vma=False)
```

```python
import jax
import jax.numpy as jnp
from jax import lax
from jax.experimental import pallas as pl
from jax.experimental.pallas import tpu as pltpu
from jax.sharding import PartitionSpec as P

MESH = pl.DeviceIdType.MESH
F32 = jnp.float32
BF16 = jnp.bfloat16
GROUPS = 4
SLOTS = 4
FINAL_LAG = 4
FORWARD_LAG = 11
BACK_LAG = 12
EARLY = 4


def dot(lhs, rhs):
    return lax.dot_general(lhs, rhs, (((1,), (0,)), ((), ())), preferred_element_type=F32)


def dot_t(lhs, rhs):
    return lax.dot_general(lhs, rhs, (((1,), (1,)), ((), ())), preferred_element_type=F32)


def make_kernel(chunks, width):
    total = GROUPS * chunks

    def kernel(x_hbm, dy_hbm, wg_hbm, wu_hbm, wd_hbm,
               rows, hid, cols, x_turned,
               wg, wu, wd, x_ref, dy_ref, part, near, far, acc, acc_in, tail,
               w_sem, first_send, first_recv, spread_send, spread_recv,
               near_send, near_recv, far_send, far_recv,
               hc_send, hc_recv, hx_send, hx_recv, hf_send, hf_recv,
               acc_send, acc_recv, tail_send, tail_recv, in_sem, open_send, open_recv, lead_send, lead_recv):
        tp = lax.axis_index("tp")
        dp = lax.axis_index("dp")
        z, y = tp // 2, tp % 2
        x, core = dp // 2, dp % 2
        ox, oc = 1 - x, 1 - core
        core_peer = {"tp": tp, "dp": x * 2 + oc}
        x_peer = {"tp": tp, "dp": ox * 2 + core}
        home = core * 2 + x
        owned = core * 2 + ox
        depth = cols.shape[-1]

        tp_peers = [{"tp": pz * 2 + py, "dp": dp} for pz, py in ((z, 1 - y), (1 - z, y), (1 - z, 1 - y))]
        rows_of = (pl.ds(0, 8), pl.ds(8, 8))

        def chunk_at(s):
            return jnp.where(s < EARLY, s, jnp.where(s < total - chunks + EARLY, s + chunks - EARLY, s + chunks - total))

        def dp_peer(k):
            px, pc = (x + k // 2) % 2, (core + k % 2) % 2
            return px * 2 + pc, pc * 2 + px

        def weight_copies(c):
            span = pl.ds(pl.multiple_of(c * width, width), width)
            return (pltpu.make_async_copy(wg_hbm.at[:, span], wg.at[c], w_sem.at[c, 0]),
                    pltpu.make_async_copy(wu_hbm.at[:, span], wu.at[c], w_sem.at[c, 1]),
                    pltpu.make_async_copy(wd_hbm.at[span], wd.at[c], w_sem.at[c, 2]))

        def remote(src, dst, send, recv, device):
            return pltpu.make_async_remote_copy(src_ref=src, dst_ref=dst, send_sem=send, recv_sem=recv,
                                                device_id=device, device_id_type=MESH)

        def first_copy(micro, kind, k):
            peer, _ = dp_peer(k)
            src = (x_ref, dy_ref)[kind].at[rows_of[micro], pl.ds(pl.multiple_of(peer * depth, depth), depth)]
            return remote(src, cols.at[0, kind, home, rows_of[micro]], first_send.at[micro, kind, k - 1], first_recv.at[micro, kind, k - 1],
                          {"tp": tp, "dp": peer})

        def spread_copies(group, kind):
            if group == 2:
                return [remote(cols.at[0, kind], cols.at[2, kind], spread_send.at[1, kind, 0], spread_recv.at[1, kind, 0], tp_peers[2])]
            return [remote(cols.at[0, kind, :, rows_of[group // 2]], cols.at[group, kind, :, rows_of[way]],
                           spread_send.at[group - 1, kind, way], spread_recv.at[group - 1, kind, way], tp_peers[way]) for way in range(2)]

        def lead_copies(far_side, kind):
            side = ox if far_side else x
            return [remote(cols.at[0, kind, core_slot * 2 + side, rows_of[0]], cols.at[1, kind, core_slot * 2 + side, rows_of[way]],
                           lead_send.at[far_side, kind, core_slot, way], lead_recv.at[far_side, kind, core_slot, way], tp_peers[way])
                    for core_slot in range(2) for way in range(2)]

        def near_copy(i):
            return remote(part.at[i, pl.ds(oc * 2, 2)], near.at[i], near_send.at[i], near_recv.at[i], core_peer)

        def open_copy(i, side, send, recv):
            return remote(part.at[i, oc * 2 + side], near.at[i, side], send.at[i], recv.at[i], core_peer)

        def here_copy(i):
            return open_copy(i, x, open_send, open_recv)

        def there_copy(i):
            return open_copy(i, ox, near_send, near_recv)

        def far_copy(i):
            return remote(near.at[i, x], far.at[i], far_send.at[i], far_recv.at[i], x_peer)

        def hc_copy(i):
            here = hid.at[i, :, owned]
            return remote(here, here, hc_send.at[i], hc_recv.at[i], core_peer)

        def hx_copy(i):
            here = hid.at[i, :, owned]
            return remote(here, here, hx_send.at[i], hx_recv.at[i], x_peer)

        def hf_copy(i):
            there = hid.at[i, :, home]
            return remote(there, there, hf_send.at[i], hf_recv.at[i], core_peer)

        def acc_copies(group):
            if group == 2:
                return [remote(acc.at[2], acc_in.at[2], acc_send.at[1, 0], acc_recv.at[1, 0], tp_peers[2])]
            return [remote(acc.at[group, :, :, rows_of[way]], acc_in.at[way, :, :, rows_of[group // 2]],
                           acc_send.at[group - 1, way], acc_recv.at[group - 1, way], tp_peers[way]) for way in range(2)]

        def tail_copy(kind, k):
            peer, slot = dp_peer(k)
            dst = rows.at[kind, :, pl.ds(pl.multiple_of(dp * depth, depth), depth)]
            return remote(tail.at[kind, slot], dst, tail_send.at[kind, k - 1], tail_recv.at[kind, k - 1], {"tp": tp, "dp": peer})

        barrier = pltpu.get_barrier_semaphore()
        for k in range(1, 4):
            pl.semaphore_signal(barrier, inc=1, device_id=tp_peers[k - 1], device_id_type=MESH)
            pl.semaphore_signal(barrier, inc=1, device_id={"tp": tp, "dp": dp_peer(k)[0]}, device_id_type=MESH)
        row_loads = [pltpu.make_async_copy(src, dst, in_sem.at[k]) for k, (src, dst) in enumerate(((x_hbm, x_ref), (dy_hbm, dy_ref)))]
        for copy in row_loads:
            copy.start()
        for c in range(chunks):
            for copy in weight_copies(c):
                copy.start()

        for copy in row_loads:
            copy.wait()
        pl.semaphore_wait(barrier, 6)

        for micro in range(2):
            for kind in range(2):
                for k in (1, 2, 3):
                    first_copy(micro, kind, k).start()
        own = pl.ds(pl.multiple_of(dp * depth, depth), depth)
        cols[0, 0, home] = x_ref[:, own]
        cols[0, 1, home] = dy_ref[:, own]
        acc[...] = jnp.zeros_like(acc)

        def half_products(i, side):
            rows_in = [jnp.concatenate([cols[0, kind, side], cols[0, kind, 2 + side]]) for kind in range(2)]
            for k, value in enumerate((dot(rows_in[0], wg[i]), dot(rows_in[0], wu[i]), dot_t(rows_in[1], wd[i]))):
                part[i, side, k] = value[:16]
                part[i, 2 + side, k] = value[16:]

        def half_sum(i, copy):
            copy.wait_recv()
            near[i, x] = near[i, x] + part[i, home]
            far_copy(i).start()

        for micro in range(2):
            for kind in range(2):
                first_copy(micro, kind, 1).wait_recv()
        for kind in range(2):
            for copy in lead_copies(0, kind):
                copy.start()

        def open_here(i, carry):
            for copy in weight_copies(i):
                copy.wait()
            half_products(i, x)
            here_copy(i).start()

            @pl.when(i > 0)
            def _():
                half_sum(i - 1, here_copy(i - 1))

            return carry

        lax.fori_loop(0, EARLY, open_here, 0)
        for kind in range(2):
            for k in (2, 3):
                first_copy(0, kind, k).wait_recv()
            for copy in lead_copies(1, kind):
                copy.start()
        half_sum(EARLY - 1, here_copy(EARLY - 1))

        for kind in range(2):
            for k in (2, 3):
                first_copy(1, kind, k).wait_recv()

        def open_there(i, carry):
            half_products(i, ox)
            there_copy(i).start()
            return carry

        lax.fori_loop(0, EARLY, open_there, 0)

        def products(i):
            group, c = i // chunks, i % chunks

            @pl.when(jnp.logical_and(group == 1, c >= EARLY))
            def _():
                for copy in weight_copies(c):
                    copy.wait()

            for other in (1, 2, 3):
                @pl.when(i == other * chunks)
                def _(other=other):
                    for kind in range(2):
                        for copy in spread_copies(other, kind) if other > 1 else lead_copies(0, kind) + lead_copies(1, kind):
                            copy.wait_recv()

            x_rows = cols[group, 0].reshape(SLOTS * 16, depth)
            dy_rows = cols[group, 1].reshape(SLOTS * 16, depth)
            for k, value in enumerate((dot(x_rows, wg[c]), dot(x_rows, wu[c]), dot_t(dy_rows, wd[c]))):
                for slot in range(SLOTS):
                    part[i, slot, k] = value[slot * 16:(slot + 1) * 16]
            near_copy(i).start()

        def activations(i):
            @pl.when(i < EARLY)
            def _():
                there_copy(i).wait_recv()

            far_copy(i).wait_recv()
            gate = part[i, owned, 0] + near[i, ox, 0] + far[i, 0]
            up = part[i, owned, 1] + near[i, ox, 1] + far[i, 1]
            grad = part[i, owned, 2] + near[i, ox, 2] + far[i, 2]
            sig = jax.nn.sigmoid(gate)
            act = gate * sig
            hid[i, 0, owned] = (act * up).astype(BF16)
            hid[i, 1, owned] = (grad * up * sig * (1.0 + gate * (1.0 - sig))).astype(BF16)
            hid[i, 2, owned] = (grad * act).astype(BF16)
            hc_copy(i).start()

        def back_rows(i, k):
            return hid[i, k].reshape(SLOTS * 16, width)

        def add_y(group, i, c):
            acc[group, 0] += dot(back_rows(i, 0), wd[c]).reshape(SLOTS, 16, depth)

        def add_dx(group, i, c):
            acc[group, 1] += (dot_t(back_rows(i, 1), wg[c]) + dot_t(back_rows(i, 2), wu[c])).reshape(SLOTS, 16, depth)

        def back(i):
            group, c = i // chunks, i % chunks
            hc_copy(i).wait_recv()
            hf_copy(i).wait_recv()
            add_y(group, i, c)
            add_dx(group, i, c)
            for other in (1, 2, 3):
                @pl.when(i == other * chunks + chunks - 1)
                def _(other=other):
                    for copy in acc_copies(other):
                        copy.start()

        def step(s, carry):
            @pl.when(s < total)
            def _():
                products(chunk_at(s))

            for other in (2, 3):
                @pl.when(s == EARLY + 3 * (other - 2))
                def _(other=other):
                    for kind in range(2):
                        for copy in spread_copies(other, kind):
                            copy.start()

            @pl.when(jnp.logical_and(s > EARLY, s < total + 1))
            def _():
                i = chunk_at(s - 1)
                half_sum(i, near_copy(i))

            @pl.when(jnp.logical_and(s >= FINAL_LAG, s < total + FINAL_LAG))
            def _():
                activations(chunk_at(s - FINAL_LAG))

            @pl.when(jnp.logical_and(s >= EARLY + FINAL_LAG, s < total - chunks + EARLY + FINAL_LAG))
            def _():
                hx_copy(s - FINAL_LAG + chunks - EARLY).start()

            @pl.when(s == total)
            def _():
                for c in range(EARLY):
                    hx_copy(c).start()

            @pl.when(jnp.logical_and(s >= total - chunks + EARLY + FINAL_LAG, s < total + FINAL_LAG))
            def _():
                hx_copy(s - FINAL_LAG + chunks - total).start()

            @pl.when(jnp.logical_and(s >= FORWARD_LAG, s < FORWARD_LAG + total))
            def _():
                i = (s - FORWARD_LAG + chunks) % total
                hx_copy(i).wait_recv()
                hf_copy(i).start()

            @pl.when(s == total - chunks)
            def _():
                x_turned[...] = cols[:, 0].reshape(GROUPS * SLOTS * 16, depth).T

            @pl.when(s >= BACK_LAG)
            def _():
                back((s - BACK_LAG + chunks) % total)

            return carry

        lax.fori_loop(EARLY, total + BACK_LAG - 1, step, 0)

        last = chunks - 1
        hc_copy(last).wait_recv()
        hf_copy(last).wait_recv()
        for kind in range(2):
            (add_y, add_dx)[kind](0, last, last)
            if kind == 0:
                for group in (1, 2, 3):
                    for copy in acc_copies(group):
                        copy.wait_recv()
            value = acc[0, kind] + acc_in[0, kind] + acc_in[1, kind] + acc_in[2, kind]
            tail[kind] = (cols[0, kind].astype(F32) + value).astype(BF16)
            for k in (2, 3, 1):
                tail_copy(kind, k).start()
        for kind in range(2):
            rows[kind, :, own] = tail[kind, home]

        for k in (1, 2, 3):
            for kind in range(2):
                spread = spread_copies(k, kind) if k > 1 else lead_copies(0, kind) + lead_copies(1, kind)
                for copy in [first_copy(0, kind, k), first_copy(1, kind, k)] + spread:
                    copy.wait_send()
            for copy in acc_copies(k):
                copy.wait_send()

        def drain(i, carry):
            @pl.when(i < EARLY)
            def _():
                here_copy(i).wait_send()
                there_copy(i).wait_send()

            @pl.when(i >= EARLY)
            def _():
                near_copy(i).wait_send()

            far_copy(i).wait_send()
            hc_copy(i).wait_send()
            hx_copy(i).wait_send()
            hf_copy(i).wait_send()
            return carry

        lax.fori_loop(0, total, drain, 0)
        for kind in range(2):
            for k in (1, 2, 3):
                tail_copy(kind, k).wait()

    return kernel, total


def finish(rows, hid, cols, x_turned):
    _, local_rows, model = rows.shape
    total, _, _, _, width = hid.shape
    depth, count = x_turned.shape
    chunks = total // GROUPS
    hidden = chunks * width
    ring = 4
    high = 128

    def kernel(rows_ref, hid_ref, cols_ref, x_ref, y_hbm, dx_hbm, dg_hbm, du_hbm, dd_hbm, g_tile, u_tile, d_tile, row_sem, out_sem):
        row_copies = [pltpu.make_async_copy(rows_ref.at[k], dst, row_sem.at[k]) for k, dst in enumerate((y_hbm, dx_hbm))]

        def all_rows(c, k):
            return jnp.concatenate([hid_ref[group * chunks + c, k].reshape(SLOTS * 16, width) for group in range(GROUPS)])

        def block(k, b):
            span = pl.ds(pl.multiple_of(b * high, high), high)
            return pltpu.make_async_copy((g_tile, u_tile)[k].at[b % ring], (dg_hbm, du_hbm)[k].at[span], out_sem.at[k, b % ring])

        def tile(c):
            span = pl.ds(pl.multiple_of(c * width, width), width)
            return pltpu.make_async_copy(d_tile.at[c % ring], dd_hbm.at[span], out_sem.at[2, c % ring])

        def across(b, carry):
            x_block = x_ref[pl.ds(pl.multiple_of(b * high, high), high)]
            for k, held in enumerate((g_tile, u_tile)):
                @pl.when(b >= ring)
                def _(k=k):
                    block(k, b - ring).wait()
                for c in range(chunks):
                    held[b % ring, :, c * width:(c + 1) * width] = dot(x_block, all_rows(c, k + 1))
                block(k, b).start()
            return carry

        def down(c, carry):
            @pl.when(c >= ring)
            def _():
                tile(c - ring).wait()
            d_tile[c % ring] = dot(all_rows(c, 0).T, cols_ref[:, 1].reshape(count, depth))
            tile(c).start()
            return carry

        lax.fori_loop(0, depth // high, across, 0)
        for copy in row_copies:
            copy.start()
        lax.fori_loop(0, chunks, down, 0)
        for b in range(depth // high - ring, depth // high):
            for k in range(2):
                block(k, b).wait()
        for c in range(chunks - ring, chunks):
            tile(c).wait()
        for copy in row_copies:
            copy.wait()

    dma = pltpu.SemaphoreType.DMA
    any_space = pl.BlockSpec(memory_space=pl.ANY)
    vmem = pl.BlockSpec(memory_space=pltpu.VMEM)
    row_shape = jax.ShapeDtypeStruct((local_rows, model), BF16)
    held = [pltpu.with_memory_space_constraint(value, pltpu.VMEM) for value in (rows, hid, cols, x_turned)]
    return pl.pallas_call(
        kernel,
        out_shape=[row_shape, row_shape, jax.ShapeDtypeStruct((depth, hidden), F32), jax.ShapeDtypeStruct((depth, hidden), F32), jax.ShapeDtypeStruct((hidden, depth), F32)],
        in_specs=[vmem] * 4,
        out_specs=[any_space] * 5,
        scratch_shapes=[
            pltpu.VMEM((ring, high, hidden), F32),
            pltpu.VMEM((ring, high, hidden), F32),
            pltpu.VMEM((ring, width, depth), F32),
            dma((2,)), dma((3, ring)),
        ],
        compiler_params=pltpu.CompilerParams(vmem_limit_bytes=40 * 2**20),
        cost_estimate=pl.CostEstimate(flops=6 * count * depth * hidden, bytes_accessed=12 * depth * hidden, transcendentals=0),
    )(*held)


def solution(mesh):
    row_spec = P(None, ("dp", "tp"), None)
    in_specs = (row_spec, P("dp", "tp"), P("dp", "tp"), P("tp", "dp"), row_spec)
    out_specs = (row_spec, row_spec, P("dp", "tp"), P("dp", "tp"), P("tp", "dp"))

    def local_step(x_loc, w_gate_loc, w_up_loc, w_down_loc, dy_loc):
        depth, hidden = w_gate_loc.shape
        micro, local_rows, model = x_loc.shape
        width = 512
        chunks = hidden // width
        kernel, total = make_kernel(chunks, width)
        dma = pltpu.SemaphoreType.DMA
        any_space = pl.BlockSpec(memory_space=pl.ANY)
        vmem = pl.BlockSpec(memory_space=pltpu.VMEM)
        outs = pl.pallas_call(
            kernel,
            out_shape=[
                pltpu.VMEM((2, micro * local_rows, model), BF16),
                pltpu.VMEM((total, 3, SLOTS, 16, width), BF16),
                pltpu.VMEM((GROUPS, 2, SLOTS, 16, depth), BF16),
                pltpu.VMEM((depth, GROUPS * SLOTS * 16), BF16),
            ],
            in_specs=[any_space] * 5,
            out_specs=[vmem] * 4,
            scratch_shapes=[
                pltpu.VMEM((chunks, depth, width), BF16),
                pltpu.VMEM((chunks, depth, width), BF16),
                pltpu.VMEM((chunks, width, depth), BF16),
                pltpu.VMEM((16, model), BF16),
                pltpu.VMEM((16, model), BF16),
                pltpu.VMEM((total, SLOTS, 3, 16, width), F32),
                pltpu.VMEM((total, 2, 3, 16, width), F32),
                pltpu.VMEM((total, 3, 16, width), F32),
                pltpu.VMEM((GROUPS, 2, SLOTS, 16, depth), F32),
                pltpu.VMEM((GROUPS - 1, 2, SLOTS, 16, depth), F32),
                pltpu.VMEM((2, SLOTS, 16, depth), BF16),
                dma((chunks, 3)),
                dma((2, 2, 3)), dma((2, 2, 3)),
                dma((3, 2, 2)), dma((3, 2, 2)),
                dma((total,)), dma((total,)),
                dma((total,)), dma((total,)),
                dma((total,)), dma((total,)),
                dma((total,)), dma((total,)),
                dma((total,)), dma((total,)),
                dma((3, 2)), dma((3, 2)),
                dma((2, 3)), dma((2, 3)),
                dma((2,)), dma((EARLY,)), dma((EARLY,)),
                dma((2, 2, 2, 2)), dma((2, 2, 2, 2)),
            ],
            compiler_params=pltpu.CompilerParams(collective_id=0, has_side_effects=True, vmem_limit_bytes=53 * 2**20),
        )(x_loc.reshape(micro * local_rows, model), dy_loc.reshape(micro * local_rows, model), w_gate_loc, w_up_loc, w_down_loc)
        y_rows, dx_rows, dw_gate, dw_up, dw_down = finish(*outs)
        return y_rows.reshape(x_loc.shape), dx_rows.reshape(x_loc.shape), dw_gate, dw_up, dw_down

    return jax.shard_map(local_step, mesh=mesh, in_specs=in_specs, out_specs=out_specs, check_vma=False)
```

```python
import jax
import jax.numpy as jnp
from jax import lax
from jax.experimental import pallas as pl
from jax.experimental.pallas import tpu as pltpu
from jax.sharding import PartitionSpec as P

MESH = pl.DeviceIdType.MESH
F32 = jnp.float32
BF16 = jnp.bfloat16
GROUPS = 4
SLOTS = 4
FINAL_LAG = 4
FORWARD_LAG = 10
BACK_LAG = 11
EARLY = 4


def dot(lhs, rhs):
    return lax.dot_general(lhs, rhs, (((1,), (0,)), ((), ())), preferred_element_type=F32)


def dot_t(lhs, rhs):
    return lax.dot_general(lhs, rhs, (((1,), (1,)), ((), ())), preferred_element_type=F32)


def make_kernel(chunks, width):
    total = GROUPS * chunks

    def kernel(x_hbm, dy_hbm, wg_hbm, wu_hbm, wd_hbm,
               rows, hid, cols, x_turned,
               wg, wu, wd, x_ref, dy_ref, part, near, far, acc, acc_in, tail,
               w_sem, first_send, first_recv, spread_send, spread_recv,
               near_send, near_recv, far_send, far_recv,
               hc_send, hc_recv, hx_send, hx_recv, hf_send, hf_recv,
               acc_send, acc_recv, tail_send, tail_recv, in_sem, open_send, open_recv, lead_send, lead_recv):
        tp = lax.axis_index("tp")
        dp = lax.axis_index("dp")
        z, y = tp // 2, tp % 2
        x, core = dp // 2, dp % 2
        ox, oc = 1 - x, 1 - core
        core_peer = {"tp": tp, "dp": x * 2 + oc}
        x_peer = {"tp": tp, "dp": ox * 2 + core}
        home = core * 2 + x
        owned = core * 2 + ox
        depth = cols.shape[-1]

        tp_peers = [{"tp": pz * 2 + py, "dp": dp} for pz, py in ((z, 1 - y), (1 - z, y), (1 - z, 1 - y))]
        rows_of = (pl.ds(0, 8), pl.ds(8, 8))

        def chunk_at(s):
            return jnp.where(s < EARLY, s, jnp.where(s < total - chunks + EARLY, s + chunks - EARLY, s + chunks - total))

        def dp_peer(k):
            px, pc = (x + k // 2) % 2, (core + k % 2) % 2
            return px * 2 + pc, pc * 2 + px

        def weight_copies(c):
            span = pl.ds(pl.multiple_of(c * width, width), width)
            return (pltpu.make_async_copy(wg_hbm.at[:, span], wg.at[c], w_sem.at[c, 0]),
                    pltpu.make_async_copy(wu_hbm.at[:, span], wu.at[c], w_sem.at[c, 1]),
                    pltpu.make_async_copy(wd_hbm.at[span], wd.at[c], w_sem.at[c, 2]))

        def remote(src, dst, send, recv, device):
            return pltpu.make_async_remote_copy(src_ref=src, dst_ref=dst, send_sem=send, recv_sem=recv,
                                                device_id=device, device_id_type=MESH)

        def first_copy(micro, kind, k):
            peer, _ = dp_peer(k)
            src = (x_ref, dy_ref)[kind].at[rows_of[micro], pl.ds(pl.multiple_of(peer * depth, depth), depth)]
            return remote(src, cols.at[0, kind, home, rows_of[micro]], first_send.at[micro, kind, k - 1], first_recv.at[micro, kind, k - 1],
                          {"tp": tp, "dp": peer})

        def spread_copies(group, kind):
            if group == 2:
                return [remote(cols.at[0, kind], cols.at[2, kind], spread_send.at[1, kind, 0], spread_recv.at[1, kind, 0], tp_peers[2])]
            return [remote(cols.at[0, kind, :, rows_of[group // 2]], cols.at[group, kind, :, rows_of[way]],
                           spread_send.at[group - 1, kind, way], spread_recv.at[group - 1, kind, way], tp_peers[way]) for way in range(2)]

        def lead_copies(far_side, kind):
            side = ox if far_side else x
            return [remote(cols.at[0, kind, core_slot * 2 + side, rows_of[0]], cols.at[1, kind, core_slot * 2 + side, rows_of[way]],
                           lead_send.at[far_side, kind, core_slot, way], lead_recv.at[far_side, kind, core_slot, way], tp_peers[way])
                    for core_slot in range(2) for way in range(2)]

        def near_copy(i):
            return remote(part.at[i, pl.ds(oc * 2, 2)], near.at[i], near_send.at[i], near_recv.at[i], core_peer)

        def open_copy(i, side, send, recv):
            return remote(part.at[i, oc * 2 + side], near.at[i, side], send.at[i], recv.at[i], core_peer)

        def here_copy(i):
            return open_copy(i, x, open_send, open_recv)

        def there_copy(i):
            return open_copy(i, ox, near_send, near_recv)

        def far_copy(i):
            return remote(near.at[i, x], far.at[i], far_send.at[i], far_recv.at[i], x_peer)

        def hc_copy(i):
            here = hid.at[i, :, owned]
            return remote(here, here, hc_send.at[i], hc_recv.at[i], core_peer)

        def hx_copy(i):
            here = hid.at[i, :, owned]
            return remote(here, here, hx_send.at[i], hx_recv.at[i], x_peer)

        def hf_copy(i):
            there = hid.at[i, :, home]
            return remote(there, there, hf_send.at[i], hf_recv.at[i], core_peer)

        def acc_copies(group):
            if group == 2:
                return [remote(acc.at[2], acc_in.at[2], acc_send.at[1, 0], acc_recv.at[1, 0], tp_peers[2])]
            return [remote(acc.at[group, :, :, rows_of[way]], acc_in.at[way, :, :, rows_of[group // 2]],
                           acc_send.at[group - 1, way], acc_recv.at[group - 1, way], tp_peers[way]) for way in range(2)]

        def tail_copy(kind, k):
            peer, slot = dp_peer(k)
            dst = rows.at[kind, :, pl.ds(pl.multiple_of(dp * depth, depth), depth)]
            return remote(tail.at[kind, slot], dst, tail_send.at[kind, k - 1], tail_recv.at[kind, k - 1], {"tp": tp, "dp": peer})

        barrier = pltpu.get_barrier_semaphore()
        for k in range(1, 4):
            pl.semaphore_signal(barrier, inc=1, device_id=tp_peers[k - 1], device_id_type=MESH)
            pl.semaphore_signal(barrier, inc=1, device_id={"tp": tp, "dp": dp_peer(k)[0]}, device_id_type=MESH)
        row_loads = [pltpu.make_async_copy(src, dst, in_sem.at[k]) for k, (src, dst) in enumerate(((x_hbm, x_ref), (dy_hbm, dy_ref)))]
        for copy in row_loads:
            copy.start()
        for c in range(chunks):
            for copy in weight_copies(c):
                copy.start()

        for copy in row_loads:
            copy.wait()
        pl.semaphore_wait(barrier, 6)

        for micro in range(2):
            for kind in range(2):
                for k in (1, 2, 3):
                    first_copy(micro, kind, k).start()
        own = pl.ds(pl.multiple_of(dp * depth, depth), depth)
        cols[0, 0, home] = x_ref[:, own]
        cols[0, 1, home] = dy_ref[:, own]
        acc[...] = jnp.zeros_like(acc)

        def half_products(i, side):
            rows_in = [jnp.concatenate([cols[0, kind, side], cols[0, kind, 2 + side]]) for kind in range(2)]
            for k, value in enumerate((dot(rows_in[0], wg[i]), dot(rows_in[0], wu[i]), dot_t(rows_in[1], wd[i]))):
                part[i, side, k] = value[:16]
                part[i, 2 + side, k] = value[16:]

        def half_sum(i, copy):
            copy.wait_recv()
            near[i, x] = near[i, x] + part[i, home]
            far_copy(i).start()

        for micro in range(2):
            for kind in range(2):
                first_copy(micro, kind, 1).wait_recv()
        for kind in range(2):
            for copy in lead_copies(0, kind):
                copy.start()

        def open_here(i, carry):
            for copy in weight_copies(i):
                copy.wait()
            half_products(i, x)
            here_copy(i).start()

            @pl.when(i > 0)
            def _():
                half_sum(i - 1, here_copy(i - 1))

            return carry

        lax.fori_loop(0, EARLY, open_here, 0)
        for kind in range(2):
            for k in (2, 3):
                first_copy(0, kind, k).wait_recv()
            for copy in lead_copies(1, kind):
                copy.start()
        half_sum(EARLY - 1, here_copy(EARLY - 1))

        for kind in range(2):
            for k in (2, 3):
                first_copy(1, kind, k).wait_recv()

        def open_there(i, carry):
            half_products(i, ox)
            there_copy(i).start()
            return carry

        lax.fori_loop(0, EARLY, open_there, 0)

        def products(i):
            group, c = i // chunks, i % chunks

            @pl.when(jnp.logical_and(group == 1, c >= EARLY))
            def _():
                for copy in weight_copies(c):
                    copy.wait()

            for other in (1, 2, 3):
                @pl.when(i == other * chunks)
                def _(other=other):
                    for kind in range(2):
                        for copy in spread_copies(other, kind) if other > 1 else lead_copies(0, kind) + lead_copies(1, kind):
                            copy.wait_recv()

            x_rows = cols[group, 0].reshape(SLOTS * 16, depth)
            dy_rows = cols[group, 1].reshape(SLOTS * 16, depth)
            for k, value in enumerate((dot(x_rows, wg[c]), dot(x_rows, wu[c]), dot_t(dy_rows, wd[c]))):
                for slot in range(SLOTS):
                    part[i, slot, k] = value[slot * 16:(slot + 1) * 16]
            near_copy(i).start()

        def activations(i):
            @pl.when(i < EARLY)
            def _():
                there_copy(i).wait_recv()

            far_copy(i).wait_recv()
            gate = part[i, owned, 0] + near[i, ox, 0] + far[i, 0]
            up = part[i, owned, 1] + near[i, ox, 1] + far[i, 1]
            grad = part[i, owned, 2] + near[i, ox, 2] + far[i, 2]
            sig = jax.nn.sigmoid(gate)
            act = gate * sig
            hid[i, 0, owned] = (act * up).astype(BF16)
            hid[i, 1, owned] = (grad * up * sig * (1.0 + gate * (1.0 - sig))).astype(BF16)
            hid[i, 2, owned] = (grad * act).astype(BF16)
            hc_copy(i).start()

        def back_rows(i, k):
            return hid[i, k].reshape(SLOTS * 16, width)

        def add_y(group, i, c):
            acc[group, 0] += dot(back_rows(i, 0), wd[c]).reshape(SLOTS, 16, depth)

        def add_dx(group, i, c):
            acc[group, 1] += (dot_t(back_rows(i, 1), wg[c]) + dot_t(back_rows(i, 2), wu[c])).reshape(SLOTS, 16, depth)

        def back(i):
            group, c = i // chunks, i % chunks
            hc_copy(i).wait_recv()
            hf_copy(i).wait_recv()
            add_y(group, i, c)
            add_dx(group, i, c)
            for other in (1, 2, 3):
                @pl.when(i == other * chunks + chunks - 1)
                def _(other=other):
                    for copy in acc_copies(other):
                        copy.start()

        def step(s, carry):
            @pl.when(s < total)
            def _():
                products(chunk_at(s))

            for other in (2, 3):
                @pl.when(s == EARLY + 3 * (other - 2))
                def _(other=other):
                    for kind in range(2):
                        for copy in spread_copies(other, kind):
                            copy.start()

            @pl.when(jnp.logical_and(s > EARLY, s < total + 1))
            def _():
                i = chunk_at(s - 1)
                half_sum(i, near_copy(i))

            @pl.when(jnp.logical_and(s >= FINAL_LAG, s < total + FINAL_LAG))
            def _():
                activations(chunk_at(s - FINAL_LAG))

            @pl.when(jnp.logical_and(s >= EARLY + FINAL_LAG, s < total - chunks + EARLY + FINAL_LAG))
            def _():
                hx_copy(s - FINAL_LAG + chunks - EARLY).start()

            @pl.when(s == total)
            def _():
                for c in range(EARLY):
                    hx_copy(c).start()

            @pl.when(jnp.logical_and(s >= total - chunks + EARLY + FINAL_LAG, s < total + FINAL_LAG))
            def _():
                hx_copy(s - FINAL_LAG + chunks - total).start()

            @pl.when(jnp.logical_and(s >= FORWARD_LAG, s < FORWARD_LAG + total))
            def _():
                i = (s - FORWARD_LAG + chunks) % total
                hx_copy(i).wait_recv()
                hf_copy(i).start()

            @pl.when(s == total - chunks)
            def _():
                x_turned[...] = cols[:, 0].reshape(GROUPS * SLOTS * 16, depth).T

            @pl.when(s >= BACK_LAG)
            def _():
                back((s - BACK_LAG + chunks) % total)

            return carry

        lax.fori_loop(EARLY, total + BACK_LAG - 1, step, 0)

        last = chunks - 1
        hc_copy(last).wait_recv()
        hf_copy(last).wait_recv()
        for kind in range(2):
            (add_y, add_dx)[kind](0, last, last)
            if kind == 0:
                for group in (1, 2, 3):
                    for copy in acc_copies(group):
                        copy.wait_recv()
            value = acc[0, kind] + acc_in[0, kind] + acc_in[1, kind] + acc_in[2, kind]
            tail[kind] = (cols[0, kind].astype(F32) + value).astype(BF16)
            for k in (2, 3, 1):
                tail_copy(kind, k).start()
        for kind in range(2):
            rows[kind, :, own] = tail[kind, home]

        for k in (1, 2, 3):
            for kind in range(2):
                spread = spread_copies(k, kind) if k > 1 else lead_copies(0, kind) + lead_copies(1, kind)
                for copy in [first_copy(0, kind, k), first_copy(1, kind, k)] + spread:
                    copy.wait_send()
            for copy in acc_copies(k):
                copy.wait_send()

        def drain(i, carry):
            @pl.when(i < EARLY)
            def _():
                here_copy(i).wait_send()
                there_copy(i).wait_send()

            @pl.when(i >= EARLY)
            def _():
                near_copy(i).wait_send()

            far_copy(i).wait_send()
            hc_copy(i).wait_send()
            hx_copy(i).wait_send()
            hf_copy(i).wait_send()
            return carry

        lax.fori_loop(0, total, drain, 0)
        for kind in range(2):
            for k in (1, 2, 3):
                tail_copy(kind, k).wait()

    return kernel, total


def finish(rows, hid, cols, x_turned):
    _, local_rows, model = rows.shape
    total, _, _, _, width = hid.shape
    depth, count = x_turned.shape
    chunks = total // GROUPS
    hidden = chunks * width
    ring = 4
    high = 128

    def kernel(rows_ref, hid_ref, cols_ref, x_ref, y_hbm, dx_hbm, dg_hbm, du_hbm, dd_hbm, g_tile, u_tile, d_tile, row_sem, out_sem):
        row_copies = [pltpu.make_async_copy(rows_ref.at[k], dst, row_sem.at[k]) for k, dst in enumerate((y_hbm, dx_hbm))]

        def all_rows(c, k):
            return jnp.concatenate([hid_ref[group * chunks + c, k].reshape(SLOTS * 16, width) for group in range(GROUPS)])

        def block(k, b):
            span = pl.ds(pl.multiple_of(b * high, high), high)
            return pltpu.make_async_copy((g_tile, u_tile)[k].at[b % ring], (dg_hbm, du_hbm)[k].at[span], out_sem.at[k, b % ring])

        def tile(c):
            span = pl.ds(pl.multiple_of(c * width, width), width)
            return pltpu.make_async_copy(d_tile.at[c % ring], dd_hbm.at[span], out_sem.at[2, c % ring])

        def across(b, carry):
            x_block = x_ref[pl.ds(pl.multiple_of(b * high, high), high)]
            for k, held in enumerate((g_tile, u_tile)):
                @pl.when(b >= ring)
                def _(k=k):
                    block(k, b - ring).wait()
                for c in range(chunks):
                    held[b % ring, :, c * width:(c + 1) * width] = dot(x_block, all_rows(c, k + 1))
                block(k, b).start()
            return carry

        def down(c, carry):
            @pl.when(c >= ring)
            def _():
                tile(c - ring).wait()
            d_tile[c % ring] = dot(all_rows(c, 0).T, cols_ref[:, 1].reshape(count, depth))
            tile(c).start()
            return carry

        lax.fori_loop(0, depth // high, across, 0)
        for copy in row_copies:
            copy.start()
        lax.fori_loop(0, chunks, down, 0)
        for b in range(depth // high - ring, depth // high):
            for k in range(2):
                block(k, b).wait()
        for c in range(chunks - ring, chunks):
            tile(c).wait()
        for copy in row_copies:
            copy.wait()

    dma = pltpu.SemaphoreType.DMA
    any_space = pl.BlockSpec(memory_space=pl.ANY)
    vmem = pl.BlockSpec(memory_space=pltpu.VMEM)
    row_shape = jax.ShapeDtypeStruct((local_rows, model), BF16)
    held = [pltpu.with_memory_space_constraint(value, pltpu.VMEM) for value in (rows, hid, cols, x_turned)]
    return pl.pallas_call(
        kernel,
        out_shape=[row_shape, row_shape, jax.ShapeDtypeStruct((depth, hidden), F32), jax.ShapeDtypeStruct((depth, hidden), F32), jax.ShapeDtypeStruct((hidden, depth), F32)],
        in_specs=[vmem] * 4,
        out_specs=[any_space] * 5,
        scratch_shapes=[
            pltpu.VMEM((ring, high, hidden), F32),
            pltpu.VMEM((ring, high, hidden), F32),
            pltpu.VMEM((ring, width, depth), F32),
            dma((2,)), dma((3, ring)),
        ],
        compiler_params=pltpu.CompilerParams(vmem_limit_bytes=40 * 2**20),
        cost_estimate=pl.CostEstimate(flops=6 * count * depth * hidden, bytes_accessed=12 * depth * hidden, transcendentals=0),
    )(*held)


def solution(mesh):
    row_spec = P(None, ("dp", "tp"), None)
    in_specs = (row_spec, P("dp", "tp"), P("dp", "tp"), P("tp", "dp"), row_spec)
    out_specs = (row_spec, row_spec, P("dp", "tp"), P("dp", "tp"), P("tp", "dp"))

    def local_step(x_loc, w_gate_loc, w_up_loc, w_down_loc, dy_loc):
        depth, hidden = w_gate_loc.shape
        micro, local_rows, model = x_loc.shape
        width = 512
        chunks = hidden // width
        kernel, total = make_kernel(chunks, width)
        dma = pltpu.SemaphoreType.DMA
        any_space = pl.BlockSpec(memory_space=pl.ANY)
        vmem = pl.BlockSpec(memory_space=pltpu.VMEM)
        outs = pl.pallas_call(
            kernel,
            out_shape=[
                pltpu.VMEM((2, micro * local_rows, model), BF16),
                pltpu.VMEM((total, 3, SLOTS, 16, width), BF16),
                pltpu.VMEM((GROUPS, 2, SLOTS, 16, depth), BF16),
                pltpu.VMEM((depth, GROUPS * SLOTS * 16), BF16),
            ],
            in_specs=[any_space] * 5,
            out_specs=[vmem] * 4,
            scratch_shapes=[
                pltpu.VMEM((chunks, depth, width), BF16),
                pltpu.VMEM((chunks, depth, width), BF16),
                pltpu.VMEM((chunks, width, depth), BF16),
                pltpu.VMEM((16, model), BF16),
                pltpu.VMEM((16, model), BF16),
                pltpu.VMEM((total, SLOTS, 3, 16, width), F32),
                pltpu.VMEM((total, 2, 3, 16, width), F32),
                pltpu.VMEM((total, 3, 16, width), F32),
                pltpu.VMEM((GROUPS, 2, SLOTS, 16, depth), F32),
                pltpu.VMEM((GROUPS - 1, 2, SLOTS, 16, depth), F32),
                pltpu.VMEM((2, SLOTS, 16, depth), BF16),
                dma((chunks, 3)),
                dma((2, 2, 3)), dma((2, 2, 3)),
                dma((3, 2, 2)), dma((3, 2, 2)),
                dma((total,)), dma((total,)),
                dma((total,)), dma((total,)),
                dma((total,)), dma((total,)),
                dma((total,)), dma((total,)),
                dma((total,)), dma((total,)),
                dma((3, 2)), dma((3, 2)),
                dma((2, 3)), dma((2, 3)),
                dma((2,)), dma((EARLY,)), dma((EARLY,)),
                dma((2, 2, 2, 2)), dma((2, 2, 2, 2)),
            ],
            compiler_params=pltpu.CompilerParams(collective_id=0, has_side_effects=True, vmem_limit_bytes=53 * 2**20),
        )(x_loc.reshape(micro * local_rows, model), dy_loc.reshape(micro * local_rows, model), w_gate_loc, w_up_loc, w_down_loc)
        y_rows, dx_rows, dw_gate, dw_up, dw_down = finish(*outs)
        return y_rows.reshape(x_loc.shape), dx_rows.reshape(x_loc.shape), dw_gate, dw_up, dw_down

    return jax.shard_map(local_step, mesh=mesh, in_specs=in_specs, out_specs=out_specs, check_vma=False)
```

```python
import jax
import jax.numpy as jnp
from jax import lax
from jax.experimental import pallas as pl
from jax.experimental.pallas import tpu as pltpu
from jax.sharding import PartitionSpec as P

MESH = pl.DeviceIdType.MESH
F32 = jnp.float32
BF16 = jnp.bfloat16
GROUPS = 4
SLOTS = 4
FINAL_LAG = 4
FORWARD_LAG = 10
BACK_LAG = 11
EARLY = 4


def dot(lhs, rhs):
    return lax.dot_general(lhs, rhs, (((1,), (0,)), ((), ())), preferred_element_type=F32)


def dot_t(lhs, rhs):
    return lax.dot_general(lhs, rhs, (((1,), (1,)), ((), ())), preferred_element_type=F32)


def make_kernel(chunks, width):
    total = GROUPS * chunks

    def kernel(x_hbm, dy_hbm, wg_hbm, wu_hbm, wd_hbm,
               rows, hid, cols, x_turned,
               wg, wu, wd, x_ref, dy_ref, part, near, far, acc, acc_in, tail,
               w_sem, first_send, first_recv, spread_send, spread_recv,
               near_send, near_recv, far_send, far_recv,
               hc_send, hc_recv, hx_send, hx_recv, hf_send, hf_recv,
               acc_send, acc_recv, tail_send, tail_recv, in_sem, open_recv, lead_send, lead_recv):
        tp = lax.axis_index("tp")
        dp = lax.axis_index("dp")
        z, y = tp // 2, tp % 2
        x, core = dp // 2, dp % 2
        ox, oc = 1 - x, 1 - core
        core_peer = {"tp": tp, "dp": x * 2 + oc}
        x_peer = {"tp": tp, "dp": ox * 2 + core}
        home = core * 2 + x
        owned = core * 2 + ox
        depth = cols.shape[-1]

        tp_peers = [{"tp": pz * 2 + py, "dp": dp} for pz, py in ((z, 1 - y), (1 - z, y), (1 - z, 1 - y))]
        rows_of = (pl.ds(0, 8), pl.ds(8, 8))

        def place(i):
            return jnp.where(i < EARLY, i, jnp.where(i < chunks, i + total - chunks, i - chunks + EARLY))

        def turn(i):
            return (i + total - chunks) % total

        def chunk_at(s):
            return jnp.where(s < EARLY, s, jnp.where(s < total - chunks + EARLY, s + chunks - EARLY, s + chunks - total))

        def dp_peer(k):
            px, pc = (x + k // 2) % 2, (core + k % 2) % 2
            return px * 2 + pc, pc * 2 + px

        def weight_copies(c):
            span = pl.ds(pl.multiple_of(c * width, width), width)
            return (pltpu.make_async_copy(wg_hbm.at[:, span], wg.at[c], w_sem.at[c, 0]),
                    pltpu.make_async_copy(wu_hbm.at[:, span], wu.at[c], w_sem.at[c, 1]),
                    pltpu.make_async_copy(wd_hbm.at[span], wd.at[c], w_sem.at[c, 2]))

        def remote(src, dst, send, recv, device):
            return pltpu.make_async_remote_copy(src_ref=src, dst_ref=dst, send_sem=send, recv_sem=recv,
                                                device_id=device, device_id_type=MESH)

        def first_copy(micro, kind, k):
            peer, _ = dp_peer(k)
            src = (x_ref, dy_ref)[kind].at[rows_of[micro], pl.ds(pl.multiple_of(peer * depth, depth), depth)]
            return remote(src, cols.at[0, kind, home, rows_of[micro]], first_send.at[0], first_recv.at[0 if k == 1 else 1 + micro],
                          {"tp": tp, "dp": peer})

        def spread_copies(group, kind):
            if group == 2:
                return [remote(cols.at[0, kind], cols.at[2, kind], spread_send.at[0], spread_recv.at[0], tp_peers[2])]
            return [remote(cols.at[0, kind, :, rows_of[group // 2]], cols.at[group, kind, :, rows_of[way]],
                           spread_send.at[0], spread_recv.at[1], tp_peers[way]) for way in range(2)]

        def lead_copies(far_side, kind):
            side = ox if far_side else x
            return [remote(cols.at[0, kind, core_slot * 2 + side, rows_of[0]], cols.at[1, kind, core_slot * 2 + side, rows_of[way]],
                           lead_send.at[0], lead_recv.at[0], tp_peers[way])
                    for core_slot in range(2) for way in range(2)]

        def near_copy(i):
            return remote(part.at[i, pl.ds(oc * 2, 2)], near.at[i], near_send.at[0], near_recv.at[place(i) % 8], core_peer)

        def open_copy(i, side, recv):
            return remote(part.at[i, oc * 2 + side], near.at[i, side], near_send.at[0], recv, core_peer)

        def here_copy(i):
            return open_copy(i, x, open_recv.at[i])

        def there_copy(i):
            return open_copy(i, ox, near_recv.at[i % 8])

        def far_copy(i):
            return remote(near.at[i, x], far.at[i], far_send.at[0], far_recv.at[place(i) % 10], x_peer)

        def hc_copy(i):
            here = hid.at[i, :, owned]
            return remote(here, here, hc_send.at[0], hc_recv.at[jnp.where(i < EARLY, i, EARLY + turn(i) % 12)], core_peer)

        def hx_copy(i):
            here = hid.at[i, :, owned]
            return remote(here, here, hx_send.at[0], hx_recv.at[turn(i) % 12], x_peer)

        def hf_copy(i):
            there = hid.at[i, :, home]
            return remote(there, there, hf_send.at[0], hf_recv.at[turn(i) % 8], core_peer)

        def acc_copies(group):
            if group == 2:
                return [remote(acc.at[2], acc_in.at[2], acc_send.at[0], acc_recv.at[0], tp_peers[2])]
            return [remote(acc.at[group, :, :, rows_of[way]], acc_in.at[way, :, :, rows_of[group // 2]],
                           acc_send.at[0], acc_recv.at[0], tp_peers[way]) for way in range(2)]

        def tail_copy(kind, k):
            peer, slot = dp_peer(k)
            dst = rows.at[kind, :, pl.ds(pl.multiple_of(dp * depth, depth), depth)]
            return remote(tail.at[kind, slot], dst, tail_send.at[0], tail_recv.at[0], {"tp": tp, "dp": peer})

        barrier = pltpu.get_barrier_semaphore()
        for k in range(1, 4):
            pl.semaphore_signal(barrier, inc=1, device_id=tp_peers[k - 1], device_id_type=MESH)
            pl.semaphore_signal(barrier, inc=1, device_id={"tp": tp, "dp": dp_peer(k)[0]}, device_id_type=MESH)
        row_loads = [pltpu.make_async_copy(src, dst, in_sem.at[k]) for k, (src, dst) in enumerate(((x_hbm, x_ref), (dy_hbm, dy_ref)))]
        for copy in row_loads:
            copy.start()
        for c in range(chunks):
            for copy in weight_copies(c):
                copy.start()

        for copy in row_loads:
            copy.wait()
        pl.semaphore_wait(barrier, 6)

        for micro in range(2):
            for kind in range(2):
                for k in (1, 2, 3):
                    first_copy(micro, kind, k).start()
        own = pl.ds(pl.multiple_of(dp * depth, depth), depth)
        cols[0, 0, home] = x_ref[:, own]
        cols[0, 1, home] = dy_ref[:, own]
        acc[...] = jnp.zeros_like(acc)

        def half_products(i, side):
            rows_in = [jnp.concatenate([cols[0, kind, side], cols[0, kind, 2 + side]]) for kind in range(2)]
            for k, value in enumerate((dot(rows_in[0], wg[i]), dot(rows_in[0], wu[i]), dot_t(rows_in[1], wd[i]))):
                part[i, side, k] = value[:16]
                part[i, 2 + side, k] = value[16:]

        def half_sum(i, copy):
            copy.wait_recv()
            near[i, x] = near[i, x] + part[i, home]
            far_copy(i).start()

        def took(ref, recv):
            remote(ref, ref, recv, recv, core_peer).wait_recv()

        def sent(ref, send):
            remote(ref, ref, send, send, core_peer).wait_send()

        took(cols.at[0, :, 0], first_recv.at[0])
        for kind in range(2):
            for copy in lead_copies(0, kind):
                copy.start()

        def open_here(i, carry):
            for copy in weight_copies(i):
                copy.wait()
            half_products(i, x)
            here_copy(i).start()

            @pl.when(i > 0)
            def _():
                half_sum(i - 1, here_copy(i - 1))

            return carry

        lax.fori_loop(0, EARLY, open_here, 0)
        took(cols.at[0, :, 0], first_recv.at[1])
        for kind in range(2):
            for copy in lead_copies(1, kind):
                copy.start()
        half_sum(EARLY - 1, here_copy(EARLY - 1))

        took(cols.at[0, :, 0], first_recv.at[2])

        def open_there(i, carry):
            half_products(i, ox)
            there_copy(i).start()
            return carry

        lax.fori_loop(0, EARLY, open_there, 0)

        def products(i):
            group, c = i // chunks, i % chunks

            @pl.when(jnp.logical_and(group == 1, c >= EARLY))
            def _():
                for copy in weight_copies(c):
                    copy.wait()

            for other in (1, 2, 3):
                @pl.when(i == other * chunks)
                def _(other=other):
                    took(cols.at[other], lead_recv.at[0] if other == 1 else spread_recv.at[other - 2])

            x_rows = cols[group, 0].reshape(SLOTS * 16, depth)
            dy_rows = cols[group, 1].reshape(SLOTS * 16, depth)
            for k, value in enumerate((dot(x_rows, wg[c]), dot(x_rows, wu[c]), dot_t(dy_rows, wd[c]))):
                for slot in range(SLOTS):
                    part[i, slot, k] = value[slot * 16:(slot + 1) * 16]
            near_copy(i).start()

        def activations(i):
            @pl.when(i < EARLY)
            def _():
                there_copy(i).wait_recv()

            far_copy(i).wait_recv()
            gate = part[i, owned, 0] + near[i, ox, 0] + far[i, 0]
            up = part[i, owned, 1] + near[i, ox, 1] + far[i, 1]
            grad = part[i, owned, 2] + near[i, ox, 2] + far[i, 2]
            sig = jax.nn.sigmoid(gate)
            act = gate * sig
            hid[i, 0, owned] = (act * up).astype(BF16)
            hid[i, 1, owned] = (grad * up * sig * (1.0 + gate * (1.0 - sig))).astype(BF16)
            hid[i, 2, owned] = (grad * act).astype(BF16)
            hc_copy(i).start()

        def back_rows(i, k):
            return hid[i, k].reshape(SLOTS * 16, width)

        def add_y(group, i, c):
            acc[group, 0] += dot(back_rows(i, 0), wd[c]).reshape(SLOTS, 16, depth)

        def add_dx(group, i, c):
            acc[group, 1] += (dot_t(back_rows(i, 1), wg[c]) + dot_t(back_rows(i, 2), wu[c])).reshape(SLOTS, 16, depth)

        def back(i):
            group, c = i // chunks, i % chunks
            hc_copy(i).wait_recv()
            hf_copy(i).wait_recv()
            add_y(group, i, c)
            add_dx(group, i, c)
            for other in (1, 2, 3):
                @pl.when(i == other * chunks + chunks - 1)
                def _(other=other):
                    for copy in acc_copies(other):
                        copy.start()

        def step(s, carry):
            @pl.when(s < total)
            def _():
                products(chunk_at(s))

            for other in (2, 3):
                @pl.when(s == EARLY + 3 * (other - 2))
                def _(other=other):
                    for kind in range(2):
                        for copy in spread_copies(other, kind):
                            copy.start()

            @pl.when(jnp.logical_and(s > EARLY, s < total + 1))
            def _():
                i = chunk_at(s - 1)
                half_sum(i, near_copy(i))

            @pl.when(jnp.logical_and(s >= FINAL_LAG, s < total + FINAL_LAG))
            def _():
                activations(chunk_at(s - FINAL_LAG))

            @pl.when(jnp.logical_and(s >= EARLY + FINAL_LAG, s < total - chunks + EARLY + FINAL_LAG))
            def _():
                hx_copy(s - FINAL_LAG + chunks - EARLY).start()

            @pl.when(s == total)
            def _():
                for c in range(EARLY):
                    hx_copy(c).start()

            @pl.when(jnp.logical_and(s >= total - chunks + EARLY + FINAL_LAG, s < total + FINAL_LAG))
            def _():
                hx_copy(s - FINAL_LAG + chunks - total).start()

            @pl.when(jnp.logical_and(s >= FORWARD_LAG, s < FORWARD_LAG + total))
            def _():
                i = (s - FORWARD_LAG + chunks) % total
                hx_copy(i).wait_recv()
                hf_copy(i).start()

            @pl.when(s == total - chunks)
            def _():
                x_turned[...] = cols[:, 0].reshape(GROUPS * SLOTS * 16, depth).T

            @pl.when(s >= BACK_LAG)
            def _():
                back((s - BACK_LAG + chunks) % total)

            return carry

        lax.fori_loop(EARLY, total + BACK_LAG - 1, step, 0)

        last = chunks - 1
        hc_copy(last).wait_recv()
        hf_copy(last).wait_recv()
        for kind in range(2):
            (add_y, add_dx)[kind](0, last, last)
            if kind == 0:
                took(acc_in, acc_recv.at[0])
            value = acc[0, kind] + acc_in[0, kind] + acc_in[1, kind] + acc_in[2, kind]
            tail[kind] = (cols[0, kind].astype(F32) + value).astype(BF16)
            for k in (2, 3, 1):
                tail_copy(kind, k).start()
        for kind in range(2):
            rows[kind, :, own] = tail[kind, home]

        sent(cols.at[0, :, pl.ds(0, 3)], first_send.at[0])
        sent(cols.at[0], lead_send.at[0])
        sent(cols.at[pl.ds(0, 2)], spread_send.at[0])
        sent(acc_in, acc_send.at[0])
        sent(near, near_send.at[0])
        sent(far, far_send.at[0])
        for send in (hc_send, hx_send, hf_send):
            sent(hid.at[:, :, 0], send.at[0])
        took(tail.at[:, pl.ds(0, 3)], tail_recv.at[0])
        sent(tail.at[:, pl.ds(0, 3)], tail_send.at[0])

    return kernel, total


def finish(rows, hid, cols, x_turned):
    _, local_rows, model = rows.shape
    total, _, _, _, width = hid.shape
    depth, count = x_turned.shape
    chunks = total // GROUPS
    hidden = chunks * width
    ring = 4
    high = 128

    def kernel(rows_ref, hid_ref, cols_ref, x_ref, y_hbm, dx_hbm, dg_hbm, du_hbm, dd_hbm, g_tile, u_tile, d_tile, row_sem, out_sem):
        row_copies = [pltpu.make_async_copy(rows_ref.at[k], dst, row_sem.at[k]) for k, dst in enumerate((y_hbm, dx_hbm))]

        def all_rows(c, k):
            return jnp.concatenate([hid_ref[group * chunks + c, k].reshape(SLOTS * 16, width) for group in range(GROUPS)])

        def block(k, b):
            span = pl.ds(pl.multiple_of(b * high, high), high)
            return pltpu.make_async_copy((g_tile, u_tile)[k].at[b % ring], (dg_hbm, du_hbm)[k].at[span], out_sem.at[k, b % ring])

        def tile(c):
            span = pl.ds(pl.multiple_of(c * width, width), width)
            return pltpu.make_async_copy(d_tile.at[c % ring], dd_hbm.at[span], out_sem.at[2, c % ring])

        def across(b, carry):
            x_block = x_ref[pl.ds(pl.multiple_of(b * high, high), high)]
            for k, held in enumerate((g_tile, u_tile)):
                @pl.when(b >= ring)
                def _(k=k):
                    block(k, b - ring).wait()
                for c in range(chunks):
                    held[b % ring, :, c * width:(c + 1) * width] = dot(x_block, all_rows(c, k + 1))
                block(k, b).start()
            return carry

        def down(c, carry):
            @pl.when(c >= ring)
            def _():
                tile(c - ring).wait()
            d_tile[c % ring] = dot(all_rows(c, 0).T, cols_ref[:, 1].reshape(count, depth))
            tile(c).start()
            return carry

        lax.fori_loop(0, depth // high, across, 0)
        for copy in row_copies:
            copy.start()
        lax.fori_loop(0, chunks, down, 0)
        for b in range(depth // high - ring, depth // high):
            for k in range(2):
                block(k, b).wait()
        for c in range(chunks - ring, chunks):
            tile(c).wait()
        for copy in row_copies:
            copy.wait()

    dma = pltpu.SemaphoreType.DMA
    any_space = pl.BlockSpec(memory_space=pl.ANY)
    vmem = pl.BlockSpec(memory_space=pltpu.VMEM)
    row_shape = jax.ShapeDtypeStruct((local_rows, model), BF16)
    held = [pltpu.with_memory_space_constraint(value, pltpu.VMEM) for value in (rows, hid, cols, x_turned)]
    return pl.pallas_call(
        kernel,
        out_shape=[row_shape, row_shape, jax.ShapeDtypeStruct((depth, hidden), F32), jax.ShapeDtypeStruct((depth, hidden), F32), jax.ShapeDtypeStruct((hidden, depth), F32)],
        in_specs=[vmem] * 4,
        out_specs=[any_space] * 5,
        scratch_shapes=[
            pltpu.VMEM((ring, high, hidden), F32),
            pltpu.VMEM((ring, high, hidden), F32),
            pltpu.VMEM((ring, width, depth), F32),
            dma((2,)), dma((3, ring)),
        ],
        compiler_params=pltpu.CompilerParams(vmem_limit_bytes=40 * 2**20),
        cost_estimate=pl.CostEstimate(flops=6 * count * depth * hidden, bytes_accessed=12 * depth * hidden, transcendentals=0),
    )(*held)


def solution(mesh):
    row_spec = P(None, ("dp", "tp"), None)
    in_specs = (row_spec, P("dp", "tp"), P("dp", "tp"), P("tp", "dp"), row_spec)
    out_specs = (row_spec, row_spec, P("dp", "tp"), P("dp", "tp"), P("tp", "dp"))

    def local_step(x_loc, w_gate_loc, w_up_loc, w_down_loc, dy_loc):
        depth, hidden = w_gate_loc.shape
        micro, local_rows, model = x_loc.shape
        width = 512
        chunks = hidden // width
        kernel, total = make_kernel(chunks, width)
        dma = pltpu.SemaphoreType.DMA
        any_space = pl.BlockSpec(memory_space=pl.ANY)
        vmem = pl.BlockSpec(memory_space=pltpu.VMEM)
        outs = pl.pallas_call(
            kernel,
            out_shape=[
                pltpu.VMEM((2, micro * local_rows, model), BF16),
                pltpu.VMEM((total, 3, SLOTS, 16, width), BF16),
                pltpu.VMEM((GROUPS, 2, SLOTS, 16, depth), BF16),
                pltpu.VMEM((depth, GROUPS * SLOTS * 16), BF16),
            ],
            in_specs=[any_space] * 5,
            out_specs=[vmem] * 4,
            scratch_shapes=[
                pltpu.VMEM((chunks, depth, width), BF16),
                pltpu.VMEM((chunks, depth, width), BF16),
                pltpu.VMEM((chunks, width, depth), BF16),
                pltpu.VMEM((16, model), BF16),
                pltpu.VMEM((16, model), BF16),
                pltpu.VMEM((total, SLOTS, 3, 16, width), F32),
                pltpu.VMEM((total, 2, 3, 16, width), F32),
                pltpu.VMEM((total, 3, 16, width), F32),
                pltpu.VMEM((GROUPS, 2, SLOTS, 16, depth), F32),
                pltpu.VMEM((GROUPS - 1, 2, SLOTS, 16, depth), F32),
                pltpu.VMEM((2, SLOTS, 16, depth), BF16),
                dma((chunks, 3)),
                dma((1,)), dma((3,)),
                dma((1,)), dma((2,)),
                dma((1,)), dma((8,)),
                dma((1,)), dma((10,)),
                dma((1,)), dma((EARLY + 12,)),
                dma((1,)), dma((12,)),
                dma((1,)), dma((8,)),
                dma((1,)), dma((1,)),
                dma((1,)), dma((1,)),
                dma((2,)), dma((EARLY,)),
                dma((1,)), dma((1,)),
            ],
            compiler_params=pltpu.CompilerParams(collective_id=0, has_side_effects=True, vmem_limit_bytes=53 * 2**20),
        )(x_loc.reshape(micro * local_rows, model), dy_loc.reshape(micro * local_rows, model), w_gate_loc, w_up_loc, w_down_loc)
        y_rows, dx_rows, dw_gate, dw_up, dw_down = finish(*outs)
        return y_rows.reshape(x_loc.shape), dx_rows.reshape(x_loc.shape), dw_gate, dw_up, dw_down

    return jax.shard_map(local_step, mesh=mesh, in_specs=in_specs, out_specs=out_specs, check_vma=False)
```

```python
import jax
import jax.numpy as jnp
from jax import lax
from jax.experimental import pallas as pl
from jax.experimental.pallas import tpu as pltpu
from jax.sharding import PartitionSpec as P

MESH = pl.DeviceIdType.MESH
F32 = jnp.float32
BF16 = jnp.bfloat16
GROUPS = 4
SLOTS = 4
FINAL_LAG = 4
FORWARD_LAG = 10
BACK_LAG = 11
EARLY = 4


def dot(lhs, rhs):
    return lax.dot_general(lhs, rhs, (((1,), (0,)), ((), ())), preferred_element_type=F32)


def dot_t(lhs, rhs):
    return lax.dot_general(lhs, rhs, (((1,), (1,)), ((), ())), preferred_element_type=F32)


def make_kernel(chunks, width):
    total = GROUPS * chunks

    def kernel(x_hbm, dy_hbm, wg_hbm, wu_hbm, wd_hbm,
               rows, hid, cols, x_turned,
               wg, wu, wd, x_ref, dy_ref, part, near, far, acc, acc_in, tail,
               w_sem, first_send, first_recv, spread_send, spread_recv,
               near_send, near_recv, far_send, far_recv,
               hc_send, hc_recv, hx_send, hx_recv, hf_send, hf_recv,
               acc_send, acc_recv, tail_send, tail_recv, in_sem, open_recv, lead_send, lead_recv):
        tp = lax.axis_index("tp")
        dp = lax.axis_index("dp")
        z, y = tp // 2, tp % 2
        x, core = dp // 2, dp % 2
        ox, oc = 1 - x, 1 - core
        core_peer = {"tp": tp, "dp": x * 2 + oc}
        x_peer = {"tp": tp, "dp": ox * 2 + core}
        home = core * 2 + x
        owned = core * 2 + ox
        depth = cols.shape[-1]

        tp_peers = [{"tp": pz * 2 + py, "dp": dp} for pz, py in ((z, 1 - y), (1 - z, y), (1 - z, 1 - y))]
        rows_of = (pl.ds(0, 8), pl.ds(8, 8))

        def place(i):
            return jnp.where(i < EARLY, i, jnp.where(i < chunks, i + total - chunks, i - chunks + EARLY))

        def turn(i):
            return (i + total - chunks) % total

        def chunk_at(s):
            return jnp.where(s < EARLY, s, jnp.where(s < total - chunks + EARLY, s + chunks - EARLY, s + chunks - total))

        def dp_peer(k):
            px, pc = (x + k // 2) % 2, (core + k % 2) % 2
            return px * 2 + pc, pc * 2 + px

        def weight_copies(c):
            span = pl.ds(pl.multiple_of(c * width, width), width)
            return (pltpu.make_async_copy(wg_hbm.at[:, span], wg.at[c], w_sem.at[c]),
                    pltpu.make_async_copy(wu_hbm.at[:, span], wu.at[c], w_sem.at[c]),
                    pltpu.make_async_copy(wd_hbm.at[span], wd.at[c], w_sem.at[c]))

        def weights_in(c):
            size = part.at[pl.ds(0, 8)]
            pltpu.make_async_copy(size, size, w_sem.at[c]).wait()

        def remote(src, dst, send, recv, device):
            return pltpu.make_async_remote_copy(src_ref=src, dst_ref=dst, send_sem=send, recv_sem=recv,
                                                device_id=device, device_id_type=MESH)

        def first_copy(micro, kind, k):
            peer, _ = dp_peer(k)
            src = (x_ref, dy_ref)[kind].at[rows_of[micro], pl.ds(pl.multiple_of(peer * depth, depth), depth)]
            return remote(src, cols.at[0, kind, home, rows_of[micro]], first_send.at[0], first_recv.at[0 if k == 1 else 1 + micro],
                          {"tp": tp, "dp": peer})

        def spread_copies(group, kind):
            if group == 2:
                return [remote(cols.at[0, kind], cols.at[2, kind], spread_send.at[0], spread_recv.at[0], tp_peers[2])]
            return [remote(cols.at[0, kind, :, rows_of[group // 2]], cols.at[group, kind, :, rows_of[way]],
                           spread_send.at[0], spread_recv.at[1], tp_peers[way]) for way in range(2)]

        def lead_copies(far_side, kind):
            side = ox if far_side else x
            return [remote(cols.at[0, kind, core_slot * 2 + side, rows_of[0]], cols.at[1, kind, core_slot * 2 + side, rows_of[way]],
                           lead_send.at[0], lead_recv.at[0], tp_peers[way])
                    for core_slot in range(2) for way in range(2)]

        def near_copy(i):
            return remote(part.at[i, pl.ds(oc * 2, 2)], near.at[i], near_send.at[0], near_recv.at[place(i) % 8], core_peer)

        def open_copy(i, side, recv):
            return remote(part.at[i, oc * 2 + side], near.at[i, side], near_send.at[0], recv, core_peer)

        def here_copy(i):
            return open_copy(i, x, open_recv.at[i])

        def there_copy(i):
            return open_copy(i, ox, near_recv.at[i % 8])

        def far_copy(i):
            return remote(near.at[i, x], far.at[i], far_send.at[0], far_recv.at[place(i) % 10], x_peer)

        def hc_copy(i):
            here = hid.at[i, :, owned]
            return remote(here, here, hc_send.at[0], hc_recv.at[jnp.where(i < EARLY, i, EARLY + turn(i) % 12)], core_peer)

        def hx_copy(i):
            here = hid.at[i, :, owned]
            return remote(here, here, hx_send.at[0], hx_recv.at[turn(i) % 12], x_peer)

        def hf_copy(i):
            there = hid.at[i, :, home]
            return remote(there, there, hf_send.at[0], hf_recv.at[turn(i) % 8], core_peer)

        def acc_copies(group):
            if group == 2:
                return [remote(acc.at[2], acc_in.at[2], acc_send.at[0], acc_recv.at[0], tp_peers[2])]
            return [remote(acc.at[group, :, :, rows_of[way]], acc_in.at[way, :, :, rows_of[group // 2]],
                           acc_send.at[0], acc_recv.at[0], tp_peers[way]) for way in range(2)]

        def tail_copy(kind, k):
            peer, slot = dp_peer(k)
            dst = rows.at[kind, :, pl.ds(pl.multiple_of(dp * depth, depth), depth)]
            return remote(tail.at[kind, slot], dst, tail_send.at[0], tail_recv.at[0], {"tp": tp, "dp": peer})

        barrier = pltpu.get_barrier_semaphore()
        for k in range(1, 4):
            pl.semaphore_signal(barrier, inc=1, device_id=tp_peers[k - 1], device_id_type=MESH)
            pl.semaphore_signal(barrier, inc=1, device_id={"tp": tp, "dp": dp_peer(k)[0]}, device_id_type=MESH)
        row_loads = [pltpu.make_async_copy(src, dst, in_sem.at[k]) for k, (src, dst) in enumerate(((x_hbm, x_ref), (dy_hbm, dy_ref)))]
        for copy in row_loads:
            copy.start()
        for c in range(chunks):
            for copy in weight_copies(c):
                copy.start()

        for copy in row_loads:
            copy.wait()
        pl.semaphore_wait(barrier, 6)

        for micro in range(2):
            for kind in range(2):
                for k in (1, 2, 3):
                    first_copy(micro, kind, k).start()
        own = pl.ds(pl.multiple_of(dp * depth, depth), depth)
        cols[0, 0, home] = x_ref[:, own]
        cols[0, 1, home] = dy_ref[:, own]
        acc[...] = jnp.zeros_like(acc)

        def half_products(i, side):
            rows_in = [jnp.concatenate([cols[0, kind, side], cols[0, kind, 2 + side]]) for kind in range(2)]
            for k, value in enumerate((dot(rows_in[0], wg[i]), dot(rows_in[0], wu[i]), dot_t(rows_in[1], wd[i]))):
                part[i, side, k] = value[:16]
                part[i, 2 + side, k] = value[16:]

        def half_sum(i, copy):
            copy.wait_recv()
            near[i, x] = near[i, x] + part[i, home]
            far_copy(i).start()

        def took(ref, recv):
            remote(ref, ref, recv, recv, core_peer).wait_recv()

        def sent(ref, send):
            remote(ref, ref, send, send, core_peer).wait_send()

        took(cols.at[0, :, 0], first_recv.at[0])
        for kind in range(2):
            for copy in lead_copies(0, kind):
                copy.start()

        def open_here(i, carry):
            weights_in(i)
            half_products(i, x)
            here_copy(i).start()

            @pl.when(i > 0)
            def _():
                half_sum(i - 1, here_copy(i - 1))

            return carry

        lax.fori_loop(0, EARLY, open_here, 0)
        took(cols.at[0, :, 0], first_recv.at[1])
        for kind in range(2):
            for copy in lead_copies(1, kind):
                copy.start()
        half_sum(EARLY - 1, here_copy(EARLY - 1))

        took(cols.at[0, :, 0], first_recv.at[2])

        def open_there(i, carry):
            half_products(i, ox)
            there_copy(i).start()
            return carry

        lax.fori_loop(0, EARLY, open_there, 0)

        def products(i):
            group, c = i // chunks, i % chunks

            @pl.when(jnp.logical_and(group == 1, c >= EARLY))
            def _():
                weights_in(c)

            for other in (1, 2, 3):
                @pl.when(i == other * chunks)
                def _(other=other):
                    took(cols.at[other], lead_recv.at[0] if other == 1 else spread_recv.at[other - 2])

            x_rows = cols[group, 0].reshape(SLOTS * 16, depth)
            dy_rows = cols[group, 1].reshape(SLOTS * 16, depth)
            for k, value in enumerate((dot(x_rows, wg[c]), dot(x_rows, wu[c]), dot_t(dy_rows, wd[c]))):
                for slot in range(SLOTS):
                    part[i, slot, k] = value[slot * 16:(slot + 1) * 16]
            near_copy(i).start()

        def activations(i):
            @pl.when(i < EARLY)
            def _():
                there_copy(i).wait_recv()

            far_copy(i).wait_recv()
            gate = part[i, owned, 0] + near[i, ox, 0] + far[i, 0]
            up = part[i, owned, 1] + near[i, ox, 1] + far[i, 1]
            grad = part[i, owned, 2] + near[i, ox, 2] + far[i, 2]
            sig = jax.nn.sigmoid(gate)
            act = gate * sig
            hid[i, 0, owned] = (act * up).astype(BF16)
            hid[i, 1, owned] = (grad * up * sig * (1.0 + gate * (1.0 - sig))).astype(BF16)
            hid[i, 2, owned] = (grad * act).astype(BF16)
            hc_copy(i).start()

        def back_rows(i, k):
            return hid[i, k].reshape(SLOTS * 16, width)

        def add_y(group, i, c):
            acc[group, 0] += dot(back_rows(i, 0), wd[c]).reshape(SLOTS, 16, depth)

        def add_dx(group, i, c):
            acc[group, 1] += (dot_t(back_rows(i, 1), wg[c]) + dot_t(back_rows(i, 2), wu[c])).reshape(SLOTS, 16, depth)

        def back(i):
            group, c = i // chunks, i % chunks
            hc_copy(i).wait_recv()
            hf_copy(i).wait_recv()
            add_y(group, i, c)
            add_dx(group, i, c)
            for other in (1, 2, 3):
                @pl.when(i == other * chunks + chunks - 1)
                def _(other=other):
                    for copy in acc_copies(other):
                        copy.start()

        def step(s, carry):
            @pl.when(jnp.logical_and(s > EARLY, s < total + 1))
            def _():
                i = chunk_at(s - 1)
                half_sum(i, near_copy(i))

            @pl.when(s < total)
            def _():
                products(chunk_at(s))

            for other in (2, 3):
                @pl.when(s == EARLY + 3 * (other - 2))
                def _(other=other):
                    for kind in range(2):
                        for copy in spread_copies(other, kind):
                            copy.start()

            @pl.when(jnp.logical_and(s >= FINAL_LAG, s < total + FINAL_LAG))
            def _():
                activations(chunk_at(s - FINAL_LAG))

            @pl.when(jnp.logical_and(s >= EARLY + FINAL_LAG, s < total - chunks + EARLY + FINAL_LAG))
            def _():
                hx_copy(s - FINAL_LAG + chunks - EARLY).start()

            @pl.when(s == total)
            def _():
                for c in range(EARLY):
                    hx_copy(c).start()

            @pl.when(jnp.logical_and(s >= total - chunks + EARLY + FINAL_LAG, s < total + FINAL_LAG))
            def _():
                hx_copy(s - FINAL_LAG + chunks - total).start()

            @pl.when(jnp.logical_and(s >= FORWARD_LAG, s < FORWARD_LAG + total))
            def _():
                i = (s - FORWARD_LAG + chunks) % total
                hx_copy(i).wait_recv()
                hf_copy(i).start()

            @pl.when(s == total - chunks)
            def _():
                x_turned[...] = cols[:, 0].reshape(GROUPS * SLOTS * 16, depth).T

            @pl.when(s >= BACK_LAG)
            def _():
                back((s - BACK_LAG + chunks) % total)

            return carry

        lax.fori_loop(EARLY, total + BACK_LAG - 1, step, 0)

        last = chunks - 1
        hc_copy(last).wait_recv()
        hf_copy(last).wait_recv()
        for kind in range(2):
            (add_y, add_dx)[kind](0, last, last)
            if kind == 0:
                took(acc_in, acc_recv.at[0])
            value = acc[0, kind] + acc_in[0, kind] + acc_in[1, kind] + acc_in[2, kind]
            tail[kind] = (cols[0, kind].astype(F32) + value).astype(BF16)
            for k in (2, 3, 1):
                tail_copy(kind, k).start()
        for kind in range(2):
            rows[kind, :, own] = tail[kind, home]

        sent(cols.at[0, :, pl.ds(0, 3)], first_send.at[0])
        sent(cols.at[0], lead_send.at[0])
        sent(cols.at[pl.ds(0, 2)], spread_send.at[0])
        sent(acc_in, acc_send.at[0])
        sent(near, near_send.at[0])
        sent(far, far_send.at[0])
        for send in (hc_send, hx_send, hf_send):
            sent(hid.at[:, :, 0], send.at[0])
        took(tail.at[:, pl.ds(0, 3)], tail_recv.at[0])
        sent(tail.at[:, pl.ds(0, 3)], tail_send.at[0])

    return kernel, total


def finish(rows, hid, cols, x_turned):
    _, local_rows, model = rows.shape
    total, _, _, _, width = hid.shape
    depth, count = x_turned.shape
    chunks = total // GROUPS
    hidden = chunks * width
    ring = 4
    high = 128

    def kernel(rows_ref, hid_ref, cols_ref, x_ref, y_hbm, dx_hbm, dg_hbm, du_hbm, dd_hbm, g_tile, u_tile, d_tile, row_sem, out_sem):
        row_copies = [pltpu.make_async_copy(rows_ref.at[k], dst, row_sem.at[k]) for k, dst in enumerate((y_hbm, dx_hbm))]

        def all_rows(c, k):
            return jnp.concatenate([hid_ref[group * chunks + c, k].reshape(SLOTS * 16, width) for group in range(GROUPS)])

        def block(k, b):
            span = pl.ds(pl.multiple_of(b * high, high), high)
            return pltpu.make_async_copy((g_tile, u_tile)[k].at[b % ring], (dg_hbm, du_hbm)[k].at[span], out_sem.at[k, b % ring])

        def tile(c):
            span = pl.ds(pl.multiple_of(c * width, width), width)
            return pltpu.make_async_copy(d_tile.at[c % ring], dd_hbm.at[span], out_sem.at[2, c % ring])

        def across(b, carry):
            x_block = x_ref[pl.ds(pl.multiple_of(b * high, high), high)]
            for k, held in enumerate((g_tile, u_tile)):
                @pl.when(b >= ring)
                def _(k=k):
                    block(k, b - ring).wait()
                for c in range(chunks):
                    held[b % ring, :, c * width:(c + 1) * width] = dot(x_block, all_rows(c, k + 1))
                block(k, b).start()
            return carry

        def down(c, carry):
            @pl.when(c >= ring)
            def _():
                tile(c - ring).wait()
            d_tile[c % ring] = dot(all_rows(c, 0).T, cols_ref[:, 1].reshape(count, depth))
            tile(c).start()
            return carry

        lax.fori_loop(0, depth // high, across, 0)
        for copy in row_copies:
            copy.start()
        lax.fori_loop(0, chunks, down, 0)
        for b in range(depth // high - ring, depth // high):
            for k in range(2):
                block(k, b).wait()
        for c in range(chunks - ring, chunks):
            tile(c).wait()
        for copy in row_copies:
            copy.wait()

    dma = pltpu.SemaphoreType.DMA
    any_space = pl.BlockSpec(memory_space=pl.ANY)
    vmem = pl.BlockSpec(memory_space=pltpu.VMEM)
    row_shape = jax.ShapeDtypeStruct((local_rows, model), BF16)
    held = [pltpu.with_memory_space_constraint(value, pltpu.VMEM) for value in (rows, hid, cols, x_turned)]
    return pl.pallas_call(
        kernel,
        out_shape=[row_shape, row_shape, jax.ShapeDtypeStruct((depth, hidden), F32), jax.ShapeDtypeStruct((depth, hidden), F32), jax.ShapeDtypeStruct((hidden, depth), F32)],
        in_specs=[vmem] * 4,
        out_specs=[any_space] * 5,
        scratch_shapes=[
            pltpu.VMEM((ring, high, hidden), F32),
            pltpu.VMEM((ring, high, hidden), F32),
            pltpu.VMEM((ring, width, depth), F32),
            dma((2,)), dma((3, ring)),
        ],
        compiler_params=pltpu.CompilerParams(vmem_limit_bytes=40 * 2**20),
        cost_estimate=pl.CostEstimate(flops=6 * count * depth * hidden, bytes_accessed=12 * depth * hidden, transcendentals=0),
    )(*held)


def solution(mesh):
    row_spec = P(None, ("dp", "tp"), None)
    in_specs = (row_spec, P("dp", "tp"), P("dp", "tp"), P("tp", "dp"), row_spec)
    out_specs = (row_spec, row_spec, P("dp", "tp"), P("dp", "tp"), P("tp", "dp"))

    def local_step(x_loc, w_gate_loc, w_up_loc, w_down_loc, dy_loc):
        depth, hidden = w_gate_loc.shape
        micro, local_rows, model = x_loc.shape
        width = 512
        chunks = hidden // width
        kernel, total = make_kernel(chunks, width)
        dma = pltpu.SemaphoreType.DMA
        any_space = pl.BlockSpec(memory_space=pl.ANY)
        vmem = pl.BlockSpec(memory_space=pltpu.VMEM)
        outs = pl.pallas_call(
            kernel,
            out_shape=[
                pltpu.VMEM((2, micro * local_rows, model), BF16),
                pltpu.VMEM((total, 3, SLOTS, 16, width), BF16),
                pltpu.VMEM((GROUPS, 2, SLOTS, 16, depth), BF16),
                pltpu.VMEM((depth, GROUPS * SLOTS * 16), BF16),
            ],
            in_specs=[any_space] * 5,
            out_specs=[vmem] * 4,
            scratch_shapes=[
                pltpu.VMEM((chunks, depth, width), BF16),
                pltpu.VMEM((chunks, depth, width), BF16),
                pltpu.VMEM((chunks, width, depth), BF16),
                pltpu.VMEM((16, model), BF16),
                pltpu.VMEM((16, model), BF16),
                pltpu.VMEM((total, SLOTS, 3, 16, width), F32),
                pltpu.VMEM((total, 2, 3, 16, width), F32),
                pltpu.VMEM((total, 3, 16, width), F32),
                pltpu.VMEM((GROUPS, 2, SLOTS, 16, depth), F32),
                pltpu.VMEM((GROUPS - 1, 2, SLOTS, 16, depth), F32),
                pltpu.VMEM((2, SLOTS, 16, depth), BF16),
                dma((chunks,)),
                dma((1,)), dma((3,)),
                dma((1,)), dma((2,)),
                dma((1,)), dma((8,)),
                dma((1,)), dma((10,)),
                dma((1,)), dma((EARLY + 12,)),
                dma((1,)), dma((12,)),
                dma((1,)), dma((8,)),
                dma((1,)), dma((1,)),
                dma((1,)), dma((1,)),
                dma((2,)), dma((EARLY,)),
                dma((1,)), dma((1,)),
            ],
            compiler_params=pltpu.CompilerParams(collective_id=0, has_side_effects=True, vmem_limit_bytes=53 * 2**20),
        )(x_loc.reshape(micro * local_rows, model), dy_loc.reshape(micro * local_rows, model), w_gate_loc, w_up_loc, w_down_loc)
        y_rows, dx_rows, dw_gate, dw_up, dw_down = finish(*outs)
        return y_rows.reshape(x_loc.shape), dx_rows.reshape(x_loc.shape), dw_gate, dw_up, dw_down

    return jax.shard_map(local_step, mesh=mesh, in_specs=in_specs, out_specs=out_specs, check_vma=False)
```

```python
import jax
import jax.numpy as jnp
from jax import lax
from jax.experimental import pallas as pl
from jax.experimental.pallas import tpu as pltpu
from jax.sharding import PartitionSpec as P

MESH = pl.DeviceIdType.MESH
F32 = jnp.float32
BF16 = jnp.bfloat16
GROUPS = 4
SLOTS = 4
FINAL_LAG = 4
FORWARD_LAG = 10
BACK_LAG = 11
EARLY = 3


def dot(lhs, rhs):
    return lax.dot_general(lhs, rhs, (((1,), (0,)), ((), ())), preferred_element_type=F32)


def dot_t(lhs, rhs):
    return lax.dot_general(lhs, rhs, (((1,), (1,)), ((), ())), preferred_element_type=F32)


def make_kernel(chunks, width):
    total = GROUPS * chunks

    def kernel(x_hbm, dy_hbm, wg_hbm, wu_hbm, wd_hbm,
               rows, hid, cols, x_turned,
               wg, wu, wd, x_ref, dy_ref, part, near, far, acc, acc_in, tail,
               w_sem, first_send, first_recv, spread_send, spread_recv,
               near_send, near_recv, far_send, far_recv,
               hc_send, hc_recv, hx_send, hx_recv, hf_send, hf_recv,
               acc_send, acc_recv, tail_send, tail_recv, in_sem, open_recv, lead_send, lead_recv):
        tp = lax.axis_index("tp")
        dp = lax.axis_index("dp")
        z, y = tp // 2, tp % 2
        x, core = dp // 2, dp % 2
        ox, oc = 1 - x, 1 - core
        core_peer = {"tp": tp, "dp": x * 2 + oc}
        x_peer = {"tp": tp, "dp": ox * 2 + core}
        home = core * 2 + x
        owned = core * 2 + ox
        depth = cols.shape[-1]

        tp_peers = [{"tp": pz * 2 + py, "dp": dp} for pz, py in ((z, 1 - y), (1 - z, y), (1 - z, 1 - y))]
        rows_of = (pl.ds(0, 8), pl.ds(8, 8))

        def place(i):
            return jnp.where(i < EARLY, i, jnp.where(i < chunks, i + total - chunks, i - chunks + EARLY))

        def turn(i):
            return (i + total - chunks) % total

        def chunk_at(s):
            return jnp.where(s < EARLY, s, jnp.where(s < total - chunks + EARLY, s + chunks - EARLY, s + chunks - total))

        def dp_peer(k):
            px, pc = (x + k // 2) % 2, (core + k % 2) % 2
            return px * 2 + pc, pc * 2 + px

        def weight_copies(c):
            span = pl.ds(pl.multiple_of(c * width, width), width)
            return (pltpu.make_async_copy(wg_hbm.at[:, span], wg.at[c], w_sem.at[c]),
                    pltpu.make_async_copy(wu_hbm.at[:, span], wu.at[c], w_sem.at[c]),
                    pltpu.make_async_copy(wd_hbm.at[span], wd.at[c], w_sem.at[c]))

        def weights_in(c):
            size = part.at[pl.ds(0, 8)]
            pltpu.make_async_copy(size, size, w_sem.at[c]).wait()

        def remote(src, dst, send, recv, device):
            return pltpu.make_async_remote_copy(src_ref=src, dst_ref=dst, send_sem=send, recv_sem=recv,
                                                device_id=device, device_id_type=MESH)

        def first_copy(micro, kind, k):
            peer, _ = dp_peer(k)
            src = (x_ref, dy_ref)[kind].at[rows_of[micro], pl.ds(pl.multiple_of(peer * depth, depth), depth)]
            return remote(src, cols.at[0, kind, home, rows_of[micro]], first_send.at[0], first_recv.at[0 if k == 1 else 1 + micro],
                          {"tp": tp, "dp": peer})

        def spread_copies(group, kind):
            if group == 2:
                return [remote(cols.at[0, kind], cols.at[2, kind], spread_send.at[0], spread_recv.at[0], tp_peers[2])]
            return [remote(cols.at[0, kind, :, rows_of[group // 2]], cols.at[group, kind, :, rows_of[way]],
                           spread_send.at[0], spread_recv.at[1], tp_peers[way]) for way in range(2)]

        def lead_copies(far_side, kind):
            side = ox if far_side else x
            return [remote(cols.at[0, kind, core_slot * 2 + side, rows_of[0]], cols.at[1, kind, core_slot * 2 + side, rows_of[way]],
                           lead_send.at[0], lead_recv.at[0], tp_peers[way])
                    for core_slot in range(2) for way in range(2)]

        def near_copy(i):
            return remote(part.at[i, pl.ds(oc * 2, 2)], near.at[i], near_send.at[0], near_recv.at[place(i) % 8], core_peer)

        def open_copy(i, side, recv):
            return remote(part.at[i, oc * 2 + side], near.at[i, side], near_send.at[0], recv, core_peer)

        def here_copy(i):
            return open_copy(i, x, open_recv.at[i])

        def there_copy(i):
            return open_copy(i, ox, near_recv.at[i % 8])

        def far_copy(i):
            return remote(near.at[i, x], far.at[i], far_send.at[0], far_recv.at[place(i) % 10], x_peer)

        def hc_copy(i):
            here = hid.at[i, :, owned]
            return remote(here, here, hc_send.at[0], hc_recv.at[jnp.where(i < EARLY, i, EARLY + turn(i) % 12)], core_peer)

        def hx_copy(i):
            here = hid.at[i, :, owned]
            return remote(here, here, hx_send.at[0], hx_recv.at[turn(i) % 12], x_peer)

        def hf_copy(i):
            there = hid.at[i, :, home]
            return remote(there, there, hf_send.at[0], hf_recv.at[turn(i) % 8], core_peer)

        def acc_copies(group):
            if group == 2:
                return [remote(acc.at[2], acc_in.at[2], acc_send.at[0], acc_recv.at[0], tp_peers[2])]
            return [remote(acc.at[group, :, :, rows_of[way]], acc_in.at[way, :, :, rows_of[group // 2]],
                           acc_send.at[0], acc_recv.at[0], tp_peers[way]) for way in range(2)]

        def tail_copy(kind, k):
            peer, slot = dp_peer(k)
            dst = rows.at[kind, :, pl.ds(pl.multiple_of(dp * depth, depth), depth)]
            return remote(tail.at[kind, slot], dst, tail_send.at[0], tail_recv.at[0], {"tp": tp, "dp": peer})

        barrier = pltpu.get_barrier_semaphore()
        for k in range(1, 4):
            pl.semaphore_signal(barrier, inc=1, device_id=tp_peers[k - 1], device_id_type=MESH)
            pl.semaphore_signal(barrier, inc=1, device_id={"tp": tp, "dp": dp_peer(k)[0]}, device_id_type=MESH)
        row_loads = [pltpu.make_async_copy(src, dst, in_sem.at[k]) for k, (src, dst) in enumerate(((x_hbm, x_ref), (dy_hbm, dy_ref)))]
        for copy in row_loads:
            copy.start()
        for c in range(chunks):
            for copy in weight_copies(c):
                copy.start()

        for copy in row_loads:
            copy.wait()
        pl.semaphore_wait(barrier, 6)

        for micro in range(2):
            for kind in range(2):
                for k in (1, 2, 3):
                    first_copy(micro, kind, k).start()
        own = pl.ds(pl.multiple_of(dp * depth, depth), depth)
        cols[0, 0, home] = x_ref[:, own]
        cols[0, 1, home] = dy_ref[:, own]
        acc[...] = jnp.zeros_like(acc)

        def half_products(i, side):
            rows_in = [jnp.concatenate([cols[0, kind, side], cols[0, kind, 2 + side]]) for kind in range(2)]
            for k, value in enumerate((dot(rows_in[0], wg[i]), dot(rows_in[0], wu[i]), dot_t(rows_in[1], wd[i]))):
                part[i, side, k] = value[:16]
                part[i, 2 + side, k] = value[16:]

        def half_sum(i, copy):
            copy.wait_recv()
            near[i, x] = near[i, x] + part[i, home]
            far_copy(i).start()

        def took(ref, recv):
            remote(ref, ref, recv, recv, core_peer).wait_recv()

        def sent(ref, send):
            remote(ref, ref, send, send, core_peer).wait_send()

        took(cols.at[0, :, 0], first_recv.at[0])
        for kind in range(2):
            for copy in lead_copies(0, kind):
                copy.start()

        def open_here(i, carry):
            weights_in(i)
            half_products(i, x)
            here_copy(i).start()

            @pl.when(i > 0)
            def _():
                half_sum(i - 1, here_copy(i - 1))

            return carry

        lax.fori_loop(0, EARLY, open_here, 0)
        took(cols.at[0, :, 0], first_recv.at[1])
        for kind in range(2):
            for copy in lead_copies(1, kind):
                copy.start()
        half_sum(EARLY - 1, here_copy(EARLY - 1))

        took(cols.at[0, :, 0], first_recv.at[2])

        def open_there(i, carry):
            half_products(i, ox)
            there_copy(i).start()
            return carry

        lax.fori_loop(0, EARLY, open_there, 0)

        def products(i):
            group, c = i // chunks, i % chunks

            @pl.when(jnp.logical_and(group == 1, c >= EARLY))
            def _():
                weights_in(c)

            for other in (1, 2, 3):
                @pl.when(i == other * chunks)
                def _(other=other):
                    took(cols.at[other], lead_recv.at[0] if other == 1 else spread_recv.at[other - 2])

            x_rows = cols[group, 0].reshape(SLOTS * 16, depth)
            dy_rows = cols[group, 1].reshape(SLOTS * 16, depth)
            for k, value in enumerate((dot(x_rows, wg[c]), dot(x_rows, wu[c]), dot_t(dy_rows, wd[c]))):
                for slot in range(SLOTS):
                    part[i, slot, k] = value[slot * 16:(slot + 1) * 16]
            near_copy(i).start()

        def activations(i):
            @pl.when(i < EARLY)
            def _():
                there_copy(i).wait_recv()

            far_copy(i).wait_recv()
            gate = part[i, owned, 0] + near[i, ox, 0] + far[i, 0]
            up = part[i, owned, 1] + near[i, ox, 1] + far[i, 1]
            grad = part[i, owned, 2] + near[i, ox, 2] + far[i, 2]
            sig = jax.nn.sigmoid(gate)
            act = gate * sig
            hid[i, 0, owned] = (act * up).astype(BF16)
            hid[i, 1, owned] = (grad * up * sig * (1.0 + gate * (1.0 - sig))).astype(BF16)
            hid[i, 2, owned] = (grad * act).astype(BF16)
            hc_copy(i).start()

        def back_rows(i, k):
            return hid[i, k].reshape(SLOTS * 16, width)

        def add_y(group, i, c):
            acc[group, 0] += dot(back_rows(i, 0), wd[c]).reshape(SLOTS, 16, depth)

        def add_dx(group, i, c):
            acc[group, 1] += (dot_t(back_rows(i, 1), wg[c]) + dot_t(back_rows(i, 2), wu[c])).reshape(SLOTS, 16, depth)

        def back(i):
            group, c = i // chunks, i % chunks
            hc_copy(i).wait_recv()
            hf_copy(i).wait_recv()
            add_y(group, i, c)
            add_dx(group, i, c)
            for other in (1, 2, 3):
                @pl.when(i == other * chunks + chunks - 1)
                def _(other=other):
                    for copy in acc_copies(other):
                        copy.start()

        def step(s, carry):
            @pl.when(jnp.logical_and(s > EARLY, s < total + 1))
            def _():
                i = chunk_at(s - 1)
                half_sum(i, near_copy(i))

            @pl.when(s < total)
            def _():
                products(chunk_at(s))

            for other in (2, 3):
                @pl.when(s == EARLY + 3 * (other - 2))
                def _(other=other):
                    for kind in range(2):
                        for copy in spread_copies(other, kind):
                            copy.start()

            @pl.when(jnp.logical_and(s >= FINAL_LAG, s < total + FINAL_LAG))
            def _():
                activations(chunk_at(s - FINAL_LAG))

            @pl.when(jnp.logical_and(s >= EARLY + FINAL_LAG, s < total - chunks + EARLY + FINAL_LAG))
            def _():
                hx_copy(s - FINAL_LAG + chunks - EARLY).start()

            @pl.when(s == total)
            def _():
                for c in range(EARLY):
                    hx_copy(c).start()

            @pl.when(jnp.logical_and(s >= total - chunks + EARLY + FINAL_LAG, s < total + FINAL_LAG))
            def _():
                hx_copy(s - FINAL_LAG + chunks - total).start()

            @pl.when(jnp.logical_and(s >= FORWARD_LAG, s < FORWARD_LAG + total))
            def _():
                i = (s - FORWARD_LAG + chunks) % total
                hx_copy(i).wait_recv()
                hf_copy(i).start()

            @pl.when(s == total - chunks)
            def _():
                x_turned[...] = cols[:, 0].reshape(GROUPS * SLOTS * 16, depth).T

            @pl.when(s >= BACK_LAG)
            def _():
                back((s - BACK_LAG + chunks) % total)

            return carry

        lax.fori_loop(EARLY, total + BACK_LAG - 1, step, 0)

        last = chunks - 1
        hc_copy(last).wait_recv()
        hf_copy(last).wait_recv()
        for kind in range(2):
            (add_y, add_dx)[kind](0, last, last)
            if kind == 0:
                took(acc_in, acc_recv.at[0])
            value = acc[0, kind] + acc_in[0, kind] + acc_in[1, kind] + acc_in[2, kind]
            tail[kind] = (cols[0, kind].astype(F32) + value).astype(BF16)
            for k in (2, 3, 1):
                tail_copy(kind, k).start()
        for kind in range(2):
            rows[kind, :, own] = tail[kind, home]

        sent(cols.at[0, :, pl.ds(0, 3)], first_send.at[0])
        sent(cols.at[0], lead_send.at[0])
        sent(cols.at[pl.ds(0, 2)], spread_send.at[0])
        sent(acc_in, acc_send.at[0])
        sent(near, near_send.at[0])
        sent(far, far_send.at[0])
        for send in (hc_send, hx_send, hf_send):
            sent(hid.at[:, :, 0], send.at[0])
        took(tail.at[:, pl.ds(0, 3)], tail_recv.at[0])
        sent(tail.at[:, pl.ds(0, 3)], tail_send.at[0])

    return kernel, total


def finish(rows, hid, cols, x_turned):
    _, local_rows, model = rows.shape
    total, _, _, _, width = hid.shape
    depth, count = x_turned.shape
    chunks = total // GROUPS
    hidden = chunks * width
    ring = 4
    high = 128

    def kernel(rows_ref, hid_ref, cols_ref, x_ref, y_hbm, dx_hbm, dg_hbm, du_hbm, dd_hbm, g_tile, u_tile, d_tile, row_sem, out_sem):
        row_copies = [pltpu.make_async_copy(rows_ref.at[k], dst, row_sem.at[k]) for k, dst in enumerate((y_hbm, dx_hbm))]

        def all_rows(c, k):
            return jnp.concatenate([hid_ref[group * chunks + c, k].reshape(SLOTS * 16, width) for group in range(GROUPS)])

        def block(k, b):
            span = pl.ds(pl.multiple_of(b * high, high), high)
            return pltpu.make_async_copy((g_tile, u_tile)[k].at[b % ring], (dg_hbm, du_hbm)[k].at[span], out_sem.at[k, b % ring])

        def tile(c):
            span = pl.ds(pl.multiple_of(c * width, width), width)
            return pltpu.make_async_copy(d_tile.at[c % ring], dd_hbm.at[span], out_sem.at[2, c % ring])

        def across(b, carry):
            x_block = x_ref[pl.ds(pl.multiple_of(b * high, high), high)]
            for k, held in enumerate((g_tile, u_tile)):
                @pl.when(b >= ring)
                def _(k=k):
                    block(k, b - ring).wait()
                for c in range(chunks):
                    held[b % ring, :, c * width:(c + 1) * width] = dot(x_block, all_rows(c, k + 1))
                block(k, b).start()
            return carry

        def down(c, carry):
            @pl.when(c >= ring)
            def _():
                tile(c - ring).wait()
            d_tile[c % ring] = dot(all_rows(c, 0).T, cols_ref[:, 1].reshape(count, depth))
            tile(c).start()
            return carry

        lax.fori_loop(0, depth // high, across, 0)
        for copy in row_copies:
            copy.start()
        lax.fori_loop(0, chunks, down, 0)
        for b in range(depth // high - ring, depth // high):
            for k in range(2):
                block(k, b).wait()
        for c in range(chunks - ring, chunks):
            tile(c).wait()
        for copy in row_copies:
            copy.wait()

    dma = pltpu.SemaphoreType.DMA
    any_space = pl.BlockSpec(memory_space=pl.ANY)
    vmem = pl.BlockSpec(memory_space=pltpu.VMEM)
    row_shape = jax.ShapeDtypeStruct((local_rows, model), BF16)
    held = [pltpu.with_memory_space_constraint(value, pltpu.VMEM) for value in (rows, hid, cols, x_turned)]
    return pl.pallas_call(
        kernel,
        out_shape=[row_shape, row_shape, jax.ShapeDtypeStruct((depth, hidden), F32), jax.ShapeDtypeStruct((depth, hidden), F32), jax.ShapeDtypeStruct((hidden, depth), F32)],
        in_specs=[vmem] * 4,
        out_specs=[any_space] * 5,
        scratch_shapes=[
            pltpu.VMEM((ring, high, hidden), F32),
            pltpu.VMEM((ring, high, hidden), F32),
            pltpu.VMEM((ring, width, depth), F32),
            dma((2,)), dma((3, ring)),
        ],
        compiler_params=pltpu.CompilerParams(vmem_limit_bytes=40 * 2**20),
        cost_estimate=pl.CostEstimate(flops=6 * count * depth * hidden, bytes_accessed=12 * depth * hidden, transcendentals=0),
    )(*held)


def solution(mesh):
    row_spec = P(None, ("dp", "tp"), None)
    in_specs = (row_spec, P("dp", "tp"), P("dp", "tp"), P("tp", "dp"), row_spec)
    out_specs = (row_spec, row_spec, P("dp", "tp"), P("dp", "tp"), P("tp", "dp"))

    def local_step(x_loc, w_gate_loc, w_up_loc, w_down_loc, dy_loc):
        depth, hidden = w_gate_loc.shape
        micro, local_rows, model = x_loc.shape
        width = 512
        chunks = hidden // width
        kernel, total = make_kernel(chunks, width)
        dma = pltpu.SemaphoreType.DMA
        any_space = pl.BlockSpec(memory_space=pl.ANY)
        vmem = pl.BlockSpec(memory_space=pltpu.VMEM)
        outs = pl.pallas_call(
            kernel,
            out_shape=[
                pltpu.VMEM((2, micro * local_rows, model), BF16),
                pltpu.VMEM((total, 3, SLOTS, 16, width), BF16),
                pltpu.VMEM((GROUPS, 2, SLOTS, 16, depth), BF16),
                pltpu.VMEM((depth, GROUPS * SLOTS * 16), BF16),
            ],
            in_specs=[any_space] * 5,
            out_specs=[vmem] * 4,
            scratch_shapes=[
                pltpu.VMEM((chunks, depth, width), BF16),
                pltpu.VMEM((chunks, depth, width), BF16),
                pltpu.VMEM((chunks, width, depth), BF16),
                pltpu.VMEM((16, model), BF16),
                pltpu.VMEM((16, model), BF16),
                pltpu.VMEM((total, SLOTS, 3, 16, width), F32),
                pltpu.VMEM((total, 2, 3, 16, width), F32),
                pltpu.VMEM((total, 3, 16, width), F32),
                pltpu.VMEM((GROUPS, 2, SLOTS, 16, depth), F32),
                pltpu.VMEM((GROUPS - 1, 2, SLOTS, 16, depth), F32),
                pltpu.VMEM((2, SLOTS, 16, depth), BF16),
                dma((chunks,)),
                dma((1,)), dma((3,)),
                dma((1,)), dma((2,)),
                dma((1,)), dma((8,)),
                dma((1,)), dma((10,)),
                dma((1,)), dma((EARLY + 12,)),
                dma((1,)), dma((12,)),
                dma((1,)), dma((8,)),
                dma((1,)), dma((1,)),
                dma((1,)), dma((1,)),
                dma((2,)), dma((EARLY,)),
                dma((1,)), dma((1,)),
            ],
            compiler_params=pltpu.CompilerParams(collective_id=0, has_side_effects=True, vmem_limit_bytes=53 * 2**20),
        )(x_loc.reshape(micro * local_rows, model), dy_loc.reshape(micro * local_rows, model), w_gate_loc, w_up_loc, w_down_loc)
        y_rows, dx_rows, dw_gate, dw_up, dw_down = finish(*outs)
        return y_rows.reshape(x_loc.shape), dx_rows.reshape(x_loc.shape), dw_gate, dw_up, dw_down

    return jax.shard_map(local_step, mesh=mesh, in_specs=in_specs, out_specs=out_specs, check_vma=False)
```

```python
import jax
import jax.numpy as jnp
from jax import lax
from jax.experimental import pallas as pl
from jax.experimental.pallas import tpu as pltpu
from jax.sharding import PartitionSpec as P

MESH = pl.DeviceIdType.MESH
F32 = jnp.float32
BF16 = jnp.bfloat16
GROUPS = 4
SLOTS = 4
FINAL_LAG = 4
FORWARD_LAG = 11
BACK_LAG = 12
EARLY = 5


def dot(lhs, rhs):
    return lax.dot_general(lhs, rhs, (((1,), (0,)), ((), ())), preferred_element_type=F32)


def dot_t(lhs, rhs):
    return lax.dot_general(lhs, rhs, (((1,), (1,)), ((), ())), preferred_element_type=F32)


def make_kernel(chunks, width):
    total = GROUPS * chunks

    def kernel(x_hbm, dy_hbm, wg_hbm, wu_hbm, wd_hbm,
               rows, hid, cols, x_turned,
               wg, wu, wd, x_ref, dy_ref, part, near, far, acc, acc_in, tail,
               w_sem, first_send, first_recv, spread_send, spread_recv,
               near_send, near_recv, far_send, far_recv,
               hc_send, hc_recv, hx_send, hx_recv, hf_send, hf_recv,
               acc_send, acc_recv, tail_send, tail_recv, in_sem, open_recv, lead_send, lead_recv):
        tp = lax.axis_index("tp")
        dp = lax.axis_index("dp")
        z, y = tp // 2, tp % 2
        x, core = dp // 2, dp % 2
        ox, oc = 1 - x, 1 - core
        core_peer = {"tp": tp, "dp": x * 2 + oc}
        x_peer = {"tp": tp, "dp": ox * 2 + core}
        home = core * 2 + x
        owned = core * 2 + ox
        depth = cols.shape[-1]

        tp_peers = [{"tp": pz * 2 + py, "dp": dp} for pz, py in ((z, 1 - y), (1 - z, y), (1 - z, 1 - y))]
        rows_of = (pl.ds(0, 8), pl.ds(8, 8))

        def place(i):
            return jnp.where(i < EARLY, i, jnp.where(i < chunks, i + total - chunks, i - chunks + EARLY))

        def turn(i):
            return (i + total - chunks) % total

        def chunk_at(s):
            return jnp.where(s < EARLY, s, jnp.where(s < total - chunks + EARLY, s + chunks - EARLY, s + chunks - total))

        def dp_peer(k):
            px, pc = (x + k // 2) % 2, (core + k % 2) % 2
            return px * 2 + pc, pc * 2 + px

        def weight_copies(c):
            span = pl.ds(pl.multiple_of(c * width, width), width)
            return (pltpu.make_async_copy(wg_hbm.at[:, span], wg.at[c], w_sem.at[c]),
                    pltpu.make_async_copy(wu_hbm.at[:, span], wu.at[c], w_sem.at[c]),
                    pltpu.make_async_copy(wd_hbm.at[span], wd.at[c], w_sem.at[c]))

        def weights_in(c):
            size = part.at[pl.ds(0, 8)]
            pltpu.make_async_copy(size, size, w_sem.at[c]).wait()

        def remote(src, dst, send, recv, device):
            return pltpu.make_async_remote_copy(src_ref=src, dst_ref=dst, send_sem=send, recv_sem=recv,
                                                device_id=device, device_id_type=MESH)

        def first_copy(micro, kind, k):
            peer, _ = dp_peer(k)
            src = (x_ref, dy_ref)[kind].at[rows_of[micro], pl.ds(pl.multiple_of(peer * depth, depth), depth)]
            return remote(src, cols.at[0, kind, home, rows_of[micro]], first_send.at[0], first_recv.at[0 if k == 1 else 1 + micro],
                          {"tp": tp, "dp": peer})

        def spread_copies(group, kind):
            if group == 2:
                return [remote(cols.at[0, kind], cols.at[2, kind], spread_send.at[0], spread_recv.at[0], tp_peers[2])]
            return [remote(cols.at[0, kind, :, rows_of[group // 2]], cols.at[group, kind, :, rows_of[way]],
                           spread_send.at[0], spread_recv.at[1], tp_peers[way]) for way in range(2)]

        def lead_copies(far_side, kind):
            side = ox if far_side else x
            return [remote(cols.at[0, kind, core_slot * 2 + side, rows_of[0]], cols.at[1, kind, core_slot * 2 + side, rows_of[way]],
                           lead_send.at[0], lead_recv.at[0], tp_peers[way])
                    for core_slot in range(2) for way in range(2)]

        def near_copy(i):
            return remote(part.at[i, pl.ds(oc * 2, 2)], near.at[i], near_send.at[0], near_recv.at[place(i) % 8], core_peer)

        def open_copy(i, side, recv):
            return remote(part.at[i, oc * 2 + side], near.at[i, side], near_send.at[0], recv, core_peer)

        def here_copy(i):
            return open_copy(i, x, open_recv.at[i])

        def there_copy(i):
            return open_copy(i, ox, near_recv.at[i % 8])

        def far_copy(i):
            return remote(near.at[i, x], far.at[i], far_send.at[0], far_recv.at[place(i) % 10], x_peer)

        def hc_copy(i):
            here = hid.at[i, :, owned]
            return remote(here, here, hc_send.at[0], hc_recv.at[jnp.where(i < EARLY, i, EARLY + turn(i) % 12)], core_peer)

        def hx_copy(i):
            here = hid.at[i, :, owned]
            return remote(here, here, hx_send.at[0], hx_recv.at[turn(i) % 12], x_peer)

        def hf_copy(i):
            there = hid.at[i, :, home]
            return remote(there, there, hf_send.at[0], hf_recv.at[turn(i) % 8], core_peer)

        def acc_copies(group):
            if group == 2:
                return [remote(acc.at[2], acc_in.at[2], acc_send.at[0], acc_recv.at[0], tp_peers[2])]
            return [remote(acc.at[group, :, :, rows_of[way]], acc_in.at[way, :, :, rows_of[group // 2]],
                           acc_send.at[0], acc_recv.at[0], tp_peers[way]) for way in range(2)]

        def tail_copy(kind, k):
            peer, slot = dp_peer(k)
            dst = rows.at[kind, :, pl.ds(pl.multiple_of(dp * depth, depth), depth)]
            return remote(tail.at[kind, slot], dst, tail_send.at[0], tail_recv.at[0], {"tp": tp, "dp": peer})

        barrier = pltpu.get_barrier_semaphore()
        for k in range(1, 4):
            pl.semaphore_signal(barrier, inc=1, device_id=tp_peers[k - 1], device_id_type=MESH)
            pl.semaphore_signal(barrier, inc=1, device_id={"tp": tp, "dp": dp_peer(k)[0]}, device_id_type=MESH)
        row_loads = [pltpu.make_async_copy(src, dst, in_sem.at[k]) for k, (src, dst) in enumerate(((x_hbm, x_ref), (dy_hbm, dy_ref)))]
        for copy in row_loads:
            copy.start()
        for c in range(chunks):
            for copy in weight_copies(c):
                copy.start()

        for copy in row_loads:
            copy.wait()
        pl.semaphore_wait(barrier, 6)

        for micro in range(2):
            for kind in range(2):
                for k in (1, 2, 3):
                    first_copy(micro, kind, k).start()
        own = pl.ds(pl.multiple_of(dp * depth, depth), depth)
        cols[0, 0, home] = x_ref[:, own]
        cols[0, 1, home] = dy_ref[:, own]
        acc[...] = jnp.zeros_like(acc)

        def half_products(i, side):
            rows_in = [jnp.concatenate([cols[0, kind, side], cols[0, kind, 2 + side]]) for kind in range(2)]
            for k, value in enumerate((dot(rows_in[0], wg[i]), dot(rows_in[0], wu[i]), dot_t(rows_in[1], wd[i]))):
                part[i, side, k] = value[:16]
                part[i, 2 + side, k] = value[16:]

        def half_sum(i, copy):
            copy.wait_recv()
            near[i, x] = near[i, x] + part[i, home]
            far_copy(i).start()

        def took(ref, recv):
            remote(ref, ref, recv, recv, core_peer).wait_recv()

        def sent(ref, send):
            remote(ref, ref, send, send, core_peer).wait_send()

        took(cols.at[0, :, 0], first_recv.at[0])
        for kind in range(2):
            for copy in lead_copies(0, kind):
                copy.start()

        def open_here(i, carry):
            weights_in(i)
            half_products(i, x)
            here_copy(i).start()

            @pl.when(i > 0)
            def _():
                half_sum(i - 1, here_copy(i - 1))

            return carry

        lax.fori_loop(0, EARLY, open_here, 0)
        took(cols.at[0, :, 0], first_recv.at[1])
        for kind in range(2):
            for copy in lead_copies(1, kind):
                copy.start()
        half_sum(EARLY - 1, here_copy(EARLY - 1))

        took(cols.at[0, :, 0], first_recv.at[2])

        def open_there(i, carry):
            half_products(i, ox)
            there_copy(i).start()
            return carry

        lax.fori_loop(0, EARLY, open_there, 0)

        def products(i):
            group, c = i // chunks, i % chunks

            @pl.when(jnp.logical_and(group == 1, c >= EARLY))
            def _():
                weights_in(c)

            for other in (1, 2, 3):
                @pl.when(i == other * chunks)
                def _(other=other):
                    took(cols.at[other], lead_recv.at[0] if other == 1 else spread_recv.at[other - 2])

            x_rows = cols[group, 0].reshape(SLOTS * 16, depth)
            dy_rows = cols[group, 1].reshape(SLOTS * 16, depth)
            for k, value in enumerate((dot(x_rows, wg[c]), dot(x_rows, wu[c]), dot_t(dy_rows, wd[c]))):
                for slot in range(SLOTS):
                    part[i, slot, k] = value[slot * 16:(slot + 1) * 16]
            near_copy(i).start()

        def activations(i):
            @pl.when(i < EARLY)
            def _():
                there_copy(i).wait_recv()

            far_copy(i).wait_recv()
            gate = part[i, owned, 0] + near[i, ox, 0] + far[i, 0]
            up = part[i, owned, 1] + near[i, ox, 1] + far[i, 1]
            grad = part[i, owned, 2] + near[i, ox, 2] + far[i, 2]
            sig = jax.nn.sigmoid(gate)
            act = gate * sig
            hid[i, 0, owned] = (act * up).astype(BF16)
            hid[i, 1, owned] = (grad * up * sig * (1.0 + gate * (1.0 - sig))).astype(BF16)
            hid[i, 2, owned] = (grad * act).astype(BF16)
            hc_copy(i).start()

        def back_rows(i, k):
            return hid[i, k].reshape(SLOTS * 16, width)

        def add_y(group, i, c):
            acc[group, 0] += dot(back_rows(i, 0), wd[c]).reshape(SLOTS, 16, depth)

        def add_dx(group, i, c):
            acc[group, 1] += (dot_t(back_rows(i, 1), wg[c]) + dot_t(back_rows(i, 2), wu[c])).reshape(SLOTS, 16, depth)

        def back(i):
            group, c = i // chunks, i % chunks
            hc_copy(i).wait_recv()
            hf_copy(i).wait_recv()
            add_y(group, i, c)
            add_dx(group, i, c)
            for other in (1, 2, 3):
                @pl.when(i == other * chunks + chunks - 1)
                def _(other=other):
                    for copy in acc_copies(other):
                        copy.start()

        def step(s, carry):
            @pl.when(jnp.logical_and(s > EARLY, s < total + 1))
            def _():
                i = chunk_at(s - 1)
                half_sum(i, near_copy(i))

            @pl.when(s < total)
            def _():
                products(chunk_at(s))

            for other in (2, 3):
                @pl.when(s == EARLY + 3 * (other - 2))
                def _(other=other):
                    for kind in range(2):
                        for copy in spread_copies(other, kind):
                            copy.start()

            @pl.when(jnp.logical_and(s >= FINAL_LAG, s < total + FINAL_LAG))
            def _():
                activations(chunk_at(s - FINAL_LAG))

            @pl.when(jnp.logical_and(s >= EARLY + FINAL_LAG, s < total - chunks + EARLY + FINAL_LAG))
            def _():
                hx_copy(s - FINAL_LAG + chunks - EARLY).start()

            @pl.when(s == total - chunks + EARLY + FINAL_LAG - 1)
            def _():
                for c in range(EARLY):
                    hx_copy(c).start()

            @pl.when(jnp.logical_and(s >= total - chunks + EARLY + FINAL_LAG, s < total + FINAL_LAG))
            def _():
                hx_copy(s - FINAL_LAG + chunks - total).start()

            @pl.when(jnp.logical_and(s >= FORWARD_LAG, s < FORWARD_LAG + total))
            def _():
                i = (s - FORWARD_LAG + chunks) % total
                hx_copy(i).wait_recv()
                hf_copy(i).start()

            @pl.when(s == total - chunks)
            def _():
                x_turned[...] = cols[:, 0].reshape(GROUPS * SLOTS * 16, depth).T

            @pl.when(s >= BACK_LAG)
            def _():
                back((s - BACK_LAG + chunks) % total)

            return carry

        for c in range(EARLY - FINAL_LAG):
            activations(c)
        lax.fori_loop(EARLY, total + BACK_LAG - 1, step, 0)

        last = chunks - 1
        hc_copy(last).wait_recv()
        hf_copy(last).wait_recv()
        for kind in range(2):
            (add_y, add_dx)[kind](0, last, last)
            if kind == 0:
                took(acc_in, acc_recv.at[0])
            value = acc[0, kind] + acc_in[0, kind] + acc_in[1, kind] + acc_in[2, kind]
            tail[kind] = (cols[0, kind].astype(F32) + value).astype(BF16)
            for k in (2, 3, 1):
                tail_copy(kind, k).start()
        for kind in range(2):
            rows[kind, :, own] = tail[kind, home]

        sent(cols.at[0, :, pl.ds(0, 3)], first_send.at[0])
        sent(cols.at[0], lead_send.at[0])
        sent(cols.at[pl.ds(0, 2)], spread_send.at[0])
        sent(acc_in, acc_send.at[0])
        sent(near, near_send.at[0])
        sent(far, far_send.at[0])
        for send in (hc_send, hx_send, hf_send):
            sent(hid.at[:, :, 0], send.at[0])
        took(tail.at[:, pl.ds(0, 3)], tail_recv.at[0])
        sent(tail.at[:, pl.ds(0, 3)], tail_send.at[0])

    return kernel, total


def finish(rows, hid, cols, x_turned):
    _, local_rows, model = rows.shape
    total, _, _, _, width = hid.shape
    depth, count = x_turned.shape
    chunks = total // GROUPS
    hidden = chunks * width
    ring = 4
    high = 128

    def kernel(rows_ref, hid_ref, cols_ref, x_ref, y_hbm, dx_hbm, dg_hbm, du_hbm, dd_hbm, g_tile, u_tile, d_tile, row_sem, out_sem):
        row_copies = [pltpu.make_async_copy(rows_ref.at[k], dst, row_sem.at[k]) for k, dst in enumerate((y_hbm, dx_hbm))]

        def all_rows(c, k):
            return jnp.concatenate([hid_ref[group * chunks + c, k].reshape(SLOTS * 16, width) for group in range(GROUPS)])

        def block(k, b):
            span = pl.ds(pl.multiple_of(b * high, high), high)
            return pltpu.make_async_copy((g_tile, u_tile)[k].at[b % ring], (dg_hbm, du_hbm)[k].at[span], out_sem.at[k, b % ring])

        def tile(c):
            span = pl.ds(pl.multiple_of(c * width, width), width)
            return pltpu.make_async_copy(d_tile.at[c % ring], dd_hbm.at[span], out_sem.at[2, c % ring])

        def across(b, carry):
            x_block = x_ref[pl.ds(pl.multiple_of(b * high, high), high)]
            for k, held in enumerate((g_tile, u_tile)):
                @pl.when(b >= ring)
                def _(k=k):
                    block(k, b - ring).wait()
                for c in range(chunks):
                    held[b % ring, :, c * width:(c + 1) * width] = dot(x_block, all_rows(c, k + 1))
                block(k, b).start()
            return carry

        def down(c, carry):
            @pl.when(c >= ring)
            def _():
                tile(c - ring).wait()
            d_tile[c % ring] = dot(all_rows(c, 0).T, cols_ref[:, 1].reshape(count, depth))
            tile(c).start()
            return carry

        lax.fori_loop(0, depth // high, across, 0)
        for copy in row_copies:
            copy.start()
        lax.fori_loop(0, chunks, down, 0)
        for b in range(depth // high - ring, depth // high):
            for k in range(2):
                block(k, b).wait()
        for c in range(chunks - ring, chunks):
            tile(c).wait()
        for copy in row_copies:
            copy.wait()

    dma = pltpu.SemaphoreType.DMA
    any_space = pl.BlockSpec(memory_space=pl.ANY)
    vmem = pl.BlockSpec(memory_space=pltpu.VMEM)
    row_shape = jax.ShapeDtypeStruct((local_rows, model), BF16)
    held = [pltpu.with_memory_space_constraint(value, pltpu.VMEM) for value in (rows, hid, cols, x_turned)]
    return pl.pallas_call(
        kernel,
        out_shape=[row_shape, row_shape, jax.ShapeDtypeStruct((depth, hidden), F32), jax.ShapeDtypeStruct((depth, hidden), F32), jax.ShapeDtypeStruct((hidden, depth), F32)],
        in_specs=[vmem] * 4,
        out_specs=[any_space] * 5,
        scratch_shapes=[
            pltpu.VMEM((ring, high, hidden), F32),
            pltpu.VMEM((ring, high, hidden), F32),
            pltpu.VMEM((ring, width, depth), F32),
            dma((2,)), dma((3, ring)),
        ],
        compiler_params=pltpu.CompilerParams(vmem_limit_bytes=40 * 2**20),
        cost_estimate=pl.CostEstimate(flops=6 * count * depth * hidden, bytes_accessed=12 * depth * hidden, transcendentals=0),
    )(*held)


def solution(mesh):
    row_spec = P(None, ("dp", "tp"), None)
    in_specs = (row_spec, P("dp", "tp"), P("dp", "tp"), P("tp", "dp"), row_spec)
    out_specs = (row_spec, row_spec, P("dp", "tp"), P("dp", "tp"), P("tp", "dp"))

    def local_step(x_loc, w_gate_loc, w_up_loc, w_down_loc, dy_loc):
        depth, hidden = w_gate_loc.shape
        micro, local_rows, model = x_loc.shape
        width = 512
        chunks = hidden // width
        kernel, total = make_kernel(chunks, width)
        dma = pltpu.SemaphoreType.DMA
        any_space = pl.BlockSpec(memory_space=pl.ANY)
        vmem = pl.BlockSpec(memory_space=pltpu.VMEM)
        outs = pl.pallas_call(
            kernel,
            out_shape=[
                pltpu.VMEM((2, micro * local_rows, model), BF16),
                pltpu.VMEM((total, 3, SLOTS, 16, width), BF16),
                pltpu.VMEM((GROUPS, 2, SLOTS, 16, depth), BF16),
                pltpu.VMEM((depth, GROUPS * SLOTS * 16), BF16),
            ],
            in_specs=[any_space] * 5,
            out_specs=[vmem] * 4,
            scratch_shapes=[
                pltpu.VMEM((chunks, depth, width), BF16),
                pltpu.VMEM((chunks, depth, width), BF16),
                pltpu.VMEM((chunks, width, depth), BF16),
                pltpu.VMEM((16, model), BF16),
                pltpu.VMEM((16, model), BF16),
                pltpu.VMEM((total, SLOTS, 3, 16, width), F32),
                pltpu.VMEM((total, 2, 3, 16, width), F32),
                pltpu.VMEM((total, 3, 16, width), F32),
                pltpu.VMEM((GROUPS, 2, SLOTS, 16, depth), F32),
                pltpu.VMEM((GROUPS - 1, 2, SLOTS, 16, depth), F32),
                pltpu.VMEM((2, SLOTS, 16, depth), BF16),
                dma((chunks,)),
                dma((1,)), dma((3,)),
                dma((1,)), dma((2,)),
                dma((1,)), dma((8,)),
                dma((1,)), dma((10,)),
                dma((1,)), dma((EARLY + 12,)),
                dma((1,)), dma((12,)),
                dma((1,)), dma((8,)),
                dma((1,)), dma((1,)),
                dma((1,)), dma((1,)),
                dma((2,)), dma((EARLY,)),
                dma((1,)), dma((1,)),
            ],
            compiler_params=pltpu.CompilerParams(collective_id=0, has_side_effects=True, vmem_limit_bytes=53 * 2**20),
        )(x_loc.reshape(micro * local_rows, model), dy_loc.reshape(micro * local_rows, model), w_gate_loc, w_up_loc, w_down_loc)
        y_rows, dx_rows, dw_gate, dw_up, dw_down = finish(*outs)
        return y_rows.reshape(x_loc.shape), dx_rows.reshape(x_loc.shape), dw_gate, dw_up, dw_down

    return jax.shard_map(local_step, mesh=mesh, in_specs=in_specs, out_specs=out_specs, check_vma=False)
```

```python
import jax
import jax.numpy as jnp
from jax import lax
from jax.experimental import pallas as pl
from jax.experimental.pallas import tpu as pltpu
from jax.sharding import PartitionSpec as P

MESH = pl.DeviceIdType.MESH
F32 = jnp.float32
BF16 = jnp.bfloat16
GROUPS = 4
SLOTS = 4
FINAL_LAG = 4
FORWARD_LAG = 10
BACK_LAG = 11
EARLY = 4


def dot(lhs, rhs):
    return lax.dot_general(lhs, rhs, (((1,), (0,)), ((), ())), preferred_element_type=F32)


def dot_t(lhs, rhs):
    return lax.dot_general(lhs, rhs, (((1,), (1,)), ((), ())), preferred_element_type=F32)


def make_kernel(chunks, width):
    total = GROUPS * chunks

    def kernel(x_hbm, dy_hbm, wg_hbm, wu_hbm, wd_hbm,
               rows, hid, cols, x_turned,
               wg, wu, wd, x_ref, dy_ref, part, near, far, acc, acc_in, tail,
               w_sem, first_send, first_recv, spread_send, spread_recv,
               near_send, near_recv, far_send, far_recv,
               hc_send, hc_recv, hx_send, hx_recv, hf_send, hf_recv,
               acc_send, acc_recv, tail_send, tail_recv, in_sem, open_recv, lead_send, lead_recv):
        tp = lax.axis_index("tp")
        dp = lax.axis_index("dp")
        z, y = tp // 2, tp % 2
        x, core = dp // 2, dp % 2
        ox, oc = 1 - x, 1 - core
        core_peer = {"tp": tp, "dp": x * 2 + oc}
        x_peer = {"tp": tp, "dp": ox * 2 + core}
        home = core * 2 + x
        owned = core * 2 + ox
        depth = cols.shape[-1]

        tp_peers = [{"tp": pz * 2 + py, "dp": dp} for pz, py in ((z, 1 - y), (1 - z, y), (1 - z, 1 - y))]
        rows_of = (pl.ds(0, 8), pl.ds(8, 8))

        def place(i):
            return jnp.where(i < EARLY, i, jnp.where(i < chunks, i + total - chunks, i - chunks + EARLY))

        def turn(i):
            return (i + total - chunks) % total

        def chunk_at(s):
            return jnp.where(s < EARLY, s, jnp.where(s < total - chunks + EARLY, s + chunks - EARLY, s + chunks - total))

        def dp_peer(k):
            px, pc = (x + k // 2) % 2, (core + k % 2) % 2
            return px * 2 + pc, pc * 2 + px

        def weight_copies(c):
            span = pl.ds(pl.multiple_of(c * width, width), width)
            return (pltpu.make_async_copy(wg_hbm.at[:, span], wg.at[c], w_sem.at[c]),
                    pltpu.make_async_copy(wu_hbm.at[:, span], wu.at[c], w_sem.at[c]),
                    pltpu.make_async_copy(wd_hbm.at[span], wd.at[c], w_sem.at[c]))

        def weights_in(c):
            size = part.at[pl.ds(0, 8)]
            pltpu.make_async_copy(size, size, w_sem.at[c]).wait()

        def remote(src, dst, send, recv, device):
            return pltpu.make_async_remote_copy(src_ref=src, dst_ref=dst, send_sem=send, recv_sem=recv,
                                                device_id=device, device_id_type=MESH)

        def first_copy(micro, kind, k):
            peer, _ = dp_peer(k)
            src = (x_ref, dy_ref)[kind].at[rows_of[micro], pl.ds(pl.multiple_of(peer * depth, depth), depth)]
            return remote(src, cols.at[0, kind, home, rows_of[micro]], first_send.at[0], first_recv.at[0 if k == 1 else 1 + micro],
                          {"tp": tp, "dp": peer})

        def spread_copies(group, kind):
            if group == 2:
                return [remote(cols.at[0, kind], cols.at[2, kind], spread_send.at[0], spread_recv.at[0], tp_peers[2])]
            return [remote(cols.at[0, kind, :, rows_of[group // 2]], cols.at[group, kind, :, rows_of[way]],
                           spread_send.at[0], spread_recv.at[1], tp_peers[way]) for way in range(2)]

        def lead_copies(far_side, kind):
            side = ox if far_side else x
            return [remote(cols.at[0, kind, core_slot * 2 + side, rows_of[0]], cols.at[1, kind, core_slot * 2 + side, rows_of[way]],
                           lead_send.at[0], lead_recv.at[0], tp_peers[way])
                    for core_slot in range(2) for way in range(2)]

        def near_copy(i):
            return remote(part.at[i, pl.ds(oc * 2, 2)], near.at[i], near_send.at[0], near_recv.at[place(i) % 8], core_peer)

        def open_copy(i, side, recv):
            return remote(part.at[i, oc * 2 + side], near.at[i, side], near_send.at[0], recv, core_peer)

        def here_copy(i):
            return open_copy(i, x, open_recv.at[i])

        def there_copy(i):
            return open_copy(i, ox, near_recv.at[i % 8])

        def far_copy(i):
            return remote(near.at[i, x], far.at[i], far_send.at[0], far_recv.at[place(i) % 8], x_peer)

        def hc_copy(i):
            here = hid.at[i, :, owned]
            return remote(here, here, hc_send.at[0], hc_recv.at[jnp.where(i < EARLY, i, EARLY + turn(i) % 10)], core_peer)

        def hx_copy(i):
            here = hid.at[i, :, owned]
            return remote(here, here, hx_send.at[0], hx_recv.at[turn(i) % 10], x_peer)

        def hf_copy(i):
            there = hid.at[i, :, home]
            return remote(there, there, hf_send.at[0], hf_recv.at[turn(i) % 6], core_peer)

        def acc_copies(group):
            if group == 2:
                return [remote(acc.at[2], acc_in.at[2], acc_send.at[0], acc_recv.at[0], tp_peers[2])]
            return [remote(acc.at[group, :, :, rows_of[way]], acc_in.at[way, :, :, rows_of[group // 2]],
                           acc_send.at[0], acc_recv.at[0], tp_peers[way]) for way in range(2)]

        def tail_copy(kind, k):
            peer, slot = dp_peer(k)
            dst = rows.at[kind, :, pl.ds(pl.multiple_of(dp * depth, depth), depth)]
            return remote(tail.at[kind, slot], dst, tail_send.at[0], tail_recv.at[0], {"tp": tp, "dp": peer})

        barrier = pltpu.get_barrier_semaphore()
        for k in range(1, 4):
            pl.semaphore_signal(barrier, inc=1, device_id=tp_peers[k - 1], device_id_type=MESH)
            pl.semaphore_signal(barrier, inc=1, device_id={"tp": tp, "dp": dp_peer(k)[0]}, device_id_type=MESH)
        row_loads = [pltpu.make_async_copy(src, dst, in_sem.at[k]) for k, (src, dst) in enumerate(((x_hbm, x_ref), (dy_hbm, dy_ref)))]
        for copy in row_loads:
            copy.start()
        for c in range(chunks):
            for copy in weight_copies(c):
                copy.start()

        for copy in row_loads:
            copy.wait()
        pl.semaphore_wait(barrier, 6)

        for micro in range(2):
            for kind in range(2):
                for k in (1, 2, 3):
                    first_copy(micro, kind, k).start()
        own = pl.ds(pl.multiple_of(dp * depth, depth), depth)
        cols[0, 0, home] = x_ref[:, own]
        cols[0, 1, home] = dy_ref[:, own]
        acc[...] = jnp.zeros_like(acc)

        def half_products(i, side):
            rows_in = [jnp.concatenate([cols[0, kind, side], cols[0, kind, 2 + side]]) for kind in range(2)]
            for k, value in enumerate((dot(rows_in[0], wg[i]), dot(rows_in[0], wu[i]), dot_t(rows_in[1], wd[i]))):
                part[i, side, k] = value[:16]
                part[i, 2 + side, k] = value[16:]

        def half_sum(i, copy):
            copy.wait_recv()
            near[i, x] = near[i, x] + part[i, home]
            far_copy(i).start()

        def took(ref, recv):
            remote(ref, ref, recv, recv, core_peer).wait_recv()

        def sent(ref, send):
            remote(ref, ref, send, send, core_peer).wait_send()

        took(cols.at[0, :, 0], first_recv.at[0])
        for kind in range(2):
            for copy in lead_copies(0, kind):
                copy.start()

        def open_here(i, carry):
            weights_in(i)
            half_products(i, x)
            here_copy(i).start()

            @pl.when(i > 0)
            def _():
                half_sum(i - 1, here_copy(i - 1))

            return carry

        lax.fori_loop(0, EARLY, open_here, 0)
        took(cols.at[0, :, 0], first_recv.at[1])
        for kind in range(2):
            for copy in lead_copies(1, kind):
                copy.start()
        half_sum(EARLY - 1, here_copy(EARLY - 1))

        took(cols.at[0, :, 0], first_recv.at[2])

        def open_there(i, carry):
            half_products(i, ox)
            there_copy(i).start()
            return carry

        lax.fori_loop(0, EARLY, open_there, 0)

        def products(i):
            group, c = i // chunks, i % chunks

            @pl.when(jnp.logical_and(group == 1, c >= EARLY))
            def _():
                weights_in(c)

            for other in (1, 2, 3):
                @pl.when(i == other * chunks)
                def _(other=other):
                    took(cols.at[other], lead_recv.at[0] if other == 1 else spread_recv.at[other - 2])

            x_rows = cols[group, 0].reshape(SLOTS * 16, depth)
            dy_rows = cols[group, 1].reshape(SLOTS * 16, depth)
            for k, value in enumerate((dot(x_rows, wg[c]), dot(x_rows, wu[c]), dot_t(dy_rows, wd[c]))):
                for slot in range(SLOTS):
                    part[i, slot, k] = value[slot * 16:(slot + 1) * 16]
            near_copy(i).start()

        def activations(i):
            @pl.when(i < EARLY)
            def _():
                there_copy(i).wait_recv()

            far_copy(i).wait_recv()
            gate = part[i, owned, 0] + near[i, ox, 0] + far[i, 0]
            up = part[i, owned, 1] + near[i, ox, 1] + far[i, 1]
            grad = part[i, owned, 2] + near[i, ox, 2] + far[i, 2]
            sig = jax.nn.sigmoid(gate)
            act = gate * sig
            hid[i, 0, owned] = (act * up).astype(BF16)
            hid[i, 1, owned] = (grad * up * sig * (1.0 + gate * (1.0 - sig))).astype(BF16)
            hid[i, 2, owned] = (grad * act).astype(BF16)
            hc_copy(i).start()

        def back_rows(i, k):
            return hid[i, k].reshape(SLOTS * 16, width)

        def add_y(group, i, c):
            acc[group, 0] += dot(back_rows(i, 0), wd[c]).reshape(SLOTS, 16, depth)

        def add_dx(group, i, c):
            acc[group, 1] += (dot_t(back_rows(i, 1), wg[c]) + dot_t(back_rows(i, 2), wu[c])).reshape(SLOTS, 16, depth)

        def back(i):
            group, c = i // chunks, i % chunks
            hc_copy(i).wait_recv()
            hf_copy(i).wait_recv()
            add_y(group, i, c)
            add_dx(group, i, c)
            for other in (1, 2, 3):
                @pl.when(i == other * chunks + chunks - 1)
                def _(other=other):
                    for copy in acc_copies(other):
                        copy.start()

        def step(s, carry):
            @pl.when(jnp.logical_and(s > EARLY, s < total + 1))
            def _():
                i = chunk_at(s - 1)
                half_sum(i, near_copy(i))

            @pl.when(s < total)
            def _():
                products(chunk_at(s))

            for other in (2, 3):
                @pl.when(s == EARLY + 3 * (other - 2))
                def _(other=other):
                    for kind in range(2):
                        for copy in spread_copies(other, kind):
                            copy.start()

            @pl.when(jnp.logical_and(s >= FINAL_LAG, s < total + FINAL_LAG))
            def _():
                activations(chunk_at(s - FINAL_LAG))

            @pl.when(jnp.logical_and(s >= EARLY + FINAL_LAG, s < total - chunks + EARLY + FINAL_LAG))
            def _():
                hx_copy(s - FINAL_LAG + chunks - EARLY).start()

            @pl.when(s == total)
            def _():
                for c in range(EARLY):
                    hx_copy(c).start()

            @pl.when(jnp.logical_and(s >= total - chunks + EARLY + FINAL_LAG, s < total + FINAL_LAG))
            def _():
                hx_copy(s - FINAL_LAG + chunks - total).start()

            @pl.when(jnp.logical_and(s >= FORWARD_LAG, s < FORWARD_LAG + total))
            def _():
                i = (s - FORWARD_LAG + chunks) % total
                hx_copy(i).wait_recv()
                hf_copy(i).start()

            @pl.when(s == total - chunks)
            def _():
                x_turned[...] = cols[:, 0].reshape(GROUPS * SLOTS * 16, depth).T

            @pl.when(s >= BACK_LAG)
            def _():
                back((s - BACK_LAG + chunks) % total)

            return carry

        lax.fori_loop(EARLY, total + BACK_LAG - 1, step, 0)

        last = chunks - 1
        hc_copy(last).wait_recv()
        hf_copy(last).wait_recv()
        for kind in range(2):
            (add_y, add_dx)[kind](0, last, last)
            if kind == 0:
                took(acc_in, acc_recv.at[0])
            value = acc[0, kind] + acc_in[0, kind] + acc_in[1, kind] + acc_in[2, kind]
            tail[kind] = (cols[0, kind].astype(F32) + value).astype(BF16)
            for k in (2, 3, 1):
                tail_copy(kind, k).start()
        for kind in range(2):
            rows[kind, :, own] = tail[kind, home]

        sent(cols.at[0, :, pl.ds(0, 3)], first_send.at[0])
        sent(cols.at[0], lead_send.at[0])
        sent(cols.at[pl.ds(0, 2)], spread_send.at[0])
        sent(acc_in, acc_send.at[0])
        sent(near, near_send.at[0])
        sent(far, far_send.at[0])
        for send in (hc_send, hx_send, hf_send):
            sent(hid.at[:, :, 0], send.at[0])
        took(tail.at[:, pl.ds(0, 3)], tail_recv.at[0])
        sent(tail.at[:, pl.ds(0, 3)], tail_send.at[0])

    return kernel, total


def finish(rows, hid, cols, x_turned):
    _, local_rows, model = rows.shape
    total, _, _, _, width = hid.shape
    depth, count = x_turned.shape
    chunks = total // GROUPS
    hidden = chunks * width
    ring = 4
    high = 128

    def kernel(rows_ref, hid_ref, cols_ref, x_ref, y_hbm, dx_hbm, dg_hbm, du_hbm, dd_hbm, g_tile, u_tile, d_tile, row_sem, out_sem):
        row_copies = [pltpu.make_async_copy(rows_ref.at[k], dst, row_sem.at[k]) for k, dst in enumerate((y_hbm, dx_hbm))]

        def all_rows(c, k):
            return jnp.concatenate([hid_ref[group * chunks + c, k].reshape(SLOTS * 16, width) for group in range(GROUPS)])

        def block(k, b):
            span = pl.ds(pl.multiple_of(b * high, high), high)
            return pltpu.make_async_copy((g_tile, u_tile)[k].at[b % ring], (dg_hbm, du_hbm)[k].at[span], out_sem.at[k, b % ring])

        def tile(c):
            span = pl.ds(pl.multiple_of(c * width, width), width)
            return pltpu.make_async_copy(d_tile.at[c % ring], dd_hbm.at[span], out_sem.at[2, c % ring])

        def across(b, carry):
            x_block = x_ref[pl.ds(pl.multiple_of(b * high, high), high)]
            for k, held in enumerate((g_tile, u_tile)):
                @pl.when(b >= ring)
                def _(k=k):
                    block(k, b - ring).wait()
                for c in range(chunks):
                    held[b % ring, :, c * width:(c + 1) * width] = dot(x_block, all_rows(c, k + 1))
                block(k, b).start()
            return carry

        def down(c, carry):
            @pl.when(c >= ring)
            def _():
                tile(c - ring).wait()
            d_tile[c % ring] = dot(all_rows(c, 0).T, cols_ref[:, 1].reshape(count, depth))
            tile(c).start()
            return carry

        lax.fori_loop(0, depth // high, across, 0)
        for copy in row_copies:
            copy.start()
        lax.fori_loop(0, chunks, down, 0)
        for b in range(depth // high - ring, depth // high):
            for k in range(2):
                block(k, b).wait()
        for c in range(chunks - ring, chunks):
            tile(c).wait()
        for copy in row_copies:
            copy.wait()

    dma = pltpu.SemaphoreType.DMA
    any_space = pl.BlockSpec(memory_space=pl.ANY)
    vmem = pl.BlockSpec(memory_space=pltpu.VMEM)
    row_shape = jax.ShapeDtypeStruct((local_rows, model), BF16)
    held = [pltpu.with_memory_space_constraint(value, pltpu.VMEM) for value in (rows, hid, cols, x_turned)]
    return pl.pallas_call(
        kernel,
        out_shape=[row_shape, row_shape, jax.ShapeDtypeStruct((depth, hidden), F32), jax.ShapeDtypeStruct((depth, hidden), F32), jax.ShapeDtypeStruct((hidden, depth), F32)],
        in_specs=[vmem] * 4,
        out_specs=[any_space] * 5,
        scratch_shapes=[
            pltpu.VMEM((ring, high, hidden), F32),
            pltpu.VMEM((ring, high, hidden), F32),
            pltpu.VMEM((ring, width, depth), F32),
            dma((2,)), dma((3, ring)),
        ],
        compiler_params=pltpu.CompilerParams(vmem_limit_bytes=40 * 2**20),
        cost_estimate=pl.CostEstimate(flops=6 * count * depth * hidden, bytes_accessed=12 * depth * hidden, transcendentals=0),
    )(*held)


def solution(mesh):
    row_spec = P(None, ("dp", "tp"), None)
    in_specs = (row_spec, P("dp", "tp"), P("dp", "tp"), P("tp", "dp"), row_spec)
    out_specs = (row_spec, row_spec, P("dp", "tp"), P("dp", "tp"), P("tp", "dp"))

    def local_step(x_loc, w_gate_loc, w_up_loc, w_down_loc, dy_loc):
        depth, hidden = w_gate_loc.shape
        micro, local_rows, model = x_loc.shape
        width = 512
        chunks = hidden // width
        kernel, total = make_kernel(chunks, width)
        dma = pltpu.SemaphoreType.DMA
        any_space = pl.BlockSpec(memory_space=pl.ANY)
        vmem = pl.BlockSpec(memory_space=pltpu.VMEM)
        outs = pl.pallas_call(
            kernel,
            out_shape=[
                pltpu.VMEM((2, micro * local_rows, model), BF16),
                pltpu.VMEM((total, 3, SLOTS, 16, width), BF16),
                pltpu.VMEM((GROUPS, 2, SLOTS, 16, depth), BF16),
                pltpu.VMEM((depth, GROUPS * SLOTS * 16), BF16),
            ],
            in_specs=[any_space] * 5,
            out_specs=[vmem] * 4,
            scratch_shapes=[
                pltpu.VMEM((chunks, depth, width), BF16),
                pltpu.VMEM((chunks, depth, width), BF16),
                pltpu.VMEM((chunks, width, depth), BF16),
                pltpu.VMEM((16, model), BF16),
                pltpu.VMEM((16, model), BF16),
                pltpu.VMEM((total, SLOTS, 3, 16, width), F32),
                pltpu.VMEM((total, 2, 3, 16, width), F32),
                pltpu.VMEM((total, 3, 16, width), F32),
                pltpu.VMEM((GROUPS, 2, SLOTS, 16, depth), F32),
                pltpu.VMEM((GROUPS - 1, 2, SLOTS, 16, depth), F32),
                pltpu.VMEM((2, SLOTS, 16, depth), BF16),
                dma((chunks,)),
                dma((1,)), dma((3,)),
                dma((1,)), dma((2,)),
                dma((1,)), dma((8,)),
                dma((1,)), dma((8,)),
                dma((1,)), dma((EARLY + 10,)),
                dma((1,)), dma((10,)),
                dma((1,)), dma((6,)),
                dma((1,)), dma((1,)),
                dma((1,)), dma((1,)),
                dma((2,)), dma((EARLY,)),
                dma((1,)), dma((1,)),
            ],
            compiler_params=pltpu.CompilerParams(collective_id=0, has_side_effects=True, vmem_limit_bytes=53 * 2**20),
        )(x_loc.reshape(micro * local_rows, model), dy_loc.reshape(micro * local_rows, model), w_gate_loc, w_up_loc, w_down_loc)
        y_rows, dx_rows, dw_gate, dw_up, dw_down = finish(*outs)
        return y_rows.reshape(x_loc.shape), dx_rows.reshape(x_loc.shape), dw_gate, dw_up, dw_down

    return jax.shard_map(local_step, mesh=mesh, in_specs=in_specs, out_specs=out_specs, check_vma=False)
```
